8 devices in a mesh: fsdp: 8 (over z, y, x, core).
Axes of the slice: x: 2, y: 2, z: 1, core: 2. Of those that a mesh axis runs over, the one named last changes fastest.
Arguments:
- hidden: bfloat16 [24, 512, 2048], P('fsdp')
- positions: int32 [24, 512], P('fsdp')
- grad_y: bfloat16 [24, 512, 2048], P('fsdp')
- attn_gain: bfloat16 [2048], P('fsdp')
- w_qkv: bfloat16 [2048, 2560], P('fsdp')
- b_qkv: bfloat16 [2560], P('fsdp')
- w_out: bfloat16 [2048, 2048], P('fsdp')
- mlp_gain: bfloat16 [2048], P('fsdp')
- w_up: bfloat16 [2048, 22016], P('fsdp')
- w_down: bfloat16 [11008, 2048], P('fsdp')
Outputs:
- output 1: bfloat16 [24, 512, 2048], P('fsdp')
- output 2: bfloat16 [24, 512, 2048], P('fsdp')
- output 3: float32 [2048], P('fsdp')
- output 4: float32 [2048, 2560], P('fsdp')
- output 5: float32 [2560], P('fsdp')
- output 6: float32 [2048, 2048], P('fsdp')
- output 7: float32 [2048], P('fsdp')
- output 8: float32 [2048, 22016], P('fsdp')
- output 9: float32 [11008, 2048], P('fsdp')
All inputs are finite; a program needn't handle non-finite values.
Results may differ from the reference program's by a relative error of at most 0.0161931.
Values are sent between devices in bfloat16 or wider.
A program may use at most 1 GiB of HBM per device.

```python
import jax
import jax.numpy as jnp
from jax import lax

H = 2048
HEADS = 16
KV_HEADS = 2
HEAD = 128
FF = 11008
BATCH = 24
SEQ = 512

QKV = (HEADS + 2 * KV_HEADS) * HEAD
Q_WIDTH = HEADS * HEAD
KV_WIDTH = KV_HEADS * HEAD
GROUP = HEADS // KV_HEADS
ROT_DIM = HEAD // 2
TOKENS = BATCH * SEQ
ROPE_BASE = 10000.0
EPS = 1e-5
SCALE = HEAD ** -0.5
CONTRACT_ROWS = (((0,), (0,)), ((), ()))
CONTRACT_COLS = (((1,), (1,)), ((), ()))


def setup_inputs(seed: int = 0) -> dict:
    rng_keys = jax.random.split(jax.random.key(seed), 11)
    hidden = jax.random.normal(rng_keys[0], (BATCH, SEQ, H), jnp.float32)
    pos_gaps = jax.random.randint(rng_keys[1], (BATCH, SEQ), 1, 4)
    starts = jax.random.randint(rng_keys[2], (BATCH, 1), 0, 64)
    positions = (starts + jnp.cumsum(pos_gaps, axis=1)).astype(jnp.int32)
    grad_y = jax.random.normal(rng_keys[3], (BATCH, SEQ, H), jnp.float32)
    attn_gain = 1.0 + 0.3 * jax.random.normal(rng_keys[4], (H,), jnp.float32)
    w_qkv = (1.5 * H ** -0.5) * jax.random.normal(rng_keys[5], (H, QKV), jnp.float32)
    b_qkv = 0.5 * jax.random.normal(rng_keys[6], (QKV,), jnp.float32)
    w_out = Q_WIDTH ** -0.5 * jax.random.normal(rng_keys[7], (Q_WIDTH, H), jnp.float32)
    mlp_gain = 1.0 + 0.3 * jax.random.normal(rng_keys[8], (H,), jnp.float32)
    w_up = H ** -0.5 * jax.random.normal(rng_keys[9], (H, 2 * FF), jnp.float32)
    w_down = FF ** -0.5 * jax.random.normal(rng_keys[10], (FF, H), jnp.float32)
    return {
        'hidden': hidden.astype(jnp.bfloat16),
        'positions': positions,
        'grad_y': grad_y.astype(jnp.bfloat16),
        'attn_gain': attn_gain.astype(jnp.bfloat16),
        'w_qkv': w_qkv.astype(jnp.bfloat16),
        'b_qkv': b_qkv.astype(jnp.bfloat16),
        'w_out': w_out.astype(jnp.bfloat16),
        'mlp_gain': mlp_gain.astype(jnp.bfloat16),
        'w_up': w_up.astype(jnp.bfloat16),
        'w_down': w_down.astype(jnp.bfloat16),
    }


def norm_scale(rows_in):
    return lax.rsqrt(jnp.mean(rows_in * rows_in, axis=-1, keepdims=True) + EPS)


def rope_turn(head_vals, cos_t, sin_t):
    lead_shape = head_vals.shape[:-1]
    rot_pairs = head_vals[..., :ROT_DIM].reshape(lead_shape + (ROT_DIM // 2, 2))
    even_part = rot_pairs[..., 0]
    odd_part = rot_pairs[..., 1]
    turned = jnp.stack([even_part * cos_t - odd_part * sin_t, odd_part * cos_t + even_part * sin_t], axis=-1)
    return jnp.concatenate([turned.reshape(lead_shape + (ROT_DIM,)), head_vals[..., ROT_DIM:]], axis=-1)


def causal_mask():
    token_index = jnp.arange(SEQ)
    return token_index[:, None] >= token_index[None, :]


def attend_forward(operands):
    q_rot, k_rot, values = operands
    scores = jnp.einsum('qkgd,skd->kgqs', q_rot.astype(jnp.float32), k_rot.astype(jnp.float32)) * SCALE
    attn_probs = jax.nn.softmax(jnp.where(causal_mask(), scores, -1e30), axis=-1)
    context = jnp.einsum('kgqs,skd->qkgd', attn_probs.astype(jnp.bfloat16).astype(jnp.float32), values.astype(jnp.float32))
    return context.astype(jnp.bfloat16)


def attend_backward(operands):
    q_rot, k_rot, values, d_context = operands
    q_wide = q_rot.astype(jnp.float32)
    k_wide = k_rot.astype(jnp.float32)
    v_wide = values.astype(jnp.float32)
    dc_wide = d_context.astype(jnp.float32)
    scores = jnp.einsum('qkgd,skd->kgqs', q_wide, k_wide) * SCALE
    attn_probs = jax.nn.softmax(jnp.where(causal_mask(), scores, -1e30), axis=-1)
    d_probs = jnp.einsum('qkgd,skd->kgqs', dc_wide, v_wide)
    d_values = jnp.einsum('kgqs,qkgd->skd', attn_probs.astype(jnp.bfloat16).astype(jnp.float32), dc_wide)
    d_scores = attn_probs * (d_probs - jnp.sum(attn_probs * d_probs, axis=-1, keepdims=True)) * SCALE
    ds_wide = d_scores.astype(jnp.bfloat16).astype(jnp.float32)
    d_query = jnp.einsum('kgqs,skd->qkgd', ds_wide, k_wide)
    d_key = jnp.einsum('kgqs,qkgd->skd', ds_wide, q_wide)
    return d_query, d_key, d_values


def reference(hidden, positions, grad_y, attn_gain, w_qkv, b_qkv, w_out, mlp_gain, w_up, w_down):
    inv_freq = 1.0 / (ROPE_BASE ** (jnp.arange(0, ROT_DIM, 2, dtype=jnp.float32) / ROT_DIM))
    angles = positions.astype(jnp.float32)[:, :, None, None] * inv_freq
    cos_t = jnp.cos(angles)
    sin_t = jnp.sin(angles)
    hid_wide = hidden.reshape(TOKENS, H).astype(jnp.float32)
    inv_one = norm_scale(hid_wide)
    gain_one = attn_gain.astype(jnp.float32)
    normed = (hid_wide * inv_one * gain_one).astype(jnp.bfloat16)
    qkv_proj = jnp.dot(normed, w_qkv, preferred_element_type=jnp.float32) + b_qkv.astype(jnp.float32)
    qkv_proj = qkv_proj.reshape(BATCH, SEQ, QKV)
    q_rot = rope_turn(qkv_proj[..., :Q_WIDTH].reshape(BATCH, SEQ, HEADS, HEAD), cos_t, sin_t)
    q_rot = q_rot.astype(jnp.bfloat16).reshape(BATCH, SEQ, KV_HEADS, GROUP, HEAD)
    k_rot = rope_turn(qkv_proj[..., Q_WIDTH:Q_WIDTH + KV_WIDTH].reshape(BATCH, SEQ, KV_HEADS, HEAD), cos_t, sin_t).astype(jnp.bfloat16)
    values = qkv_proj[..., Q_WIDTH + KV_WIDTH:].reshape(BATCH, SEQ, KV_HEADS, HEAD).astype(jnp.bfloat16)
    context = lax.map(attend_forward, (q_rot, k_rot, values)).reshape(TOKENS, Q_WIDTH)
    mid_state = (hid_wide + jnp.dot(context, w_out, preferred_element_type=jnp.float32)).astype(jnp.bfloat16)
    mid_wide = mid_state.astype(jnp.float32)
    inv_two = norm_scale(mid_wide)
    gain_two = mlp_gain.astype(jnp.float32)
    mlp_in = (mid_wide * inv_two * gain_two).astype(jnp.bfloat16)
    up_all = jnp.dot(mlp_in, w_up, preferred_element_type=jnp.float32).astype(jnp.bfloat16)
    gate_val = up_all[:, :FF].astype(jnp.float32)
    lin_val = up_all[:, FF:].astype(jnp.float32)
    sigmoid_gate = jax.nn.sigmoid(gate_val)
    act_val = (gate_val * sigmoid_gate * lin_val).astype(jnp.bfloat16)
    output = (mid_wide + jnp.dot(act_val, w_down, preferred_element_type=jnp.float32)).astype(jnp.bfloat16)

    dy_flat = grad_y.reshape(TOKENS, H)
    grad_w_down = lax.dot_general(act_val, dy_flat, CONTRACT_ROWS, preferred_element_type=jnp.float32)
    d_act = lax.dot_general(dy_flat, w_down, CONTRACT_COLS, preferred_element_type=jnp.float32)
    d_gate = d_act * lin_val * sigmoid_gate * (1.0 + gate_val * (1.0 - sigmoid_gate))
    d_lin = d_act * gate_val * sigmoid_gate
    d_up = jnp.concatenate([d_gate, d_lin], axis=1).astype(jnp.bfloat16)
    grad_w_up = lax.dot_general(mlp_in, d_up, CONTRACT_ROWS, preferred_element_type=jnp.float32)
    d_mlp_in = lax.dot_general(d_up, w_up, CONTRACT_COLS, preferred_element_type=jnp.float32)
    grad_mlp_gain = jnp.sum(d_mlp_in * mid_wide * inv_two, axis=0)
    scaled_two = d_mlp_in * gain_two
    d_mid = dy_flat.astype(jnp.float32) + inv_two * (scaled_two - mid_wide * inv_two * inv_two * jnp.mean(scaled_two * mid_wide, axis=-1, keepdims=True))
    d_mid_low = d_mid.astype(jnp.bfloat16)
    grad_w_out = lax.dot_general(context, d_mid_low, CONTRACT_ROWS, preferred_element_type=jnp.float32)
    d_context = lax.dot_general(d_mid_low, w_out, CONTRACT_COLS, preferred_element_type=jnp.float32)
    d_context = d_context.astype(jnp.bfloat16).reshape(BATCH, SEQ, KV_HEADS, GROUP, HEAD)
    d_query, d_key, d_values = lax.map(attend_backward, (q_rot, k_rot, values, d_context))
    d_query = rope_turn(d_query.reshape(BATCH, SEQ, HEADS, HEAD), cos_t, -sin_t)
    d_key = rope_turn(d_key, cos_t, -sin_t)
    d_proj = jnp.concatenate([d_query.reshape(TOKENS, Q_WIDTH), d_key.reshape(TOKENS, KV_WIDTH), d_values.reshape(TOKENS, KV_WIDTH)], axis=1)
    grad_b_qkv = jnp.sum(d_proj, axis=0)
    d_proj_low = d_proj.astype(jnp.bfloat16)
    grad_w_qkv = lax.dot_general(normed, d_proj_low, CONTRACT_ROWS, preferred_element_type=jnp.float32)
    d_normed = lax.dot_general(d_proj_low, w_qkv, CONTRACT_COLS, preferred_element_type=jnp.float32)
    grad_attn_gain = jnp.sum(d_normed * hid_wide * inv_one, axis=0)
    scaled_one = d_normed * gain_one
    grad_hidden = (d_mid + inv_one * (scaled_one - hid_wide * inv_one * inv_one * jnp.mean(scaled_one * hid_wide, axis=-1, keepdims=True))).astype(jnp.bfloat16)
    return (output.reshape(BATCH, SEQ, H), grad_hidden.reshape(BATCH, SEQ, H), grad_attn_gain, grad_w_qkv, grad_b_qkv, grad_w_out, grad_mlp_gain, grad_w_up, grad_w_down)
```

```python
import jax
import jax.numpy as jnp
from jax import lax
from jax.sharding import PartitionSpec as P

HEAD_DIM = 128
ROPE_BASE = 10000.0
EPS = 1e-5

NT_DIMS = (((1,), (1,)), ((), ()))
TN_DIMS = (((0,), (0,)), ((), ()))
NN_DIMS = (((1,), (0,)), ((), ()))
F32 = jnp.float32
BF16 = jnp.bfloat16


def mm(a, b, dims):
    return lax.dot_general(a, b, dims, preferred_element_type=F32)


def norm_scale(rows_in):
    return lax.rsqrt(jnp.mean(rows_in * rows_in, axis=-1, keepdims=True) + EPS)


def rope_tables(positions):
    rot_dim = HEAD_DIM // 2
    inv_freq = 1.0 / (ROPE_BASE ** (jnp.arange(0, rot_dim, 2, dtype=F32) / rot_dim))
    angles = positions.astype(F32)[:, :, None, None] * inv_freq
    return jnp.cos(angles), jnp.sin(angles)


def rope_turn(head_vals, cos_t, sin_t):
    rot_dim = HEAD_DIM // 2
    lead_shape = head_vals.shape[:-1]
    rot_pairs = head_vals[..., :rot_dim].reshape(lead_shape + (rot_dim // 2, 2))
    even_part = rot_pairs[..., 0]
    odd_part = rot_pairs[..., 1]
    turned = jnp.stack([even_part * cos_t - odd_part * sin_t, odd_part * cos_t + even_part * sin_t], axis=-1)
    return jnp.concatenate([turned.reshape(lead_shape + (rot_dim,)), head_vals[..., rot_dim:]], axis=-1)


def attend_forward(q_rot, k_rot, values):
    seq_len = q_rot.shape[1]
    token_index = jnp.arange(seq_len)
    causal = token_index[:, None] >= token_index[None, :]
    scores = jnp.einsum('bqkgd,bskd->bkgqs', q_rot, k_rot, preferred_element_type=F32) * HEAD_DIM ** -0.5
    attn_probs = jax.nn.softmax(jnp.where(causal, scores, -1e30), axis=-1)
    probs_low = attn_probs.astype(BF16)
    context = jnp.einsum('bkgqs,bskd->bqkgd', probs_low, values, preferred_element_type=F32)
    return context.astype(BF16), attn_probs, probs_low


def attend_backward(q_rot, k_rot, values, attn_probs, probs_low, d_context):
    d_probs = jnp.einsum('bqkgd,bskd->bkgqs', d_context, values, preferred_element_type=F32)
    d_values = jnp.einsum('bkgqs,bqkgd->bskd', probs_low, d_context, preferred_element_type=F32)
    d_scores = attn_probs * (d_probs - jnp.sum(attn_probs * d_probs, axis=-1, keepdims=True)) * HEAD_DIM ** -0.5
    d_scores = d_scores.astype(BF16)
    d_query = jnp.einsum('bkgqs,bskd->bqkgd', d_scores, k_rot, preferred_element_type=F32)
    d_key = jnp.einsum('bkgqs,bqkgd->bskd', d_scores, q_rot, preferred_element_type=F32)
    return d_query, d_key, d_values


def solution(mesh):
    ax = mesh.axis_names[0]
    n_dev = mesh.shape[ax]
    group = n_dev // 2

    def hop(v, k):
        return lax.ppermute(v, ax, [(i, i ^ k) for i in range(n_dev)])

    def gather_rows(shard):
        return lax.all_gather(shard, ax, axis=0, tiled=True)

    def scatter_rows(full):
        return lax.psum_scatter(full, ax, scatter_dimension=0, tiled=True)

    def local_step(hidden, positions, grad_y, attn_gain, w_qkv, b_qkv, w_out, mlp_gain, w_up, w_down):
        batch, seq_len, width = hidden.shape
        tokens = batch * seq_len
        h_loc = w_up.shape[0]
        h_half = h_loc * group
        f_loc = w_down.shape[0]
        pad = -(2 * f_loc) % 256
        f_pad = 2 * f_loc + pad
        q_loc = b_qkv.shape[0]
        me = lax.axis_index(ax)
        rank = lax.rem(me, group)
        side = lax.div(me, group)

        small = gather_rows(jnp.concatenate([attn_gain, b_qkv, mlp_gain])[None])
        gain_one = small[:, :h_loc].reshape(1, width).astype(F32)
        bias = small[:, h_loc:h_loc + q_loc].reshape(1, n_dev * q_loc).astype(F32)
        gain_two = small[:, h_loc + q_loc:].reshape(1, width).astype(F32)
        wqkv = gather_rows(w_qkv)
        wout = gather_rows(w_out)

        def blank(rows):
            return jnp.zeros((rows, pad), BF16)

        up_blocks = [w_up[:, j * f_loc:(j + 1) * f_loc] for j in range(2 * n_dev)]
        up_for = jnp.stack([jnp.concatenate([up_blocks[q], up_blocks[group + q], blank(h_loc), up_blocks[n_dev + q], up_blocks[n_dev + group + q], blank(h_loc)], axis=1) for q in range(group)])
        up_part = [lax.dynamic_index_in_dim(up_for, rank ^ k, 0, keepdims=False) for k in range(group)]
        up_near = [up_part[0]] + [hop(up_part[k], k) for k in (1, 2, 3)]
        up_far = [hop(v, group) for v in up_near]
        w_all = jnp.zeros((width, 2 * f_pad), BF16)
        for k in range(group):
            w_all = lax.dynamic_update_slice(w_all, up_near[k], ((me ^ k) * h_loc, 0))
            w_all = lax.dynamic_update_slice(w_all, up_far[k], ((me ^ group ^ k) * h_loc, 0))
        down_far = hop(w_down, group)
        first = side == 0
        wd_all = jnp.concatenate([jnp.where(first, w_down, down_far), jnp.where(first, down_far, w_down), jnp.zeros((pad, width), BF16)], axis=0)

        def spread(v):
            v1 = hop(v, 1)
            v2 = hop(v, 2)
            v3 = hop(v2, 1)
            return jnp.concatenate([v, v1, v2, v3], axis=0)

        dy = grad_y.reshape(tokens, width)
        dy_all = spread(dy)

        hid_wide = hidden.astype(F32).reshape(tokens, width)
        inv_one = norm_scale(hid_wide)
        normed = (hid_wide * inv_one * gain_one).astype(BF16)
        q_width = wout.shape[0]
        kv_width = (wqkv.shape[1] - q_width) // 2
        kv_heads = kv_width // HEAD_DIM
        heads = q_width // HEAD_DIM
        cos_t, sin_t = rope_tables(positions)
        z = (mm(normed, wqkv, NN_DIMS) + bias).reshape(batch, seq_len, q_width + 2 * kv_width)
        q_rot = rope_turn(z[..., :q_width].reshape(batch, seq_len, heads, HEAD_DIM), cos_t, sin_t).astype(BF16)
        q_rot = q_rot.reshape(batch, seq_len, kv_heads, heads // kv_heads, HEAD_DIM)
        k_rot = rope_turn(z[..., q_width:q_width + kv_width].reshape(batch, seq_len, kv_heads, HEAD_DIM), cos_t, sin_t).astype(BF16)
        values = z[..., q_width + kv_width:].reshape(batch, seq_len, kv_heads, HEAD_DIM).astype(BF16)
        context, attn_probs, probs_low = attend_forward(q_rot, k_rot, values)
        context = context.reshape(tokens, q_width)
        mid = (hid_wide + mm(context, wout, NN_DIMS)).astype(BF16)
        mid_wide = mid.astype(F32)
        inv_two = norm_scale(mid_wide)
        mlp_in = (mid_wide * inv_two * gain_two).astype(BF16)
        m_all = spread(mlp_in)

        up = mm(m_all, w_all, NN_DIMS).astype(BF16)
        gate = up[:, :f_pad].astype(F32)
        lin = up[:, f_pad:].astype(F32)
        sig = jax.nn.sigmoid(gate)
        act = (gate * sig * lin).astype(BF16)

        def fold(rows, w, dims):
            parts = [mm(rows[k * tokens:(k + 1) * tokens], w, dims) for k in range(group)]
            cross = hop(parts[2] + hop(parts[3], 1), 2)
            return parts[0], hop(parts[1], 1), cross

        half = width // 2
        down_grads = []
        for j in range(2):
            g_full = mm(act, dy_all[:, j * half:(j + 1) * half], TN_DIMS)
            mine = lax.dynamic_slice(g_full, (side * f_loc, 0), (f_loc, half))
            other = lax.dynamic_slice(g_full, ((1 - side) * f_loc, 0), (f_loc, half))
            down_grads.append(mine + hop(other, group))
        grad_w_down = jnp.concatenate(down_grads, axis=1)

        d_act = mm(dy_all, wd_all, NT_DIMS)
        d_gate = d_act * lin * sig * (1.0 + gate * (1.0 - sig))
        d_lin = d_act * gate * sig
        d_up = jnp.concatenate([d_gate, d_lin], axis=1).astype(BF16)
        d_m = sum(fold(d_up, w_all, NT_DIMS))
        y_sum = fold(act, wd_all, NN_DIMS)

        pieces = [None] * group
        for k in (2, 3, 1, 0):
            far_cols = lax.dynamic_slice(m_all, (0, (me ^ group ^ k) * h_loc), (group * tokens, h_loc))
            far_sum = hop(mm(far_cols, d_up, TN_DIMS), group)
            near_cols = lax.dynamic_slice(m_all, (0, (me ^ k) * h_loc), (group * tokens, h_loc))
            near_sum = mm(near_cols, d_up, TN_DIMS) + far_sum
            pieces[k] = near_sum if k == 0 else hop(near_sum, k)
        stacked = jnp.stack(pieces)
        by_rank = [lax.dynamic_index_in_dim(stacked, rank ^ q, 0, keepdims=False) for q in range(group)]
        cols = [v[:, lo:lo + f_loc] for lo in (0, f_loc, f_pad, f_pad + f_loc) for v in by_rank]
        grad_w_up = jnp.concatenate(cols, axis=1)

        grad_mlp_gain = jnp.sum(d_m * mid_wide * inv_two, axis=0)
        scaled_two = d_m * gain_two
        d_mid = dy.astype(F32) + inv_two * (scaled_two - mid_wide * inv_two * inv_two * jnp.mean(scaled_two * mid_wide, axis=-1, keepdims=True))
        d_mid_low = d_mid.astype(BF16)
        grad_w_out = scatter_rows(mm(context, d_mid_low, TN_DIMS))
        d_context = mm(d_mid_low, wout, NT_DIMS).astype(BF16).reshape(batch, seq_len, kv_heads, heads // kv_heads, HEAD_DIM)
        d_query, d_key, d_values = attend_backward(q_rot, k_rot, values, attn_probs, probs_low, d_context)
        d_query = rope_turn(d_query.reshape(batch, seq_len, heads, HEAD_DIM), cos_t, -sin_t)
        d_key = rope_turn(d_key, cos_t, -sin_t)
        d_proj = jnp.concatenate([d_query.reshape(tokens, q_width), d_key.reshape(tokens, kv_width), d_values.reshape(tokens, kv_width)], axis=1)
        grad_b_qkv = jnp.sum(d_proj, axis=0)
        d_proj_low = d_proj.astype(BF16)
        grad_w_qkv = scatter_rows(mm(normed, d_proj_low, TN_DIMS))
        d_normed = mm(d_proj_low, wqkv, NT_DIMS)
        y_sum, mid_late, d_normed = lax.optimization_barrier((y_sum, mid, d_normed))
        output = (mid_late.astype(F32) + (y_sum[0] + y_sum[1] + y_sum[2])).astype(BF16)
        grad_attn_gain = jnp.sum(d_normed * hid_wide * inv_one, axis=0)
        scaled_one = d_normed * gain_one
        grad_hidden = (d_mid + inv_one * (scaled_one - hid_wide * inv_one * inv_one * jnp.mean(scaled_one * hid_wide, axis=-1, keepdims=True))).astype(BF16)
        small_grads = scatter_rows(jnp.concatenate([grad_attn_gain.reshape(n_dev, h_loc), grad_b_qkv.reshape(n_dev, q_loc), grad_mlp_gain.reshape(n_dev, h_loc)], axis=1)).reshape(-1)
        return (output.reshape(hidden.shape), grad_hidden.reshape(hidden.shape), small_grads[:h_loc], grad_w_qkv, small_grads[h_loc:h_loc + q_loc], grad_w_out, small_grads[h_loc + q_loc:], grad_w_up, grad_w_down)

    row_spec = P(ax)
    return jax.shard_map(local_step, mesh=mesh, in_specs=(row_spec,) * 10, out_specs=(row_spec,) * 9, check_vma=False)
```

```python
import functools

import jax
import jax.numpy as jnp
from jax import lax
from jax.experimental import pallas as pl
from jax.experimental.pallas import tpu as pltpu
from jax.sharding import PartitionSpec as P


HEAD_DIM = 128
ROT_DIM = 64
ROPE_BASE = 10000.0
EPS = 1e-5

NT_DIMS = (((1,), (1,)), ((), ()))
TN_DIMS = (((0,), (0,)), ((), ()))
NN_DIMS = (((1,), (0,)), ((), ()))
F32 = jnp.float32
BF16 = jnp.bfloat16
SCALE = HEAD_DIM ** -0.5
MASKED = -1e30
Q_BLOCK = 256


def mm(a, b, dims):
    return lax.dot_general(a, b, dims, preferred_element_type=F32)


def after(*vals):
    return lax.optimization_barrier(vals)


def norm_scale(rows_in):
    return lax.rsqrt(jnp.mean(rows_in * rows_in, axis=-1, keepdims=True) + EPS)


def rope_tables(positions):
    lane = jnp.arange(HEAD_DIM, dtype=jnp.int32)
    pair = (lane - lane % 2).astype(F32)
    inv_freq = 1.0 / (ROPE_BASE ** (pair / ROT_DIM))
    angles = positions.astype(F32).reshape(-1, 1) * inv_freq
    turned = lane < ROT_DIM
    sines = jnp.sin(angles)
    return jnp.where(turned, jnp.cos(angles), 1.0), jnp.where(turned, jnp.where(lane % 2 == 0, -sines, sines), 0.0)


def swap_pairs(v):
    lane = lax.broadcasted_iota(jnp.int32, v.shape, 1)
    return jnp.where(lane % 2 == 0, pltpu.roll(v, HEAD_DIM - 1, 1), pltpu.roll(v, 1, 1))


def causal_probs(q, k, row0):
    s = mm(q, k, NT_DIMS) * SCALE
    row = lax.broadcasted_iota(jnp.int32, s.shape, 0) + row0
    col = lax.broadcasted_iota(jnp.int32, s.shape, 1)
    s = jnp.where(row >= col, s, MASKED)
    e = jnp.exp(s - jnp.max(s, axis=1, keepdims=True))
    return e * (1.0 / jnp.sum(e, axis=1, keepdims=True))


def attend_kernel(heads, kv_heads, z_ref, cos_ref, sin_ref, qkv_ref, ctx_ref):
    seq_len = z_ref.shape[0]
    group = heads // kv_heads
    cos_t, sin_t = cos_ref[...], sin_ref[...]

    def cols(i):
        return pl.ds(pl.multiple_of(i * HEAD_DIM, HEAD_DIM), HEAD_DIM)

    for g in range(kv_heads):
        kc, vc = cols(heads + g), cols(heads + kv_heads + g)
        zk = z_ref[:, kc]
        qkv_ref[:, kc] = (zk * cos_t + swap_pairs(zk) * sin_t).astype(BF16)
        qkv_ref[:, vc] = z_ref[:, vc].astype(BF16)

        @pl.loop(0, group)
        def _(h):
            hc = cols(g * group + h)
            zq = z_ref[:, hc]
            q = (zq * cos_t + swap_pairs(zq) * sin_t).astype(BF16)
            qkv_ref[:, hc] = q
            for r in range(0, seq_len, Q_BLOCK):
                n = r + Q_BLOCK
                p = causal_probs(q[r:n], qkv_ref[:n, kc], r).astype(BF16)
                ctx_ref[r:n, hc] = mm(p, qkv_ref[:n, vc], NN_DIMS).astype(BF16)


def attend_back_kernel(heads, kv_heads, qkv_ref, dctx_ref, cos_ref, sin_ref, dz_ref, sum_ref, dk_ref, dv_ref):
    seq_len = qkv_ref.shape[0]
    group = heads // kv_heads
    cos_t, sin_t = cos_ref[...], sin_ref[...]

    def cols(i):
        return pl.ds(pl.multiple_of(i * HEAD_DIM, HEAD_DIM), HEAD_DIM)

    @pl.when(pl.program_id(0) == 0)
    def _():
        sum_ref[...] = jnp.zeros_like(sum_ref)

    def put(c, d):
        dz_ref[:, c] = d.astype(BF16)
        sum_ref[:, c] += jnp.sum(d, axis=0, keepdims=True)

    for g in range(kv_heads):
        kc, vc = cols(heads + g), cols(heads + kv_heads + g)
        dk_ref[...] = jnp.zeros_like(dk_ref)
        dv_ref[...] = jnp.zeros_like(dv_ref)

        @pl.loop(0, group)
        def _(h):
            hc = cols(g * group + h)
            dq = []
            for r in range(0, seq_len, Q_BLOCK):
                n = r + Q_BLOCK
                q, k, v, d = qkv_ref[r:n, hc], qkv_ref[:n, kc], qkv_ref[:n, vc], dctx_ref[r:n, hc]
                p = causal_probs(q, k, r)
                dp = mm(d, v, NT_DIMS)
                dv_ref[:n] += mm(p.astype(BF16), d, TN_DIMS)
                ds = (p * (dp - jnp.sum(p * dp, axis=1, keepdims=True)) * SCALE).astype(BF16)
                dq.append(mm(ds, k, NN_DIMS))
                dk_ref[:n] += mm(ds, q, TN_DIMS)
            dq = jnp.concatenate(dq, axis=0)
            put(hc, dq * cos_t - swap_pairs(dq) * sin_t)

        dk = dk_ref[...]
        put(kc, dk * cos_t - swap_pairs(dk) * sin_t)
        put(vc, dv_ref[...])


def attend(z, cos_t, sin_t, batch, heads, kv_heads):
    tokens, width = z.shape
    seq_len = tokens // batch
    row = lambda b: (b, 0)
    flops = 4 * tokens * seq_len * heads * HEAD_DIM
    return pl.pallas_call(
        functools.partial(attend_kernel, heads, kv_heads),
        grid=(batch,),
        in_specs=[pl.BlockSpec((seq_len, width), row), pl.BlockSpec((seq_len, HEAD_DIM), row), pl.BlockSpec((seq_len, HEAD_DIM), row)],
        out_specs=[pl.BlockSpec((seq_len, width), row), pl.BlockSpec((seq_len, heads * HEAD_DIM), row)],
        out_shape=[jax.ShapeDtypeStruct((tokens, width), BF16), jax.ShapeDtypeStruct((tokens, heads * HEAD_DIM), BF16)],
        compiler_params=pltpu.CompilerParams(dimension_semantics=("arbitrary",), vmem_limit_bytes=48 * 2 ** 20),
        cost_estimate=pl.CostEstimate(flops=3 * flops, bytes_accessed=tokens * width * 8, transcendentals=tokens * seq_len * heads),
        name="attend",
    )(z, cos_t, sin_t)


def attend_back(qkv, d_ctx, cos_t, sin_t, batch, heads, kv_heads):
    tokens, width = qkv.shape
    seq_len = tokens // batch
    row = lambda b: (b, 0)
    flops = 10 * tokens * seq_len * heads * HEAD_DIM
    return pl.pallas_call(
        functools.partial(attend_back_kernel, heads, kv_heads),
        grid=(batch,),
        in_specs=[pl.BlockSpec((seq_len, width), row), pl.BlockSpec((seq_len, heads * HEAD_DIM), row), pl.BlockSpec((seq_len, HEAD_DIM), row), pl.BlockSpec((seq_len, HEAD_DIM), row)],
        out_specs=[pl.BlockSpec((seq_len, width), row), pl.BlockSpec((1, width), lambda b: (0, 0))],
        out_shape=[jax.ShapeDtypeStruct((tokens, width), BF16), jax.ShapeDtypeStruct((1, width), F32)],
        scratch_shapes=[pltpu.VMEM((seq_len, HEAD_DIM), F32), pltpu.VMEM((seq_len, HEAD_DIM), F32)],
        compiler_params=pltpu.CompilerParams(dimension_semantics=("arbitrary",), vmem_limit_bytes=48 * 2 ** 20),
        cost_estimate=pl.CostEstimate(flops=3 * flops, bytes_accessed=tokens * width * 8, transcendentals=tokens * seq_len * heads),
        name="attend_back",
    )(qkv, d_ctx, cos_t, sin_t)


def solution(mesh):
    ax = mesh.axis_names[0]
    n_dev = mesh.shape[ax]
    group = n_dev // 2

    def hop(v, k):
        return lax.ppermute(v, ax, [(i, i ^ k) for i in range(n_dev)])

    def gather_rows(shard):
        return lax.all_gather(shard, ax, axis=0, tiled=True)

    def scatter_rows(full):
        return lax.psum_scatter(full, ax, scatter_dimension=0, tiled=True)

    def spread(v):
        rows, cols = v.shape
        out = jnp.zeros((group * rows, cols), v.dtype)
        parts = [v, hop(v, 1), hop(v, 2)]
        parts.append(hop(parts[2], 1))
        for k in range(group):
            out = lax.dynamic_update_slice(out, parts[k], (k * rows, 0))
        return out

    def layer(hidden, positions, grad_y, attn_gain, w_qkv, b_qkv, w_out, mlp_gain, w_up, w_down):
        batch, seq_len, width = hidden.shape
        tokens = batch * seq_len
        h_loc = w_up.shape[0]
        h_chip = 2 * h_loc
        f_loc = w_down.shape[0]
        pad = -(2 * f_loc) % 256
        f_pad = 2 * f_loc + pad
        q_loc = b_qkv.shape[0]
        me = lax.axis_index(ax)
        rank = lax.rem(me, group)
        side = lax.div(me, group)
        core = lax.rem(me, 2)
        chip = lax.div(me, 2)

        wqkv = gather_rows(w_qkv)
        wout = gather_rows(w_out)
        small = gather_rows(jnp.concatenate([attn_gain, b_qkv, mlp_gain])[None])
        small, w_up, w_down, grad_y = lax.optimization_barrier((small, w_up, w_down, grad_y))
        gain_one = small[:, :h_loc].reshape(1, width).astype(F32)
        bias = small[:, h_loc:h_loc + q_loc].reshape(1, n_dev * q_loc).astype(F32)
        gain_two = small[:, h_loc + q_loc:].reshape(1, width).astype(F32)

        blank = jnp.zeros((h_loc, pad), BF16)
        up_blocks = [w_up[:, j * f_loc:(j + 1) * f_loc] for j in range(2 * n_dev)]
        up_for = jnp.stack([jnp.concatenate([up_blocks[q], up_blocks[group + q], blank, up_blocks[n_dev + q], up_blocks[n_dev + group + q], blank], axis=1) for q in range(group)])
        up_part = [lax.dynamic_index_in_dim(up_for, rank ^ k, 0, keepdims=False) for k in range(group)]
        up_near = [up_part[0]] + [hop(up_part[k], k) for k in (1, 2, 3)]
        up_far = [hop(v, group) for v in up_near]
        w_all = jnp.zeros((width, 2 * f_pad), BF16)
        for k in range(group):
            w_all = lax.dynamic_update_slice(w_all, up_near[k], ((me ^ k) * h_loc, 0))
            w_all = lax.dynamic_update_slice(w_all, up_far[k], ((me ^ group ^ k) * h_loc, 0))
        down_far = hop(w_down, group)
        first = side == 0
        wd_all = jnp.concatenate([jnp.where(first, w_down, down_far), jnp.where(first, down_far, w_down), jnp.zeros((pad, width), BF16)], axis=0)
        dy = grad_y.reshape(tokens, width)
        dy_all = spread(dy)

        hid_wide = hidden.astype(F32).reshape(tokens, width)
        inv_one = norm_scale(hid_wide)
        normed = (hid_wide * inv_one * gain_one).astype(BF16)
        q_width = wout.shape[0]
        kv_width = (wqkv.shape[1] - q_width) // 2
        kv_heads = kv_width // HEAD_DIM
        heads = q_width // HEAD_DIM
        cos_t, sin_t = rope_tables(positions)
        z = mm(normed, wqkv, NN_DIMS) + bias
        qkv, context = attend(z, cos_t, sin_t, batch, heads, kv_heads)
        mid = (hid_wide + mm(context, wout, NN_DIMS)).astype(BF16)
        mid_wide = mid.astype(F32)
        inv_two = norm_scale(mid_wide)
        mlp_in = (mid_wide * inv_two * gain_two).astype(BF16)
        m_all = spread(mlp_in)

        gate_low = mm(m_all, w_all[:, :f_pad], NN_DIMS).astype(BF16)
        lin_low = mm(m_all, w_all[:, f_pad:], NN_DIMS).astype(BF16)
        gate = gate_low.astype(F32)
        act = (gate * jax.nn.sigmoid(gate) * lin_low.astype(F32)).astype(BF16)
        gate_low, lin_low, act = after(gate_low, lin_low, act)

        def block(rows, k, w, dims):
            return mm(rows[k * tokens:(k + 1) * tokens], w, dims)

        half = width // 2

        def down_grad(a, j):
            return mm(a, dy_all[:, j * half:(j + 1) * half], TN_DIMS)

        def send_down(g_full):
            return hop(lax.dynamic_slice(g_full, ((1 - side) * f_loc, 0), (f_loc, half)), group)

        def up_grad(m, d_up, chip_id):
            cols = lax.dynamic_slice(m, (0, chip_id * h_chip), (group * tokens, h_chip))
            return mm(cols, d_up, TN_DIMS)

        y3 = block(act, 3, wd_all, NN_DIMS)
        act, y3 = after(act, y3)
        y3 = hop(y3, 1)
        dwd0 = down_grad(act, 0)
        act, dwd0 = after(act, dwd0)
        dwd0_far = send_down(dwd0)
        y2 = block(act, 2, wd_all, NN_DIMS) + y3
        act, y2 = after(act, y2)
        y2 = hop(y2, 2)
        dwd1 = down_grad(act, 1)
        dwd1, act, gate_low, lin_low = after(dwd1, act, gate_low, lin_low)
        dwd1_far = send_down(dwd1)

        gate, lin = gate_low.astype(F32), lin_low.astype(F32)
        sig = jax.nn.sigmoid(gate)
        d_act = mm(dy_all, wd_all, NT_DIMS)
        d_gate = (d_act * lin * sig * (1.0 + gate * (1.0 - sig))).astype(BF16)
        d_lin = (d_act * gate * sig).astype(BF16)
        d_up = jnp.concatenate([d_gate, d_lin], axis=1)
        dm3 = block(d_up, 3, w_all, NT_DIMS)
        d_gate, d_lin, dm3 = after(d_gate, d_lin, dm3)
        dm3 = hop(dm3, 1)
        d_up = jnp.concatenate([d_gate, d_lin], axis=1)
        dm1 = block(d_up, 1, w_all, NT_DIMS)
        d_gate, d_lin, dm1 = after(d_gate, d_lin, dm1)
        dm1 = hop(dm1, 1)
        d_up = jnp.concatenate([d_gate, d_lin], axis=1)
        dm2 = block(d_up, 2, w_all, NT_DIMS) + dm3
        d_gate, d_lin, dm2 = after(d_gate, d_lin, dm2)
        dm2 = hop(dm2, 2)

        d_up = jnp.concatenate([d_gate, d_lin], axis=1)
        far_a = up_grad(m_all, d_up, chip ^ 3)
        d_gate, d_lin, far_a = after(d_gate, d_lin, far_a)
        far_a = hop(far_a, group)
        d_up = jnp.concatenate([d_gate, d_lin], axis=1)
        far_b = up_grad(m_all, d_up, chip ^ 2)
        d_gate, d_lin, act, far_b = after(d_gate, d_lin, act, far_b)
        far_b = hop(far_b, group)
        y1 = block(act, 1, wd_all, NN_DIMS)
        act, d_gate, d_lin, y1 = after(act, d_gate, d_lin, y1)
        y1 = hop(y1, 1)
        d_up = jnp.concatenate([d_gate, d_lin], axis=1)
        dm0 = block(d_up, 0, w_all, NT_DIMS)
        d_gate, d_lin, dm0, act = after(d_gate, d_lin, dm0, act)
        y0 = block(act, 0, wd_all, NN_DIMS)
        d_gate, d_lin, y0 = after(d_gate, d_lin, y0)
        d_up = jnp.concatenate([d_gate, d_lin], axis=1)
        near_a = up_grad(m_all, d_up, chip ^ 1)
        d_gate, d_lin, near_a = after(d_gate, d_lin, near_a)
        d_up = jnp.concatenate([d_gate, d_lin], axis=1)
        near_b = up_grad(m_all, d_up, chip)
        near_b, dm2 = after(near_b, dm2)

        grad_w_down = jnp.concatenate([lax.dynamic_slice(g, (side * f_loc, 0), (f_loc, half)) + far for g, far in ((dwd0, dwd0_far), (dwd1, dwd1_far))], axis=1)

        def rows_of(c, *parts):
            return sum(lax.dynamic_slice(v, (c * h_loc, 0), (h_loc, 2 * f_pad)) for v in parts)

        pieces = [
            rows_of(core, near_b, far_b),
            hop(rows_of(1 - core, near_b, far_b), 1),
            hop(rows_of(core, near_a, far_a), 2),
            hop(rows_of(1 - core, near_a, far_a), 3),
        ]
        stacked = jnp.stack(pieces)
        by_rank = [lax.dynamic_index_in_dim(stacked, rank ^ q, 0, keepdims=False) for q in range(group)]
        cols = [v[:, lo:lo + f_loc] for lo in (0, f_loc, f_pad, f_pad + f_loc) for v in by_rank]
        grad_w_up = jnp.concatenate(cols, axis=1)

        d_m = dm0 + dm1 + dm2
        grad_mlp_gain = jnp.sum(d_m * mid_wide * inv_two, axis=0)
        scaled_two = d_m * gain_two
        d_mid = dy.astype(F32) + inv_two * (scaled_two - mid_wide * inv_two * inv_two * jnp.mean(scaled_two * mid_wide, axis=-1, keepdims=True))
        d_mid_low = d_mid.astype(BF16)
        grad_w_out = scatter_rows(mm(context, d_mid_low, TN_DIMS))
        d_context = mm(d_mid_low, wout, NT_DIMS).astype(BF16)
        d_proj, grad_b_qkv = attend_back(qkv, d_context, cos_t, sin_t, batch, heads, kv_heads)
        grad_w_qkv = scatter_rows(mm(normed, d_proj, TN_DIMS))
        d_normed = mm(d_proj, wqkv, NT_DIMS)
        y0, y1, y2, mid_late, d_normed = after(y0, y1, y2, mid, d_normed)
        output = (mid_late.astype(F32) + (y0 + y1 + y2)).astype(BF16)
        grad_attn_gain = jnp.sum(d_normed * hid_wide * inv_one, axis=0)
        scaled_one = d_normed * gain_one
        grad_hidden = (d_mid + inv_one * (scaled_one - hid_wide * inv_one * inv_one * jnp.mean(scaled_one * hid_wide, axis=-1, keepdims=True))).astype(BF16)
        small_grads = scatter_rows(jnp.concatenate([grad_attn_gain.reshape(n_dev, h_loc), grad_b_qkv.reshape(n_dev, q_loc), grad_mlp_gain.reshape(n_dev, h_loc)], axis=1)).reshape(-1)
        return (output.reshape(hidden.shape), grad_hidden.reshape(hidden.shape), small_grads[:h_loc], grad_w_qkv, small_grads[h_loc:h_loc + q_loc], grad_w_out, small_grads[h_loc + q_loc:], grad_w_up, grad_w_down)

    row_spec = P(ax)
    return jax.shard_map(layer, mesh=mesh, in_specs=(row_spec,) * 10, out_specs=(row_spec,) * 9, check_vma=False)
```

```python
import functools

import jax
import jax.numpy as jnp
from jax import lax
from jax.experimental import pallas as pl
from jax.experimental.pallas import tpu as pltpu
from jax.sharding import PartitionSpec as P


HEAD_DIM = 128
ROT_DIM = 64
ROPE_BASE = 10000.0
EPS = 1e-5

NT_DIMS = (((1,), (1,)), ((), ()))
TN_DIMS = (((0,), (0,)), ((), ()))
NN_DIMS = (((1,), (0,)), ((), ()))
F32 = jnp.float32
BF16 = jnp.bfloat16
SCALE = HEAD_DIM ** -0.5
MASKED = -1e30
Q_BLOCK = 128
T_BLOCK = 512
F_BLOCK = 256
LANES = 128
LOG2_E = 1.4426950408889634


def mm(a, b, dims):
    return lax.dot_general(a, b, dims, preferred_element_type=F32)


def after(*vals):
    return lax.optimization_barrier(vals)


def norm_scale(rows_in):
    return lax.rsqrt(jnp.mean(rows_in * rows_in, axis=-1, keepdims=True) + EPS)


def rope_tables(positions):
    lane = jnp.arange(HEAD_DIM, dtype=jnp.int32)
    pair = (lane - lane % 2).astype(F32)
    inv_freq = 1.0 / (ROPE_BASE ** (pair / ROT_DIM))
    angles = positions.astype(F32).reshape(-1, 1) * inv_freq
    turned = lane < ROT_DIM
    sines = jnp.sin(angles)
    return jnp.where(turned, jnp.cos(angles), 1.0), jnp.where(turned, jnp.where(lane % 2 == 0, -sines, sines), 0.0)


def swap_pairs(v):
    lane = lax.broadcasted_iota(jnp.int32, v.shape, 1)
    return jnp.where(lane % 2 == 0, pltpu.roll(v, HEAD_DIM - 1, 1), pltpu.roll(v, 1, 1))


def causal_probs(q, k):
    n = q.shape[0]
    full = k.shape[0] - n
    s = mm(q, k, NT_DIMS)
    row = lax.broadcasted_iota(jnp.int32, (n, n), 0)
    col = lax.broadcasted_iota(jnp.int32, (n, n), 1)
    own = jnp.where(row >= col, s[:, full:], MASKED)
    s = own if full == 0 else jnp.concatenate([s[:, :full], own], axis=1)
    e = jnp.exp2((s - jnp.max(s, axis=1, keepdims=True)) * (SCALE * LOG2_E))
    return e * (1.0 / jnp.sum(e, axis=1, keepdims=True))


def attend_kernel(heads, kv_heads, z_ref, cos_ref, sin_ref, qkv_ref, ctx_ref):
    seq_len = z_ref.shape[0]
    group = heads // kv_heads
    cos_t, sin_t = cos_ref[...], sin_ref[...]

    def cols(i):
        return pl.ds(pl.multiple_of(i * HEAD_DIM, HEAD_DIM), HEAD_DIM)

    for g in range(kv_heads):
        kc, vc = cols(heads + g), cols(heads + kv_heads + g)
        zk = z_ref[:, kc]
        qkv_ref[:, kc] = (zk * cos_t + swap_pairs(zk) * sin_t).astype(BF16)
        qkv_ref[:, vc] = z_ref[:, vc].astype(BF16)

        @pl.loop(0, group)
        def _(h):
            hc = cols(g * group + h)
            zq = z_ref[:, hc]
            q = (zq * cos_t + swap_pairs(zq) * sin_t).astype(BF16)
            qkv_ref[:, hc] = q
            for r in range(0, seq_len, Q_BLOCK):
                n = r + Q_BLOCK
                p = causal_probs(q[r:n], qkv_ref[:n, kc]).astype(BF16)
                ctx_ref[r:n, hc] = mm(p, qkv_ref[:n, vc], NN_DIMS).astype(BF16)


def attend_back_kernel(heads, kv_heads, qkv_ref, dctx_ref, cos_ref, sin_ref, dz_ref, sum_ref, dk_ref, dv_ref):
    seq_len = qkv_ref.shape[0]
    group = heads // kv_heads
    cos_t, sin_t = cos_ref[...], sin_ref[...]

    def cols(i):
        return pl.ds(pl.multiple_of(i * HEAD_DIM, HEAD_DIM), HEAD_DIM)

    @pl.when(pl.program_id(0) == 0)
    def _():
        sum_ref[...] = jnp.zeros_like(sum_ref)

    def put(c, d):
        dz_ref[:, c] = d.astype(BF16)
        sum_ref[:, c] += jnp.sum(d, axis=0, keepdims=True)

    for g in range(kv_heads):
        kc, vc = cols(heads + g), cols(heads + kv_heads + g)
        dk_ref[...] = jnp.zeros_like(dk_ref)
        dv_ref[...] = jnp.zeros_like(dv_ref)

        @pl.loop(0, group)
        def _(h):
            hc = cols(g * group + h)
            dq = []
            for r in range(0, seq_len, Q_BLOCK):
                n = r + Q_BLOCK
                q, k, v, d = qkv_ref[r:n, hc], qkv_ref[:n, kc], qkv_ref[:n, vc], dctx_ref[r:n, hc]
                p = causal_probs(q, k)
                dp = mm(d, v, NT_DIMS)
                dv_ref[:n] += mm(p.astype(BF16), d, TN_DIMS)
                ds = (p * (dp - jnp.sum(p * dp, axis=1, keepdims=True)) * SCALE).astype(BF16)
                dq.append(mm(ds, k, NN_DIMS))
                dk_ref[:n] += mm(ds, q, TN_DIMS)
            dq = jnp.concatenate(dq, axis=0)
            put(hc, dq * cos_t - swap_pairs(dq) * sin_t)

        dk = dk_ref[...]
        put(kc, dk * cos_t - swap_pairs(dk) * sin_t)
        put(vc, dv_ref[...])


def attend(z, cos_t, sin_t, batch, heads, kv_heads):
    tokens, width = z.shape
    seq_len = tokens // batch
    row = lambda b: (b, 0)
    flops = 4 * tokens * seq_len * heads * HEAD_DIM
    return pl.pallas_call(
        functools.partial(attend_kernel, heads, kv_heads),
        grid=(batch,),
        in_specs=[pl.BlockSpec((seq_len, width), row), pl.BlockSpec((seq_len, HEAD_DIM), row), pl.BlockSpec((seq_len, HEAD_DIM), row)],
        out_specs=[pl.BlockSpec((seq_len, width), row), pl.BlockSpec((seq_len, heads * HEAD_DIM), row)],
        out_shape=[jax.ShapeDtypeStruct((tokens, width), BF16), jax.ShapeDtypeStruct((tokens, heads * HEAD_DIM), BF16)],
        compiler_params=pltpu.CompilerParams(dimension_semantics=("arbitrary",), vmem_limit_bytes=48 * 2 ** 20),
        cost_estimate=pl.CostEstimate(flops=3 * flops, bytes_accessed=tokens * width * 8, transcendentals=tokens * seq_len * heads),
        name="attend",
    )(z, cos_t, sin_t)


def attend_back(qkv, d_ctx, cos_t, sin_t, batch, heads, kv_heads):
    tokens, width = qkv.shape
    seq_len = tokens // batch
    row = lambda b: (b, 0)
    flops = 10 * tokens * seq_len * heads * HEAD_DIM
    return pl.pallas_call(
        functools.partial(attend_back_kernel, heads, kv_heads),
        grid=(batch,),
        in_specs=[pl.BlockSpec((seq_len, width), row), pl.BlockSpec((seq_len, heads * HEAD_DIM), row), pl.BlockSpec((seq_len, HEAD_DIM), row), pl.BlockSpec((seq_len, HEAD_DIM), row)],
        out_specs=[pl.BlockSpec((seq_len, width), row), pl.BlockSpec((1, width), lambda b: (0, 0))],
        out_shape=[jax.ShapeDtypeStruct((tokens, width), BF16), jax.ShapeDtypeStruct((1, width), F32)],
        scratch_shapes=[pltpu.VMEM((seq_len, HEAD_DIM), F32), pltpu.VMEM((seq_len, HEAD_DIM), F32)],
        compiler_params=pltpu.CompilerParams(dimension_semantics=("arbitrary",), vmem_limit_bytes=48 * 2 ** 20),
        cost_estimate=pl.CostEstimate(flops=3 * flops, bytes_accessed=tokens * width * 8, transcendentals=tokens * seq_len * heads),
        name="attend_back",
    )(qkv, d_ctx, cos_t, sin_t)


def up_kernel(m_ref, w_ref, g_ref, l_ref, a_ref):
    f_pad = g_ref.shape[1]
    for j in range(0, f_pad, F_BLOCK):
        c = slice(j, j + F_BLOCK)
        gate_low = mm(m_ref[...], w_ref[:, c], NN_DIMS).astype(BF16)
        lin_low = mm(m_ref[...], w_ref[:, f_pad + j:f_pad + j + F_BLOCK], NN_DIMS).astype(BF16)
        g_ref[:, c] = gate_low
        l_ref[:, c] = lin_low
        gate = gate_low.astype(F32)
        a_ref[:, c] = (gate * (1.0 / (1.0 + jnp.exp(-gate))) * lin_low.astype(F32)).astype(BF16)


def up_act(m, w):
    tokens, width = m.shape
    f_pad = w.shape[1] // 2
    row = lambda i: (i, 0)
    return pl.pallas_call(
        up_kernel,
        grid=(tokens // T_BLOCK,),
        in_specs=[pl.BlockSpec((T_BLOCK, width), row), pl.BlockSpec(w.shape, lambda i: (0, 0), pipeline_mode=pl.Buffered(1))],
        out_specs=[pl.BlockSpec((T_BLOCK, f_pad), row)] * 3,
        out_shape=[jax.ShapeDtypeStruct((tokens, f_pad), BF16)] * 3,
        compiler_params=pltpu.CompilerParams(dimension_semantics=("arbitrary",), vmem_limit_bytes=60 * 2 ** 20),
        cost_estimate=pl.CostEstimate(flops=2 * tokens * width * 2 * f_pad, bytes_accessed=2 * (m.size + w.size + 3 * tokens * f_pad), transcendentals=2 * tokens * f_pad),
        name="up_act",
    )(m, w)


def up_back_kernel(dy_ref, wd_ref, g_ref, l_ref, out_ref):
    f_pad = g_ref.shape[1]
    for j in range(0, f_pad, F_BLOCK):
        c = slice(j, j + F_BLOCK)
        d_act = mm(dy_ref[...], wd_ref[c, :], NT_DIMS)
        gate, lin = g_ref[:, c].astype(F32), l_ref[:, c].astype(F32)
        sig = 1.0 / (1.0 + jnp.exp(-gate))
        gate_sig = gate * sig
        out_ref[:, c] = (d_act * (lin * (sig + gate_sig * (1.0 - sig)))).astype(BF16)
        out_ref[:, f_pad + j:f_pad + j + F_BLOCK] = (d_act * gate_sig).astype(BF16)


def up_back(dy, wd, gate_low, lin_low):
    tokens, width = dy.shape
    f_pad = wd.shape[0]
    row = lambda i: (i, 0)
    return pl.pallas_call(
        up_back_kernel,
        grid=(tokens // T_BLOCK,),
        in_specs=[pl.BlockSpec((T_BLOCK, width), row), pl.BlockSpec(wd.shape, lambda i: (0, 0), pipeline_mode=pl.Buffered(1)), pl.BlockSpec((T_BLOCK, f_pad), row), pl.BlockSpec((T_BLOCK, f_pad), row)],
        out_specs=pl.BlockSpec((T_BLOCK, 2 * f_pad), row),
        out_shape=jax.ShapeDtypeStruct((tokens, 2 * f_pad), BF16),
        compiler_params=pltpu.CompilerParams(dimension_semantics=("arbitrary",), vmem_limit_bytes=60 * 2 ** 20),
        cost_estimate=pl.CostEstimate(flops=2 * tokens * width * f_pad, bytes_accessed=2 * (dy.size + wd.size + 4 * tokens * f_pad), transcendentals=2 * tokens * f_pad),
        name="up_back",
    )(dy, wd, gate_low, lin_low)


def shifted_tile(load, start, limit):
    tile, phase = start // LANES, start % LANES
    near = load(min(max(tile, 0), limit - 1))
    if phase == 0:
        return near
    after_it = load(min(max(tile + 1, 0), limit - 1))
    lane = lax.broadcasted_iota(jnp.int32, near.shape, 1)
    return jnp.where(lane < LANES - phase, pltpu.roll(near, LANES - phase, 1), pltpu.roll(after_it, LANES - phase, 1))


def gathered_tile(lo, segments, shape):
    lane = lax.broadcasted_iota(jnp.int32, shape, 1)
    out = jnp.zeros(shape, F32)
    for first, length, load, there, limit in segments:
        a, b = max(first, lo), min(first + length, lo + LANES)
        if a < b:
            part = shifted_tile(load, there + lo - first, limit)
            inside = (lane >= a - lo) & (lane < b - lo)
            out = part if b - a == LANES else jnp.where(inside, part, out)
    return out


def split_kernel(group, f_loc, rank_ref, w_ref, *out_refs):
    rows, cols = w_ref.shape
    f_pad = out_refs[0].shape[1] // 2

    def load(t):
        return w_ref[:, t * LANES:(t + 1) * LANES].astype(F32)

    for r in range(group):
        @pl.when(rank_ref[0] == r)
        def _():
            for q in range(group):
                for h in range(2):
                    segments = [(s * f_loc, f_loc, load, ((2 * h + s) * group + q) * f_loc, cols // LANES) for s in range(2)]
                    for lo in range(0, f_pad, LANES):
                        out_refs[r ^ q][:, h * f_pad + lo:h * f_pad + lo + LANES] = gathered_tile(lo, segments, (rows, LANES)).astype(BF16)


def split_up(w_up, rank, group, f_loc, f_pad):
    rows, cols = w_up.shape
    step = 32
    return pl.pallas_call(
        functools.partial(split_kernel, group, f_loc),
        grid_spec=pltpu.PrefetchScalarGridSpec(
            num_scalar_prefetch=1,
            grid=(rows // step,),
            in_specs=[pl.BlockSpec((step, cols), lambda i, r: (i, 0))],
            out_specs=[pl.BlockSpec((step, 2 * f_pad), lambda i, r: (i, 0))] * group,
        ),
        out_shape=[jax.ShapeDtypeStruct((rows, 2 * f_pad), BF16)] * group,
        compiler_params=pltpu.CompilerParams(dimension_semantics=("arbitrary",)),
        cost_estimate=pl.CostEstimate(flops=20 * rows * cols, bytes_accessed=4 * rows * cols, transcendentals=0),
        name="split_up",
    )(rank.reshape(1), w_up)


def join_kernel(group, f_loc, rank_ref, *refs):
    parts, out_ref = refs[:group], refs[group]
    rows, cols = out_ref.shape
    f_pad = parts[0].shape[1] // 2
    half = cols // 2
    for r in range(group):
        @pl.when(rank_ref[0] == r)
        def _():
            def loader(ref):
                return lambda t: ref[:, t * LANES:(t + 1) * LANES]

            for h in range(2):
                segments = [(b * f_loc, f_loc, loader(parts[r ^ (b % group)]), h * f_pad + b // group * f_loc, 2 * f_pad // LANES) for b in range(2 * group)]
                for lo in range(0, half, LANES):
                    out_ref[:, h * half + lo:h * half + lo + LANES] = gathered_tile(lo, segments, (rows, LANES))


def join_up(parts, rank, group, f_loc):
    rows, width = parts[0].shape
    cols = 4 * group * f_loc
    step = 32
    return pl.pallas_call(
        functools.partial(join_kernel, group, f_loc),
        grid_spec=pltpu.PrefetchScalarGridSpec(
            num_scalar_prefetch=1,
            grid=(rows // step,),
            in_specs=[pl.BlockSpec((step, width), lambda i, r: (i, 0))] * group,
            out_specs=pl.BlockSpec((step, cols), lambda i, r: (i, 0)),
        ),
        out_shape=jax.ShapeDtypeStruct((rows, cols), F32),
        compiler_params=pltpu.CompilerParams(dimension_semantics=("arbitrary",)),
        cost_estimate=pl.CostEstimate(flops=20 * rows * cols, bytes_accessed=8 * rows * cols, transcendentals=0),
        name="join_up",
    )(rank.reshape(1), *parts)


def solution(mesh):
    ax = mesh.axis_names[0]
    n_dev = mesh.shape[ax]
    group = n_dev // 2

    def hop(v, k):
        return lax.ppermute(v, ax, [(i, i ^ k) for i in range(n_dev)])

    def gather_rows(shard):
        return lax.all_gather(shard, ax, axis=0, tiled=True)

    def scatter_rows(full):
        return lax.psum_scatter(full, ax, scatter_dimension=0, tiled=True)

    def spread(v):
        v2 = hop(v, 2)
        return [v, hop(v, 1), v2, hop(v2, 1)]

    def joined(parts):
        rows, cols = parts[0].shape
        out = jnp.zeros((group * rows, cols), parts[0].dtype)
        for k, v in enumerate(parts):
            out = lax.dynamic_update_slice(out, v, (k * rows, 0))
        return out

    def layer(hidden, positions, grad_y, attn_gain, w_qkv, b_qkv, w_out, mlp_gain, w_up, w_down):
        batch, seq_len, width = hidden.shape
        tokens = batch * seq_len
        h_loc = w_up.shape[0]
        h_chip = 2 * h_loc
        f_loc = w_down.shape[0]
        pad = -(2 * f_loc) % 256
        f_pad = 2 * f_loc + pad
        q_loc = b_qkv.shape[0]
        me = lax.axis_index(ax)
        rank = lax.rem(me, group)
        side = lax.div(me, group)
        core = lax.rem(me, 2)
        chip = lax.div(me, 2)

        wqkv = gather_rows(w_qkv)
        wout = gather_rows(w_out)
        small = jnp.concatenate([attn_gain, b_qkv, mlp_gain])[None]
        for k in (1, 2, group):
            far = hop(small, k)
            small = jnp.where((me & k) == 0, jnp.concatenate([small, far]), jnp.concatenate([far, small]))
        up_part = split_up(w_up, rank, group, f_loc, f_pad)
        small, *up_part, w_down, grad_y = after(small, *up_part, w_down, grad_y)
        gain_one = small[:, :h_loc].reshape(1, width).astype(F32)
        bias = small[:, h_loc:h_loc + q_loc].reshape(1, n_dev * q_loc).astype(F32)
        gain_two = small[:, h_loc + q_loc:].reshape(1, width).astype(F32)

        up_near = [up_part[0]] + [hop(up_part[k], k) for k in (1, 2, 3)]
        up_far = [hop(v, group) for v in up_near]
        down_far = hop(w_down, group)
        dy = grad_y.reshape(tokens, width)
        dy_parts = [dy, hop(dy, 1), hop(dy, 2)]

        hid_wide = hidden.astype(F32).reshape(tokens, width)
        inv_one = norm_scale(hid_wide)
        normed = (hid_wide * inv_one * gain_one).astype(BF16)
        q_width = wout.shape[0]
        kv_width = (wqkv.shape[1] - q_width) // 2
        kv_heads = kv_width // HEAD_DIM
        heads = q_width // HEAD_DIM
        cos_t, sin_t = rope_tables(positions)
        z = mm(normed, wqkv, NN_DIMS) + bias
        qkv, context = attend(z, cos_t, sin_t, batch, heads, kv_heads)
        mid = (hid_wide + mm(context, wout, NN_DIMS)).astype(BF16)
        mid_wide = mid.astype(F32)
        inv_two = norm_scale(mid_wide)
        mlp_in = (mid_wide * inv_two * gain_two).astype(BF16)
        m_parts = spread(mlp_in)

        w_all = jnp.zeros((width, 2 * f_pad), BF16)
        for k in range(group):
            w_all = lax.dynamic_update_slice(w_all, up_near[k], ((me ^ k) * h_loc, 0))
        m_all = joined(m_parts[:2])
        dy_all = joined(dy_parts[:2])
        wd_all = lax.dynamic_update_slice(jnp.zeros((f_pad, width), BF16), w_down, (side * f_loc, 0))
        m_all, dy_all, w_all, wd_all, up_far[2] = after(m_all, dy_all, w_all, wd_all, up_far[2])
        for k in range(group):
            w_all = lax.dynamic_update_slice(w_all, up_far[k], ((me ^ group ^ k) * h_loc, 0))
        for k in (2, 3):
            m_all = lax.dynamic_update_slice(m_all, m_parts[k], (k * tokens, 0))

        gate_low, lin_low, act = up_act(m_all, w_all)
        act, dy_far, down_far, dy_all = after(act, dy_parts[2], down_far, dy_all)
        dy_parts[2:] = [dy_far, hop(dy_far, 1)]
        for k in (2, 3):
            dy_all = lax.dynamic_update_slice(dy_all, dy_parts[k], (k * tokens, 0))
        wd_all = lax.dynamic_update_slice(wd_all, down_far, ((1 - side) * f_loc, 0))

        def block(rows, k, w, dims):
            return mm(rows[k * tokens:(k + 1) * tokens], w, dims)

        half = width // 2

        def down_grad(a, j):
            return mm(a, dy_all[:, j * half:(j + 1) * half], TN_DIMS)

        def send_down(g_full):
            return hop(lax.dynamic_slice(g_full, ((1 - side) * f_loc, 0), (f_loc, half)), group)

        def up_grad(m, d_up, chip_id):
            cols = lax.dynamic_slice(m, (0, chip_id * h_chip), (group * tokens, h_chip))
            return mm(cols, d_up, TN_DIMS)

        y3 = block(act, 3, wd_all, NN_DIMS)
        act, y3 = after(act, y3)
        y3 = hop(y3, 1)
        dwd0 = down_grad(act, 0)
        act, dwd0 = after(act, dwd0)
        dwd0_far = send_down(dwd0)
        y2 = block(act, 2, wd_all, NN_DIMS) + y3
        act, y2 = after(act, y2)
        y2 = hop(y2, 2)
        dwd1 = down_grad(act, 1)
        dwd1, act, gate_low, lin_low = after(dwd1, act, gate_low, lin_low)
        dwd1_far = send_down(dwd1)

        d_up = up_back(dy_all, wd_all, gate_low, lin_low)
        dm3 = block(d_up, 3, w_all, NT_DIMS)
        d_up, dm3 = after(d_up, dm3)
        dm3 = hop(dm3, 1)
        dm1 = block(d_up, 1, w_all, NT_DIMS)
        d_up, dm1 = after(d_up, dm1)
        dm1 = hop(dm1, 1)
        dm2 = block(d_up, 2, w_all, NT_DIMS) + dm3
        d_up, dm2 = after(d_up, dm2)
        dm2 = hop(dm2, 2)

        far_a = up_grad(m_all, d_up, chip ^ 3)
        d_up, far_a = after(d_up, far_a)
        far_a = hop(far_a, group)
        far_b = up_grad(m_all, d_up, chip ^ 2)
        d_up, act, far_b = after(d_up, act, far_b)
        far_b = hop(far_b, group)
        y1 = block(act, 1, wd_all, NN_DIMS)
        act, d_up, y1 = after(act, d_up, y1)
        y1 = hop(y1, 1)
        dm0 = block(d_up, 0, w_all, NT_DIMS)
        d_up, dm0, act = after(d_up, dm0, act)
        y0 = block(act, 0, wd_all, NN_DIMS)
        d_up, y0 = after(d_up, y0)
        near_a = up_grad(m_all, d_up, chip ^ 1)
        d_up, near_a, dm2 = after(d_up, near_a, dm2)

        grad_w_down = jnp.concatenate([lax.dynamic_slice(g, (side * f_loc, 0), (f_loc, half)) + far for g, far in ((dwd0, dwd0_far), (dwd1, dwd1_far))], axis=1)

        def rows_of(c, *parts):
            return sum(lax.dynamic_slice(v, (c * h_loc, 0), (h_loc, 2 * f_pad)) for v in parts)

        piece2 = hop(rows_of(core, near_a, far_a), 2)
        piece3 = hop(rows_of(1 - core, near_a, far_a), 3)

        d_m = dm0 + dm1 + dm2
        grad_mlp_gain = jnp.sum(d_m * mid_wide * inv_two, axis=0)
        scaled_two = d_m * gain_two
        d_mid = dy.astype(F32) + inv_two * (scaled_two - mid_wide * inv_two * inv_two * jnp.mean(scaled_two * mid_wide, axis=-1, keepdims=True))
        d_mid_low = d_mid.astype(BF16)
        grad_w_out = scatter_rows(mm(context, d_mid_low, TN_DIMS))
        d_context = mm(d_mid_low, wout, NT_DIMS).astype(BF16)
        d_proj, grad_b_qkv = attend_back(qkv, d_context, cos_t, sin_t, batch, heads, kv_heads)
        grad_w_qkv = mm(normed, d_proj, TN_DIMS)
        grad_w_qkv, d_proj = after(grad_w_qkv, d_proj)
        grad_w_qkv = scatter_rows(grad_w_qkv)
        d_normed = mm(d_proj, wqkv, NT_DIMS)
        d_normed, d_up = after(d_normed, d_up)
        near_b = up_grad(m_all, d_up, chip)
        near_b, d_normed = after(near_b, d_normed)
        piece0 = rows_of(core, near_b, far_b)
        piece1 = hop(rows_of(1 - core, near_b, far_b), 1)
        grad_w_up = join_up([piece0, piece1, piece2, piece3], rank, group, f_loc)
        y0, y1, y2, mid_late, d_normed = after(y0, y1, y2, mid, d_normed)
        output = (mid_late.astype(F32) + (y0 + y1 + y2)).astype(BF16)
        grad_attn_gain = jnp.sum(d_normed * hid_wide * inv_one, axis=0)
        scaled_one = d_normed * gain_one
        grad_hidden = (d_mid + inv_one * (scaled_one - hid_wide * inv_one * inv_one * jnp.mean(scaled_one * hid_wide, axis=-1, keepdims=True))).astype(BF16)
        small_grads = scatter_rows(jnp.concatenate([grad_attn_gain.reshape(n_dev, h_loc), grad_b_qkv.reshape(n_dev, q_loc), grad_mlp_gain.reshape(n_dev, h_loc)], axis=1)).reshape(-1)
        return (output.reshape(hidden.shape), grad_hidden.reshape(hidden.shape), small_grads[:h_loc], grad_w_qkv, small_grads[h_loc:h_loc + q_loc], grad_w_out, small_grads[h_loc + q_loc:], grad_w_up, grad_w_down)

    row_spec = P(ax)
    return jax.shard_map(layer, mesh=mesh, in_specs=(row_spec,) * 10, out_specs=(row_spec,) * 9, check_vma=False)
```

```python
import functools

import jax
import jax.numpy as jnp
from jax import lax
from jax.experimental import pallas as pl
from jax.experimental.pallas import tpu as pltpu
from jax.sharding import PartitionSpec as P


HEAD_DIM = 128
ROT_DIM = 64
ROPE_BASE = 10000.0
EPS = 1e-5

NT_DIMS = (((1,), (1,)), ((), ()))
TN_DIMS = (((0,), (0,)), ((), ()))
NN_DIMS = (((1,), (0,)), ((), ()))
F32 = jnp.float32
BF16 = jnp.bfloat16
SCALE = HEAD_DIM ** -0.5
MASKED = -1e30
Q_BLOCK = 128
S_BLOCK = 64
T_BLOCK = 768
F_BLOCK = 256
LANES = 128
LOG2_E = 1.4426950408889634


def mm(a, b, dims):
    return lax.dot_general(a, b, dims, preferred_element_type=F32)


def after(*vals):
    return lax.optimization_barrier(vals)


def norm_scale(rows_in):
    return lax.rsqrt(jnp.mean(rows_in * rows_in, axis=-1, keepdims=True) + EPS)


def rope_tables(positions):
    lane = jnp.arange(HEAD_DIM, dtype=jnp.int32)
    pair = (lane - lane % 2).astype(F32)
    inv_freq = 1.0 / (ROPE_BASE ** (pair / ROT_DIM))
    angles = positions.astype(F32).reshape(-1, 1) * inv_freq
    turned = lane < ROT_DIM
    sines = jnp.sin(angles)
    return jnp.where(turned, jnp.cos(angles), 1.0), jnp.where(turned, jnp.where(lane % 2 == 0, -sines, sines), 0.0)


def swap_pairs(v):
    lane = lax.broadcasted_iota(jnp.int32, v.shape, 1)
    return jnp.where(lane % 2 == 0, pltpu.roll(v, HEAD_DIM - 1, 1), pltpu.roll(v, 1, 1))


def attend_kernel(heads, kv_heads, z_ref, cos_ref, sin_ref, qkv_ref, ctx_ref, s_ref, p_ref):
    seq_len = z_ref.shape[0]
    group = heads // kv_heads
    cos_t, sin_t = cos_ref[...], sin_ref[...]

    def cols(i):
        return pl.ds(pl.multiple_of(i * HEAD_DIM, HEAD_DIM), HEAD_DIM)

    @pl.loop(0, heads + kv_heads)
    def _(i):
        zh = z_ref[:, cols(i)]
        qkv_ref[:, cols(i)] = (zh * cos_t + swap_pairs(zh) * sin_t).astype(BF16)

    qkv_ref[:, (heads + kv_heads) * HEAD_DIM:] = z_ref[:, (heads + kv_heads) * HEAD_DIM:].astype(BF16)

    @pl.loop(0, kv_heads)
    def _(g):
        kc, vc = cols(heads + g), cols(heads + kv_heads + g)
        for r in range(0, seq_len, Q_BLOCK):
            n = r + Q_BLOCK
            q = jnp.concatenate([qkv_ref[r:n, cols(g * group + h)] for h in range(group)], axis=0)
            s_ref[:, :n] = mm(q, qkv_ref[:n, kc], NT_DIMS)

            @pl.loop(0, group * Q_BLOCK // S_BLOCK, unroll=2)
            def _(c):
                rows = pl.ds(pl.multiple_of(c * S_BLOCK, S_BLOCK), S_BLOCK)
                s = s_ref[rows, :n]
                row = lax.broadcasted_iota(jnp.int32, (S_BLOCK, Q_BLOCK), 0) + lax.rem(c * S_BLOCK, Q_BLOCK)
                col = lax.broadcasted_iota(jnp.int32, (S_BLOCK, Q_BLOCK), 1)
                own = jnp.where(row >= col, s[:, r:], MASKED)
                s = own if r == 0 else jnp.concatenate([s[:, :r], own], axis=1)
                e = jnp.exp2((s - jnp.max(s, axis=1, keepdims=True)) * (SCALE * LOG2_E))
                p_ref[rows, :n] = (e * (1.0 / jnp.sum(e, axis=1, keepdims=True))).astype(BF16)

            ctx = mm(p_ref[:, :n], qkv_ref[:n, vc], NN_DIMS).astype(BF16)
            for h in range(group):
                ctx_ref[r:n, cols(g * group + h)] = ctx[h * Q_BLOCK:(h + 1) * Q_BLOCK]


def attend_back_kernel(heads, kv_heads, qkv_ref, dctx_ref, cos_ref, sin_ref, dz_ref, sum_ref, dk_ref, dv_ref, s_ref, dp_ref, p_ref, ds_ref):
    seq_len = qkv_ref.shape[0]
    group = heads // kv_heads

    def cols(i):
        return pl.ds(pl.multiple_of(i * HEAD_DIM, HEAD_DIM), HEAD_DIM)

    @pl.when(pl.program_id(0) == 0)
    def _():
        sum_ref[...] = jnp.zeros_like(sum_ref)

    def put(rows, c, d):
        dz_ref[rows, c] = d.astype(BF16)
        sum_ref[:, c] += jnp.sum(d, axis=0, keepdims=True)

    def turned_back(rows, d):
        return d * cos_ref[rows, :] - swap_pairs(d) * sin_ref[rows, :]

    @pl.loop(0, kv_heads)
    def _(g):
        kc, vc = cols(heads + g), cols(heads + kv_heads + g)
        dk_ref[...] = jnp.zeros_like(dk_ref)
        dv_ref[...] = jnp.zeros_like(dv_ref)
        for r in range(0, seq_len, Q_BLOCK):
            n = r + Q_BLOCK
            q = jnp.concatenate([qkv_ref[r:n, cols(g * group + h)] for h in range(group)], axis=0)
            d = jnp.concatenate([dctx_ref[r:n, cols(g * group + h)] for h in range(group)], axis=0)
            s_ref[:n] = mm(qkv_ref[:n, kc], q, NT_DIMS)
            dp_ref[:n] = mm(qkv_ref[:n, vc], d, NT_DIMS)

            @pl.loop(0, group)
            def _(h):
                c = cols(h)
                s, dp = s_ref[:n, c], dp_ref[:n, c]
                row = lax.broadcasted_iota(jnp.int32, (Q_BLOCK, Q_BLOCK), 0)
                col = lax.broadcasted_iota(jnp.int32, (Q_BLOCK, Q_BLOCK), 1)
                own = jnp.where(row <= col, s[r:], MASKED)
                s = own if r == 0 else jnp.concatenate([s[:r], own], axis=0)
                e = jnp.exp2((s - jnp.max(s, axis=0, keepdims=True)) * (SCALE * LOG2_E))
                p = e * (1.0 / jnp.sum(e, axis=0, keepdims=True))
                p_ref[:n, c] = p.astype(BF16)
                ds_ref[:n, c] = (p * (dp - jnp.sum(p * dp, axis=0, keepdims=True)) * SCALE).astype(BF16)

            dv_ref[:n] += mm(p_ref[:n], d, NN_DIMS)
            dk_ref[:n] += mm(ds_ref[:n], q, NN_DIMS)
            dq = mm(qkv_ref[:n, kc], ds_ref[:n], TN_DIMS)
            for h in range(group):
                rows = slice(r, n)
                put(rows, cols(g * group + h), turned_back(rows, jnp.transpose(dq[:, h * Q_BLOCK:(h + 1) * Q_BLOCK])))

        rows = slice(0, seq_len)
        put(rows, kc, turned_back(rows, dk_ref[...]))
        put(rows, vc, dv_ref[...])


def attend(z, cos_t, sin_t, batch, heads, kv_heads):
    tokens, width = z.shape
    seq_len = tokens // batch
    row = lambda b: (b, 0)
    flops = 4 * tokens * seq_len * heads * HEAD_DIM
    return pl.pallas_call(
        functools.partial(attend_kernel, heads, kv_heads),
        grid=(batch,),
        in_specs=[pl.BlockSpec((seq_len, width), row), pl.BlockSpec((seq_len, HEAD_DIM), row), pl.BlockSpec((seq_len, HEAD_DIM), row)],
        out_specs=[pl.BlockSpec((seq_len, width), row), pl.BlockSpec((seq_len, heads * HEAD_DIM), row)],
        out_shape=[jax.ShapeDtypeStruct((tokens, width), BF16), jax.ShapeDtypeStruct((tokens, heads * HEAD_DIM), BF16)],
        scratch_shapes=[pltpu.VMEM((heads // kv_heads * Q_BLOCK, seq_len), F32), pltpu.VMEM((heads // kv_heads * Q_BLOCK, seq_len), BF16)],
        compiler_params=pltpu.CompilerParams(dimension_semantics=("arbitrary",), vmem_limit_bytes=48 * 2 ** 20),
        cost_estimate=pl.CostEstimate(flops=3 * flops, bytes_accessed=tokens * width * 8, transcendentals=tokens * seq_len * heads),
        name="attend",
    )(z, cos_t, sin_t)


def attend_back(qkv, d_ctx, cos_t, sin_t, batch, heads, kv_heads):
    tokens, width = qkv.shape
    seq_len = tokens // batch
    row = lambda b: (b, 0)
    flops = 10 * tokens * seq_len * heads * HEAD_DIM
    return pl.pallas_call(
        functools.partial(attend_back_kernel, heads, kv_heads),
        grid=(batch,),
        in_specs=[pl.BlockSpec((seq_len, width), row), pl.BlockSpec((seq_len, heads * HEAD_DIM), row), pl.BlockSpec((seq_len, HEAD_DIM), row), pl.BlockSpec((seq_len, HEAD_DIM), row)],
        out_specs=[pl.BlockSpec((seq_len, width), row), pl.BlockSpec((1, width), lambda b: (0, 0))],
        out_shape=[jax.ShapeDtypeStruct((tokens, width), BF16), jax.ShapeDtypeStruct((1, width), F32)],
        scratch_shapes=[pltpu.VMEM((seq_len, HEAD_DIM), F32)] * 2 + [pltpu.VMEM((seq_len, heads // kv_heads * Q_BLOCK), F32)] * 2 + [pltpu.VMEM((seq_len, heads // kv_heads * Q_BLOCK), BF16)] * 2,
        compiler_params=pltpu.CompilerParams(dimension_semantics=("arbitrary",), vmem_limit_bytes=48 * 2 ** 20),
        cost_estimate=pl.CostEstimate(flops=3 * flops, bytes_accessed=tokens * width * 8, transcendentals=tokens * seq_len * heads),
        name="attend_back",
    )(qkv, d_ctx, cos_t, sin_t)


def up_kernel(m_ref, w_ref, g_ref, l_ref, a_ref):
    f_pad = g_ref.shape[1]
    for j in range(0, f_pad, F_BLOCK):
        c = slice(j, j + F_BLOCK)
        gate_low = mm(m_ref[...], w_ref[:, c], NN_DIMS).astype(BF16)
        lin_low = mm(m_ref[...], w_ref[:, f_pad + j:f_pad + j + F_BLOCK], NN_DIMS).astype(BF16)
        g_ref[:, c] = gate_low
        l_ref[:, c] = lin_low
        gate = gate_low.astype(F32)
        a_ref[:, c] = (gate * (1.0 / (1.0 + jnp.exp(-gate))) * lin_low.astype(F32)).astype(BF16)


def up_act(m, w):
    tokens, width = m.shape
    f_pad = w.shape[1] // 2
    row = lambda i: (i, 0)
    return pl.pallas_call(
        up_kernel,
        grid=(tokens // T_BLOCK,),
        in_specs=[pl.BlockSpec((T_BLOCK, width), row), pl.BlockSpec(w.shape, lambda i: (0, 0), pipeline_mode=pl.Buffered(1))],
        out_specs=[pl.BlockSpec((T_BLOCK, f_pad), row)] * 3,
        out_shape=[jax.ShapeDtypeStruct((tokens, f_pad), BF16)] * 3,
        compiler_params=pltpu.CompilerParams(dimension_semantics=("arbitrary",), vmem_limit_bytes=60 * 2 ** 20),
        cost_estimate=pl.CostEstimate(flops=2 * tokens * width * 2 * f_pad, bytes_accessed=2 * (m.size + w.size + 3 * tokens * f_pad), transcendentals=2 * tokens * f_pad),
        name="up_act",
    )(m, w)


def up_back_kernel(dy_ref, wd_ref, g_ref, l_ref, out_ref):
    f_pad = g_ref.shape[1]
    for j in range(0, f_pad, F_BLOCK):
        c = slice(j, j + F_BLOCK)
        d_act = mm(dy_ref[...], wd_ref[c, :], NT_DIMS)
        gate, lin = g_ref[:, c].astype(F32), l_ref[:, c].astype(F32)
        sig = 1.0 / (1.0 + jnp.exp(-gate))
        gate_sig = gate * sig
        out_ref[:, c] = (d_act * (lin * (sig + gate_sig * (1.0 - sig)))).astype(BF16)
        out_ref[:, f_pad + j:f_pad + j + F_BLOCK] = (d_act * gate_sig).astype(BF16)


def up_back(dy, wd, gate_low, lin_low):
    tokens, width = dy.shape
    f_pad = wd.shape[0]
    row = lambda i: (i, 0)
    return pl.pallas_call(
        up_back_kernel,
        grid=(tokens // T_BLOCK,),
        in_specs=[pl.BlockSpec((T_BLOCK, width), row), pl.BlockSpec(wd.shape, lambda i: (0, 0), pipeline_mode=pl.Buffered(1)), pl.BlockSpec((T_BLOCK, f_pad), row), pl.BlockSpec((T_BLOCK, f_pad), row)],
        out_specs=pl.BlockSpec((T_BLOCK, 2 * f_pad), row),
        out_shape=jax.ShapeDtypeStruct((tokens, 2 * f_pad), BF16),
        compiler_params=pltpu.CompilerParams(dimension_semantics=("arbitrary",), vmem_limit_bytes=60 * 2 ** 20),
        cost_estimate=pl.CostEstimate(flops=2 * tokens * width * f_pad, bytes_accessed=2 * (dy.size + wd.size + 4 * tokens * f_pad), transcendentals=2 * tokens * f_pad),
        name="up_back",
    )(dy, wd, gate_low, lin_low)


def shifted_tile(load, start, limit):
    tile, phase = start // LANES, start % LANES
    near = load(min(max(tile, 0), limit - 1))
    if phase == 0:
        return near
    after_it = load(min(max(tile + 1, 0), limit - 1))
    lane = lax.broadcasted_iota(jnp.int32, near.shape, 1)
    return jnp.where(lane < LANES - phase, pltpu.roll(near, LANES - phase, 1), pltpu.roll(after_it, LANES - phase, 1))


def gathered_tile(lo, segments, shape):
    lane = lax.broadcasted_iota(jnp.int32, shape, 1)
    out = jnp.zeros(shape, F32)
    for first, length, load, there, limit in segments:
        a, b = max(first, lo), min(first + length, lo + LANES)
        if a < b:
            part = shifted_tile(load, there + lo - first, limit)
            inside = (lane >= a - lo) & (lane < b - lo)
            out = part if b - a == LANES else jnp.where(inside, part, out)
    return out


def split_kernel(group, f_loc, rank_ref, w_ref, *out_refs):
    rows, cols = w_ref.shape
    f_pad = out_refs[0].shape[1] // 2

    def load(t):
        return w_ref[:, t * LANES:(t + 1) * LANES].astype(F32)

    for r in range(group):
        @pl.when(rank_ref[0] == r)
        def _():
            for q in range(group):
                for h in range(2):
                    segments = [(s * f_loc, f_loc, load, ((2 * h + s) * group + q) * f_loc, cols // LANES) for s in range(2)]
                    for lo in range(0, f_pad, LANES):
                        out_refs[r ^ q][:, h * f_pad + lo:h * f_pad + lo + LANES] = gathered_tile(lo, segments, (rows, LANES)).astype(BF16)


def split_up(w_up, rank, group, f_loc, f_pad):
    rows, cols = w_up.shape
    step = 32
    return pl.pallas_call(
        functools.partial(split_kernel, group, f_loc),
        grid_spec=pltpu.PrefetchScalarGridSpec(
            num_scalar_prefetch=1,
            grid=(rows // step,),
            in_specs=[pl.BlockSpec((step, cols), lambda i, r: (i, 0))],
            out_specs=[pl.BlockSpec((step, 2 * f_pad), lambda i, r: (i, 0))] * group,
        ),
        out_shape=[jax.ShapeDtypeStruct((rows, 2 * f_pad), BF16)] * group,
        compiler_params=pltpu.CompilerParams(dimension_semantics=("arbitrary",)),
        cost_estimate=pl.CostEstimate(flops=20 * rows * cols, bytes_accessed=4 * rows * cols, transcendentals=0),
        name="split_up",
    )(rank.reshape(1), w_up)


def join_kernel(group, f_loc, rank_ref, *refs):
    parts, out_ref = refs[:group], refs[group]
    rows, cols = out_ref.shape
    f_pad = parts[0].shape[1] // 2
    half = cols // 2
    for r in range(group):
        @pl.when(rank_ref[0] == r)
        def _():
            def loader(ref):
                return lambda t: ref[:, t * LANES:(t + 1) * LANES]

            for h in range(2):
                segments = [(b * f_loc, f_loc, loader(parts[r ^ (b % group)]), h * f_pad + b // group * f_loc, 2 * f_pad // LANES) for b in range(2 * group)]
                for lo in range(0, half, LANES):
                    out_ref[:, h * half + lo:h * half + lo + LANES] = gathered_tile(lo, segments, (rows, LANES))


def join_up(parts, rank, group, f_loc):
    rows, width = parts[0].shape
    cols = 4 * group * f_loc
    step = 32
    return pl.pallas_call(
        functools.partial(join_kernel, group, f_loc),
        grid_spec=pltpu.PrefetchScalarGridSpec(
            num_scalar_prefetch=1,
            grid=(rows // step,),
            in_specs=[pl.BlockSpec((step, width), lambda i, r: (i, 0))] * group,
            out_specs=pl.BlockSpec((step, cols), lambda i, r: (i, 0)),
        ),
        out_shape=jax.ShapeDtypeStruct((rows, cols), F32),
        compiler_params=pltpu.CompilerParams(dimension_semantics=("arbitrary",)),
        cost_estimate=pl.CostEstimate(flops=20 * rows * cols, bytes_accessed=8 * rows * cols, transcendentals=0),
        name="join_up",
    )(rank.reshape(1), *parts)


def solution(mesh):
    ax = mesh.axis_names[0]
    n_dev = mesh.shape[ax]
    group = n_dev // 2

    def hop(v, k):
        return lax.ppermute(v, ax, [(i, i ^ k) for i in range(n_dev)])

    def gather_rows(shard):
        return lax.all_gather(shard, ax, axis=0, tiled=True)

    def scatter_rows(full):
        return lax.psum_scatter(full, ax, scatter_dimension=0, tiled=True)

    def joined(parts):
        rows, cols = parts[0].shape
        out = jnp.zeros((group * rows, cols), parts[0].dtype)
        for k, v in enumerate(parts):
            out = lax.dynamic_update_slice(out, v, (k * rows, 0))
        return out

    def layer(hidden, positions, grad_y, attn_gain, w_qkv, b_qkv, w_out, mlp_gain, w_up, w_down):
        batch, seq_len, width = hidden.shape
        tokens = batch * seq_len
        h_loc = w_up.shape[0]
        h_chip = 2 * h_loc
        f_loc = w_down.shape[0]
        pad = -(2 * f_loc) % 256
        f_pad = 2 * f_loc + pad
        q_loc = b_qkv.shape[0]
        me = lax.axis_index(ax)
        rank = lax.rem(me, group)
        side = lax.div(me, group)
        core = lax.rem(me, 2)
        chip = lax.div(me, 2)

        wqkv = gather_rows(w_qkv)
        wout = gather_rows(w_out)
        small = jnp.concatenate([attn_gain, b_qkv, mlp_gain])[None]
        for k in (1, 2, group):
            far = hop(small, k)
            small = jnp.where((me & k) == 0, jnp.concatenate([small, far]), jnp.concatenate([far, small]))
        up_part = split_up(w_up, rank, group, f_loc, f_pad)
        small, *up_part, w_down, grad_y = after(small, *up_part, w_down, grad_y)
        gain_one = small[:, :h_loc].reshape(1, width).astype(F32)
        bias = small[:, h_loc:h_loc + q_loc].reshape(1, n_dev * q_loc).astype(F32)
        gain_two = small[:, h_loc + q_loc:].reshape(1, width).astype(F32)

        wqkv, up_part[2], up_part[3] = after(wqkv, up_part[2], up_part[3])
        up_near = [up_part[0]] + [hop(up_part[k], k) for k in (1, 2, 3)]
        up_far = [hop(v, group) for v in up_near]
        down_far = hop(w_down, group)
        dy = grad_y.reshape(tokens, width)
        dy_parts = [dy, hop(dy, 1), hop(dy, 2)]

        hid_wide = hidden.astype(F32).reshape(tokens, width)
        inv_one = norm_scale(hid_wide)
        normed = (hid_wide * inv_one * gain_one).astype(BF16)
        q_width = wout.shape[0]
        kv_width = (wqkv.shape[1] - q_width) // 2
        kv_heads = kv_width // HEAD_DIM
        heads = q_width // HEAD_DIM
        cos_t, sin_t = rope_tables(positions)
        z = mm(normed, wqkv, NN_DIMS) + bias
        qkv, context = attend(z, cos_t, sin_t, batch, heads, kv_heads)
        mid = (hid_wide + mm(context, wout, NN_DIMS)).astype(BF16)
        mid_wide = mid.astype(F32)
        inv_two = norm_scale(mid_wide)
        mlp_in = (mid_wide * inv_two * gain_two).astype(BF16)
        w_all = jnp.zeros((width, 2 * f_pad), BF16)
        for k in range(group):
            w_all = lax.dynamic_update_slice(w_all, up_near[k], ((me ^ k) * h_loc, 0))
        for k in (0, 1, 2):
            w_all = lax.dynamic_update_slice(w_all, up_far[k], ((me ^ group ^ k) * h_loc, 0))
        m_all = joined([mlp_in, hop(mlp_in, 1)])
        dy_all = joined(dy_parts[:2])
        wd_all = lax.dynamic_update_slice(jnp.zeros((f_pad, width), BF16), w_down, (side * f_loc, 0))
        m_far = hop(mlp_in, 2)
        m_all, dy_all, w_all, wd_all, m_far = after(m_all, dy_all, w_all, wd_all, m_far)
        w_all = lax.dynamic_update_slice(w_all, up_far[3], ((me ^ group ^ 3) * h_loc, 0))
        m_all = lax.dynamic_update_slice(m_all, m_far, (2 * tokens, 0))
        m_all = lax.dynamic_update_slice(m_all, hop(m_far, 1), (3 * tokens, 0))

        gate_low, lin_low, act = up_act(m_all, w_all)
        act, dy_far, down_far, dy_all = after(act, dy_parts[2], down_far, dy_all)
        dy_parts[2:] = [dy_far, hop(dy_far, 1)]
        for k in (2, 3):
            dy_all = lax.dynamic_update_slice(dy_all, dy_parts[k], (k * tokens, 0))
        wd_all = lax.dynamic_update_slice(wd_all, down_far, ((1 - side) * f_loc, 0))

        def block(rows, k, w, dims):
            return mm(rows[k * tokens:(k + 1) * tokens], w, dims)

        half = width // 2

        def down_grad(a, j):
            return mm(a, dy_all[:, j * half:(j + 1) * half], TN_DIMS)

        def send_down(g_full):
            return hop(lax.dynamic_slice(g_full, ((1 - side) * f_loc, 0), (f_loc, half)), group)

        def up_grad(m, d_up, chip_id):
            cols = lax.dynamic_slice(m, (0, chip_id * h_chip), (group * tokens, h_chip))
            return mm(cols, d_up, TN_DIMS)

        y3 = block(act, 3, wd_all, NN_DIMS)
        act, y3 = after(act, y3)
        y3 = hop(y3, 1)
        dwd0 = down_grad(act, 0)
        act, dwd0 = after(act, dwd0)
        dwd0_far = send_down(dwd0)
        y2 = block(act, 2, wd_all, NN_DIMS) + y3
        act, y2 = after(act, y2)
        y2 = hop(y2, 2)
        dwd1 = down_grad(act, 1)
        dwd1, act, gate_low, lin_low = after(dwd1, act, gate_low, lin_low)
        dwd1_far = send_down(dwd1)

        d_up = up_back(dy_all, wd_all, gate_low, lin_low)
        dm3 = block(d_up, 3, w_all, NT_DIMS)
        d_up, dm3 = after(d_up, dm3)
        dm3 = hop(dm3, 1)
        dm2 = block(d_up, 2, w_all, NT_DIMS)
        d_up, dm2 = after(d_up, dm2)
        d_up, dm2 = after(d_up, dm2 + dm3)
        dm2 = hop(dm2, 2)

        far_a = up_grad(m_all, d_up, chip ^ 3)
        d_up, far_a = after(d_up, far_a)
        far_a = hop(far_a, group)
        far_b = up_grad(m_all, d_up, chip ^ 2)
        d_up, act, far_b = after(d_up, act, far_b)
        far_b = hop(far_b, group)
        y1 = block(act, 1, wd_all, NN_DIMS)
        act, d_up, y1 = after(act, d_up, y1)
        y1 = hop(y1, 1)
        dm1 = block(d_up, 1, w_all, NT_DIMS)
        d_up, dm1 = after(d_up, dm1)
        dm1 = hop(dm1, 1)
        dm0 = block(d_up, 0, w_all, NT_DIMS)
        d_up, dm0, act = after(d_up, dm0, act)
        y0 = block(act, 0, wd_all, NN_DIMS)
        d_up, y0 = after(d_up, y0)
        near_a = up_grad(m_all, d_up, chip ^ 1)
        d_up, near_a, dm2 = after(d_up, near_a, dm2)

        grad_w_down = jnp.concatenate([lax.dynamic_slice(g, (side * f_loc, 0), (f_loc, half)) + far for g, far in ((dwd0, dwd0_far), (dwd1, dwd1_far))], axis=1)

        def rows_of(c, *parts):
            return sum(lax.dynamic_slice(v, (c * h_loc, 0), (h_loc, 2 * f_pad)) for v in parts)

        piece2 = hop(rows_of(core, near_a, far_a), 2)
        piece3 = hop(rows_of(1 - core, near_a, far_a), 3)

        d_m = dm0 + dm1 + dm2
        grad_mlp_gain = jnp.sum(d_m * mid_wide * inv_two, axis=0)
        scaled_two = d_m * gain_two
        d_mid = dy.astype(F32) + inv_two * (scaled_two - mid_wide * inv_two * inv_two * jnp.mean(scaled_two * mid_wide, axis=-1, keepdims=True))
        d_mid_low = d_mid.astype(BF16)
        grad_w_out = scatter_rows(mm(context, d_mid_low, TN_DIMS))
        d_context = mm(d_mid_low, wout, NT_DIMS).astype(BF16)
        d_proj, grad_b_qkv = attend_back(qkv, d_context, cos_t, sin_t, batch, heads, kv_heads)
        grad_w_qkv = mm(normed, d_proj, TN_DIMS)
        grad_w_qkv, d_proj = after(grad_w_qkv, d_proj)
        grad_w_qkv = scatter_rows(grad_w_qkv)
        d_normed = mm(d_proj, wqkv, NT_DIMS)
        d_normed, d_up = after(d_normed, d_up)
        near_b = up_grad(m_all, d_up, chip)
        near_b, d_normed = after(near_b, d_normed)
        grad_attn_gain = jnp.sum(d_normed * hid_wide * inv_one, axis=0)
        small_grads = jnp.concatenate([grad_attn_gain.reshape(n_dev, h_loc), grad_b_qkv.reshape(n_dev, q_loc), grad_mlp_gain.reshape(n_dev, h_loc)], axis=1)
        for k in (1, 2, group):
            pair = small_grads.reshape(n_dev // 2, 2, -1) if k == 1 else small_grads.reshape(-1, 2, h_loc + q_loc + h_loc)
            mine = lax.div(me, k) % 2
            small_grads = lax.dynamic_index_in_dim(pair, mine, 1, keepdims=False) + hop(lax.dynamic_index_in_dim(pair, 1 - mine, 1, keepdims=False), k)
        small_grads = small_grads.reshape(-1)
        scaled_one = d_normed * gain_one
        grad_hidden = (d_mid + inv_one * (scaled_one - hid_wide * inv_one * inv_one * jnp.mean(scaled_one * hid_wide, axis=-1, keepdims=True))).astype(BF16)
        y0, y1, y2, mid_late, grad_hidden = after(y0, y1, y2, mid, grad_hidden)
        output = (mid_late.astype(F32) + (y0 + y1 + y2)).astype(BF16)
        far_b, output, grad_hidden, grad_w_down = after(far_b, output, grad_hidden, grad_w_down)
        piece0 = rows_of(core, near_b, far_b)
        piece1 = hop(rows_of(1 - core, near_b, far_b), 1)
        grad_w_up = join_up([piece0, piece1, piece2, piece3], rank, group, f_loc)
        return (output.reshape(hidden.shape), grad_hidden.reshape(hidden.shape), small_grads[:h_loc], grad_w_qkv, small_grads[h_loc:h_loc + q_loc], grad_w_out, small_grads[h_loc + q_loc:], grad_w_up, grad_w_down)

    row_spec = P(ax)
    return jax.shard_map(layer, mesh=mesh, in_specs=(row_spec,) * 10, out_specs=(row_spec,) * 9, check_vma=False)
```

```python
import functools

import jax
import jax.numpy as jnp
from jax import lax
from jax.experimental import pallas as pl
from jax.experimental.pallas import tpu as pltpu
from jax.sharding import PartitionSpec as P


HEAD_DIM = 128
ROT_DIM = 64
ROPE_BASE = 10000.0
EPS = 1e-5

NT_DIMS = (((1,), (1,)), ((), ()))
TN_DIMS = (((0,), (0,)), ((), ()))
NN_DIMS = (((1,), (0,)), ((), ()))
F32 = jnp.float32
BF16 = jnp.bfloat16
SCALE = HEAD_DIM ** -0.5
MASKED = -1e30
Q_BLOCK = 128
S_BLOCK = 64
T_BLOCK = 768
F_BLOCK = 256
LANES = 128
LOG2_E = 1.4426950408889634


def mm(a, b, dims):
    return lax.dot_general(a, b, dims, preferred_element_type=F32)


def after(*vals):
    return lax.optimization_barrier(vals)


def norm_scale(rows_in):
    return lax.rsqrt(jnp.mean(rows_in * rows_in, axis=-1, keepdims=True) + EPS)


def rope_tables(positions):
    lane = jnp.arange(HEAD_DIM, dtype=jnp.int32)
    pair = (lane - lane % 2).astype(F32)
    inv_freq = 1.0 / (ROPE_BASE ** (pair / ROT_DIM))
    angles = positions.astype(F32).reshape(-1, 1) * inv_freq
    turned = lane < ROT_DIM
    sines = jnp.sin(angles)
    return jnp.where(turned, jnp.cos(angles), 1.0), jnp.where(turned, jnp.where(lane % 2 == 0, -sines, sines), 0.0)


def swap_pairs(v):
    lane = lax.broadcasted_iota(jnp.int32, v.shape, 1)
    return jnp.where(lane % 2 == 0, pltpu.roll(v, HEAD_DIM - 1, 1), pltpu.roll(v, 1, 1))


def attend_kernel(heads, kv_heads, z_ref, cos_ref, sin_ref, qkv_ref, ctx_ref, *bufs):
    s_refs, p_refs = bufs[:2], bufs[2:]
    seq_len = z_ref.shape[0]
    group = heads // kv_heads
    cos_t, sin_t = cos_ref[...], sin_ref[...]

    def cols(i):
        return pl.ds(pl.multiple_of(i * HEAD_DIM, HEAD_DIM), HEAD_DIM)

    @pl.loop(0, heads + kv_heads, unroll=3)
    def _(i):
        zh = z_ref[:, cols(i)]
        qkv_ref[:, cols(i)] = (zh * cos_t + swap_pairs(zh) * sin_t).astype(BF16)

    qkv_ref[:, (heads + kv_heads) * HEAD_DIM:] = z_ref[:, (heads + kv_heads) * HEAD_DIM:].astype(BF16)

    @pl.loop(0, kv_heads)
    def _(g):
        kc, vc = cols(heads + g), cols(heads + kv_heads + g)
        for r in range(0, seq_len, Q_BLOCK):
            n = r + Q_BLOCK
            q = jnp.concatenate([qkv_ref[r:n, cols(g * group + h)] for h in range(group)], axis=0)
            s_ref, p_ref = s_refs[r // Q_BLOCK % 2], p_refs[r // Q_BLOCK % 2]
            s_ref[:, :n] = mm(q, qkv_ref[:n, kc], NT_DIMS)

            @pl.loop(0, group * Q_BLOCK // S_BLOCK, unroll=True)
            def _(c):
                rows = pl.ds(pl.multiple_of(c * S_BLOCK, S_BLOCK), S_BLOCK)
                s = s_ref[rows, :n]
                row = lax.broadcasted_iota(jnp.int32, (S_BLOCK, Q_BLOCK), 0) + lax.rem(c * S_BLOCK, Q_BLOCK)
                col = lax.broadcasted_iota(jnp.int32, (S_BLOCK, Q_BLOCK), 1)
                own = jnp.where(row >= col, s[:, r:], MASKED)
                s = own if r == 0 else jnp.concatenate([s[:, :r], own], axis=1)
                e = jnp.exp2((s - jnp.max(s, axis=1, keepdims=True)) * (SCALE * LOG2_E))
                p_ref[rows, :n] = (e * (1.0 / jnp.sum(e, axis=1, keepdims=True))).astype(BF16)

            ctx = mm(p_ref[:, :n], qkv_ref[:n, vc], NN_DIMS).astype(BF16)
            for h in range(group):
                ctx_ref[r:n, cols(g * group + h)] = ctx[h * Q_BLOCK:(h + 1) * Q_BLOCK]


def attend_back_kernel(heads, kv_heads, qkv_ref, dctx_ref, cos_ref, sin_ref, dz_ref, sum_ref, dk_ref, dv_ref, s_ref, dp_ref, p_ref, ds_ref):
    seq_len = qkv_ref.shape[0]
    group = heads // kv_heads

    def cols(i):
        return pl.ds(pl.multiple_of(i * HEAD_DIM, HEAD_DIM), HEAD_DIM)

    @pl.when(pl.program_id(0) == 0)
    def _():
        sum_ref[...] = jnp.zeros_like(sum_ref)

    def put(rows, c, d):
        dz_ref[rows, c] = d.astype(BF16)
        sum_ref[:, c] += jnp.sum(d, axis=0, keepdims=True)

    def turned_back(rows, d):
        return d * cos_ref[rows, :] - swap_pairs(d) * sin_ref[rows, :]

    @pl.loop(0, kv_heads)
    def _(g):
        kc, vc = cols(heads + g), cols(heads + kv_heads + g)
        dk_ref[...] = jnp.zeros_like(dk_ref)
        dv_ref[...] = jnp.zeros_like(dv_ref)
        for r in range(0, seq_len, Q_BLOCK):
            n = r + Q_BLOCK
            q = jnp.concatenate([qkv_ref[r:n, cols(g * group + h)] for h in range(group)], axis=0)
            d = jnp.concatenate([dctx_ref[r:n, cols(g * group + h)] for h in range(group)], axis=0)
            s_ref[:n] = mm(qkv_ref[:n, kc], q, NT_DIMS)
            dp_ref[:n] = mm(qkv_ref[:n, vc], d, NT_DIMS)

            @pl.loop(0, group, unroll=True)
            def _(h):
                c = cols(h)
                s, dp = s_ref[:n, c], dp_ref[:n, c]
                row = lax.broadcasted_iota(jnp.int32, (Q_BLOCK, Q_BLOCK), 0)
                col = lax.broadcasted_iota(jnp.int32, (Q_BLOCK, Q_BLOCK), 1)
                own = jnp.where(row <= col, s[r:], MASKED)
                s = own if r == 0 else jnp.concatenate([s[:r], own], axis=0)
                e = jnp.exp2((s - jnp.max(s, axis=0, keepdims=True)) * (SCALE * LOG2_E))
                p = e * (1.0 / jnp.sum(e, axis=0, keepdims=True))
                p_ref[:n, c] = p.astype(BF16)
                ds_ref[:n, c] = (p * (dp - jnp.sum(p * dp, axis=0, keepdims=True)) * SCALE).astype(BF16)

            dv_ref[:n] += mm(p_ref[:n], d, NN_DIMS)
            dk_ref[:n] += mm(ds_ref[:n], q, NN_DIMS)
            dq = mm(qkv_ref[:n, kc], ds_ref[:n], TN_DIMS)
            for h in range(group):
                rows = slice(r, n)
                put(rows, cols(g * group + h), turned_back(rows, jnp.transpose(dq[:, h * Q_BLOCK:(h + 1) * Q_BLOCK])))

        rows = slice(0, seq_len)
        put(rows, kc, turned_back(rows, dk_ref[...]))
        put(rows, vc, dv_ref[...])


def attend(z, cos_t, sin_t, batch, heads, kv_heads):
    tokens, width = z.shape
    seq_len = tokens // batch
    row = lambda b: (b, 0)
    flops = 4 * tokens * seq_len * heads * HEAD_DIM
    return pl.pallas_call(
        functools.partial(attend_kernel, heads, kv_heads),
        grid=(batch,),
        in_specs=[pl.BlockSpec((seq_len, width), row), pl.BlockSpec((seq_len, HEAD_DIM), row), pl.BlockSpec((seq_len, HEAD_DIM), row)],
        out_specs=[pl.BlockSpec((seq_len, width), row), pl.BlockSpec((seq_len, heads * HEAD_DIM), row)],
        out_shape=[jax.ShapeDtypeStruct((tokens, width), BF16), jax.ShapeDtypeStruct((tokens, heads * HEAD_DIM), BF16)],
        scratch_shapes=[pltpu.VMEM((heads // kv_heads * Q_BLOCK, seq_len), t) for t in (F32, F32, BF16, BF16)],
        compiler_params=pltpu.CompilerParams(dimension_semantics=("arbitrary",), vmem_limit_bytes=48 * 2 ** 20),
        cost_estimate=pl.CostEstimate(flops=3 * flops, bytes_accessed=tokens * width * 8, transcendentals=tokens * seq_len * heads),
        name="attend",
    )(z, cos_t, sin_t)


def attend_back(qkv, d_ctx, cos_t, sin_t, batch, heads, kv_heads):
    tokens, width = qkv.shape
    seq_len = tokens // batch
    row = lambda b: (b, 0)
    flops = 10 * tokens * seq_len * heads * HEAD_DIM
    return pl.pallas_call(
        functools.partial(attend_back_kernel, heads, kv_heads),
        grid=(batch,),
        in_specs=[pl.BlockSpec((seq_len, width), row), pl.BlockSpec((seq_len, heads * HEAD_DIM), row), pl.BlockSpec((seq_len, HEAD_DIM), row), pl.BlockSpec((seq_len, HEAD_DIM), row)],
        out_specs=[pl.BlockSpec((seq_len, width), row), pl.BlockSpec((1, width), lambda b: (0, 0))],
        out_shape=[jax.ShapeDtypeStruct((tokens, width), BF16), jax.ShapeDtypeStruct((1, width), F32)],
        scratch_shapes=[pltpu.VMEM((seq_len, HEAD_DIM), F32)] * 2 + [pltpu.VMEM((seq_len, heads // kv_heads * Q_BLOCK), F32)] * 2 + [pltpu.VMEM((seq_len, heads // kv_heads * Q_BLOCK), BF16)] * 2,
        compiler_params=pltpu.CompilerParams(dimension_semantics=("arbitrary",), vmem_limit_bytes=48 * 2 ** 20),
        cost_estimate=pl.CostEstimate(flops=3 * flops, bytes_accessed=tokens * width * 8, transcendentals=tokens * seq_len * heads),
        name="attend_back",
    )(qkv, d_ctx, cos_t, sin_t)


def up_kernel(m_ref, w_ref, g_ref, l_ref, a_ref):
    f_pad = g_ref.shape[1]
    for j in range(0, f_pad, F_BLOCK):
        c = slice(j, j + F_BLOCK)
        gate_low = mm(m_ref[...], w_ref[:, c], NN_DIMS).astype(BF16)
        lin_low = mm(m_ref[...], w_ref[:, f_pad + j:f_pad + j + F_BLOCK], NN_DIMS).astype(BF16)
        g_ref[:, c] = gate_low
        l_ref[:, c] = lin_low
        gate = gate_low.astype(F32)
        a_ref[:, c] = (gate * (1.0 / (1.0 + jnp.exp(-gate))) * lin_low.astype(F32)).astype(BF16)


def up_act(m, w):
    tokens, width = m.shape
    f_pad = w.shape[1] // 2
    row = lambda i: (i, 0)
    return pl.pallas_call(
        up_kernel,
        grid=(tokens // T_BLOCK,),
        in_specs=[pl.BlockSpec((T_BLOCK, width), row), pl.BlockSpec(w.shape, lambda i: (0, 0), pipeline_mode=pl.Buffered(1))],
        out_specs=[pl.BlockSpec((T_BLOCK, f_pad), row)] * 3,
        out_shape=[jax.ShapeDtypeStruct((tokens, f_pad), BF16)] * 3,
        compiler_params=pltpu.CompilerParams(dimension_semantics=("arbitrary",), vmem_limit_bytes=60 * 2 ** 20),
        cost_estimate=pl.CostEstimate(flops=2 * tokens * width * 2 * f_pad, bytes_accessed=2 * (m.size + w.size + 3 * tokens * f_pad), transcendentals=2 * tokens * f_pad),
        name="up_act",
    )(m, w)


def up_back_kernel(dy_ref, wd_ref, g_ref, l_ref, out_ref):
    f_pad = g_ref.shape[1]
    for j in range(0, f_pad, F_BLOCK):
        c = slice(j, j + F_BLOCK)
        d_act = mm(dy_ref[...], wd_ref[c, :], NT_DIMS)
        gate, lin = g_ref[:, c].astype(F32), l_ref[:, c].astype(F32)
        sig = 1.0 / (1.0 + jnp.exp(-gate))
        gate_sig = gate * sig
        out_ref[:, c] = (d_act * (lin * (sig + gate_sig * (1.0 - sig)))).astype(BF16)
        out_ref[:, f_pad + j:f_pad + j + F_BLOCK] = (d_act * gate_sig).astype(BF16)


def up_back(dy, wd, gate_low, lin_low):
    tokens, width = dy.shape
    f_pad = wd.shape[0]
    row = lambda i: (i, 0)
    return pl.pallas_call(
        up_back_kernel,
        grid=(tokens // T_BLOCK,),
        in_specs=[pl.BlockSpec((T_BLOCK, width), row), pl.BlockSpec(wd.shape, lambda i: (0, 0), pipeline_mode=pl.Buffered(1)), pl.BlockSpec((T_BLOCK, f_pad), row), pl.BlockSpec((T_BLOCK, f_pad), row)],
        out_specs=pl.BlockSpec((T_BLOCK, 2 * f_pad), row),
        out_shape=jax.ShapeDtypeStruct((tokens, 2 * f_pad), BF16),
        compiler_params=pltpu.CompilerParams(dimension_semantics=("arbitrary",), vmem_limit_bytes=60 * 2 ** 20),
        cost_estimate=pl.CostEstimate(flops=2 * tokens * width * f_pad, bytes_accessed=2 * (dy.size + wd.size + 4 * tokens * f_pad), transcendentals=2 * tokens * f_pad),
        name="up_back",
    )(dy, wd, gate_low, lin_low)


def shifted_tile(load, start, limit):
    tile, phase = start // LANES, start % LANES
    near = load(min(max(tile, 0), limit - 1))
    if phase == 0:
        return near
    after_it = load(min(max(tile + 1, 0), limit - 1))
    lane = lax.broadcasted_iota(jnp.int32, near.shape, 1)
    return jnp.where(lane < LANES - phase, pltpu.roll(near, LANES - phase, 1), pltpu.roll(after_it, LANES - phase, 1))


def gathered_tile(lo, segments, shape):
    lane = lax.broadcasted_iota(jnp.int32, shape, 1)
    out = jnp.zeros(shape, F32)
    for first, length, load, there, limit in segments:
        a, b = max(first, lo), min(first + length, lo + LANES)
        if a < b:
            part = shifted_tile(load, there + lo - first, limit)
            inside = (lane >= a - lo) & (lane < b - lo)
            out = part if b - a == LANES else jnp.where(inside, part, out)
    return out


def split_kernel(group, f_loc, rank_ref, w_ref, *out_refs):
    rows, cols = w_ref.shape
    f_pad = out_refs[0].shape[1] // 2

    def load(t):
        return w_ref[:, t * LANES:(t + 1) * LANES].astype(F32)

    for r in range(group):
        @pl.when(rank_ref[0] == r)
        def _():
            for q in range(group):
                for h in range(2):
                    segments = [(s * f_pad // 2, f_loc, load, ((2 * h + s) * group + q) * f_loc, cols // LANES) for s in range(2)]
                    for lo in range(0, f_pad, LANES):
                        out_refs[r ^ q][:, h * f_pad + lo:h * f_pad + lo + LANES] = gathered_tile(lo, segments, (rows, LANES)).astype(BF16)


def split_up(w_up, rank, group, f_loc, f_pad):
    rows, cols = w_up.shape
    step = 32
    return pl.pallas_call(
        functools.partial(split_kernel, group, f_loc),
        grid_spec=pltpu.PrefetchScalarGridSpec(
            num_scalar_prefetch=1,
            grid=(rows // step,),
            in_specs=[pl.BlockSpec((step, cols), lambda i, r: (i, 0))],
            out_specs=[pl.BlockSpec((step, 2 * f_pad), lambda i, r: (i, 0))] * group,
        ),
        out_shape=[jax.ShapeDtypeStruct((rows, 2 * f_pad), BF16)] * group,
        compiler_params=pltpu.CompilerParams(dimension_semantics=("arbitrary",)),
        cost_estimate=pl.CostEstimate(flops=20 * rows * cols, bytes_accessed=4 * rows * cols, transcendentals=0),
        name="split_up",
    )(rank.reshape(1), w_up)


def join_kernel(group, f_loc, rank_ref, *refs):
    parts, out_ref = refs[:group], refs[group]
    rows, cols = out_ref.shape
    f_pad = parts[0].shape[1] // 2
    half = cols // 2
    for r in range(group):
        @pl.when(rank_ref[0] == r)
        def _():
            def loader(ref):
                return lambda t: ref[:, t * LANES:(t + 1) * LANES]

            for h in range(2):
                segments = [(b * f_loc, f_loc, loader(parts[r ^ (b % group)]), h * f_pad + b // group * f_pad // 2, 2 * f_pad // LANES) for b in range(2 * group)]
                for lo in range(0, half, LANES):
                    out_ref[:, h * half + lo:h * half + lo + LANES] = gathered_tile(lo, segments, (rows, LANES))


def join_up(parts, rank, group, f_loc):
    rows, width = parts[0].shape
    cols = 4 * group * f_loc
    step = 32
    return pl.pallas_call(
        functools.partial(join_kernel, group, f_loc),
        grid_spec=pltpu.PrefetchScalarGridSpec(
            num_scalar_prefetch=1,
            grid=(rows // step,),
            in_specs=[pl.BlockSpec((step, width), lambda i, r: (i, 0))] * group,
            out_specs=pl.BlockSpec((step, cols), lambda i, r: (i, 0)),
        ),
        out_shape=jax.ShapeDtypeStruct((rows, cols), F32),
        compiler_params=pltpu.CompilerParams(dimension_semantics=("arbitrary",)),
        cost_estimate=pl.CostEstimate(flops=20 * rows * cols, bytes_accessed=8 * rows * cols, transcendentals=0),
        name="join_up",
    )(rank.reshape(1), *parts)


def solution(mesh):
    ax = mesh.axis_names[0]
    n_dev = mesh.shape[ax]
    group = n_dev // 2

    def hop(v, k):
        return lax.ppermute(v, ax, [(i, i ^ k) for i in range(n_dev)])

    def gather_rows(shard):
        return lax.all_gather(shard, ax, axis=0, tiled=True)

    def scatter_rows(full):
        return lax.psum_scatter(full, ax, scatter_dimension=0, tiled=True)

    def joined(parts):
        rows, cols = parts[0].shape
        out = jnp.zeros((group * rows, cols), parts[0].dtype)
        for k, v in enumerate(parts):
            out = lax.dynamic_update_slice(out, v, (k * rows, 0))
        return out

    def layer(hidden, positions, grad_y, attn_gain, w_qkv, b_qkv, w_out, mlp_gain, w_up, w_down):
        batch, seq_len, width = hidden.shape
        tokens = batch * seq_len
        h_loc = w_up.shape[0]
        h_chip = 2 * h_loc
        f_loc = w_down.shape[0]
        f_blk = f_loc + -f_loc % LANES
        f_pad = 2 * f_blk
        q_loc = b_qkv.shape[0]
        me = lax.axis_index(ax)
        rank = lax.rem(me, group)
        side = lax.div(me, group)
        core = lax.rem(me, 2)
        chip = lax.div(me, 2)

        wqkv = gather_rows(w_qkv)
        wout = gather_rows(w_out)
        small = jnp.concatenate([attn_gain, b_qkv, mlp_gain])[None]
        for k in (1, 2, group):
            far = hop(small, k)
            small = jnp.where((me & k) == 0, jnp.concatenate([small, far]), jnp.concatenate([far, small]))
        up_part = split_up(w_up, rank, group, f_loc, f_pad)
        small, *up_part, w_down, grad_y = after(small, *up_part, w_down, grad_y)
        gain_one = small[:, :h_loc].reshape(1, width).astype(F32)
        bias = small[:, h_loc:h_loc + q_loc].reshape(1, n_dev * q_loc).astype(F32)
        gain_two = small[:, h_loc + q_loc:].reshape(1, width).astype(F32)

        up_near = [up_part[0]] + [hop(up_part[k], k) for k in (1, 2, 3)]
        up_far = [hop(v, group) for v in up_near]
        down_far = hop(w_down, group)
        dy = grad_y.reshape(tokens, width)
        dy_parts = [dy, hop(dy, 1), hop(dy, 2)]

        hid_wide = hidden.astype(F32).reshape(tokens, width)
        inv_one = norm_scale(hid_wide)
        normed = (hid_wide * inv_one * gain_one).astype(BF16)
        q_width = wout.shape[0]
        kv_width = (wqkv.shape[1] - q_width) // 2
        kv_heads = kv_width // HEAD_DIM
        heads = q_width // HEAD_DIM
        cos_t, sin_t = rope_tables(positions)
        z = mm(normed, wqkv, NN_DIMS) + bias
        qkv, context = attend(z, cos_t, sin_t, batch, heads, kv_heads)
        mid = (hid_wide + mm(context, wout, NN_DIMS)).astype(BF16)
        mid_wide = mid.astype(F32)
        inv_two = norm_scale(mid_wide)
        mlp_in = (mid_wide * inv_two * gain_two).astype(BF16)
        w_all = jnp.zeros((width, 2 * f_pad), BF16)
        for k in range(group):
            w_all = lax.dynamic_update_slice(w_all, up_near[k], ((me ^ k) * h_loc, 0))
        for k in (0, 1, 2):
            w_all = lax.dynamic_update_slice(w_all, up_far[k], ((me ^ group ^ k) * h_loc, 0))
        m_all = joined([mlp_in, hop(mlp_in, 1)])
        dy_all = joined(dy_parts[:2])
        wd_all = lax.dynamic_update_slice(jnp.zeros((f_pad, width), BF16), w_down, (side * f_blk, 0))
        m_far = hop(mlp_in, 2)
        m_all, dy_all, w_all, wd_all, m_far = after(m_all, dy_all, w_all, wd_all, m_far)
        w_all = lax.dynamic_update_slice(w_all, up_far[3], ((me ^ group ^ 3) * h_loc, 0))
        m_all = lax.dynamic_update_slice(m_all, m_far, (2 * tokens, 0))
        m_all = lax.dynamic_update_slice(m_all, hop(m_far, 1), (3 * tokens, 0))

        gate_low, lin_low, act = up_act(m_all, w_all)
        act, dy_far, down_far, dy_all = after(act, dy_parts[2], down_far, dy_all)
        dy_parts[2:] = [dy_far, hop(dy_far, 1)]
        for k in (2, 3):
            dy_all = lax.dynamic_update_slice(dy_all, dy_parts[k], (k * tokens, 0))
        wd_all = lax.dynamic_update_slice(wd_all, down_far, ((1 - side) * f_blk, 0))

        def block(rows, k, w, dims):
            return mm(rows[k * tokens:(k + 1) * tokens], w, dims)

        def down_grad(a, blk):
            return mm(lax.dynamic_slice(a, (0, blk * f_blk), (group * tokens, f_blk)), dy_all, TN_DIMS)

        def up_grad(m, d_up, chip_id):
            cols = lax.dynamic_slice(m, (0, chip_id * h_chip), (group * tokens, h_chip))
            return mm(cols, d_up, TN_DIMS)

        y3 = block(act, 3, wd_all, NN_DIMS)
        act, y3 = after(act, y3)
        y3 = hop(y3, 1)
        y2 = block(act, 2, wd_all, NN_DIMS)
        act, y2 = after(act, y2)
        act, dy_all, y2 = after(act, dy_all, y2 + y3)
        y2 = hop(y2, 2)
        down_sum = down_grad(act, 1 - side)
        down_sum, act, gate_low, lin_low = after(down_sum, act, gate_low, lin_low)
        down_sum = hop(down_sum, group)
        d_up = up_back(dy_all, wd_all, gate_low, lin_low)

        far_a = up_grad(m_all, d_up, chip ^ 3)
        d_up, far_a = after(d_up, far_a)
        far_a = hop(far_a, group)
        dm3 = block(d_up, 3, w_all, NT_DIMS)
        d_up, dm3 = after(d_up, dm3)
        dm3 = hop(dm3, 1)
        dm2 = block(d_up, 2, w_all, NT_DIMS)
        d_up, dm2 = after(d_up, dm2)
        d_up, dm2 = after(d_up, dm2 + dm3)
        dm2 = hop(dm2, 2)
        far_b = up_grad(m_all, d_up, chip ^ 2)
        d_up, far_b = after(d_up, far_b)
        far_b = hop(far_b, group)
        near_a = up_grad(m_all, d_up, chip ^ 1)
        d_up, near_a = after(d_up, near_a)
        dm1 = block(d_up, 1, w_all, NT_DIMS)
        d_up, dm1, near_a = after(d_up, dm1, near_a)
        dm1 = hop(dm1, 1)
        dm0 = block(d_up, 0, w_all, NT_DIMS)
        d_up, dm0, act = after(d_up, dm0, act)
        y1 = block(act, 1, wd_all, NN_DIMS)
        act, d_up, y1 = after(act, d_up, y1)
        y1 = hop(y1, 1)
        y0 = block(act, 0, wd_all, NN_DIMS)
        d_up, y0, dm2 = after(d_up, y0, dm2)

        def rows_of(c, *parts):
            return sum(lax.dynamic_slice(v, (c * h_loc, 0), (h_loc, 2 * f_pad)) for v in parts)

        piece2 = hop(rows_of(core, near_a, far_a), 2)
        piece3 = hop(rows_of(1 - core, near_a, far_a), 3)

        d_m = dm0 + dm1 + dm2
        grad_mlp_gain = jnp.sum(d_m * mid_wide * inv_two, axis=0)
        scaled_two = d_m * gain_two
        d_mid = dy.astype(F32) + inv_two * (scaled_two - mid_wide * inv_two * inv_two * jnp.mean(scaled_two * mid_wide, axis=-1, keepdims=True))
        d_mid_low = d_mid.astype(BF16)
        grad_w_out = scatter_rows(mm(context, d_mid_low, TN_DIMS))
        d_context = mm(d_mid_low, wout, NT_DIMS).astype(BF16)
        d_proj, grad_b_qkv = attend_back(qkv, d_context, cos_t, sin_t, batch, heads, kv_heads)
        grad_w_qkv = mm(normed, d_proj, TN_DIMS)
        grad_w_qkv, d_proj = after(grad_w_qkv, d_proj)
        grad_w_qkv = scatter_rows(grad_w_qkv)
        d_normed = mm(d_proj, wqkv, NT_DIMS)
        d_normed, d_up = after(d_normed, d_up)
        near_b = up_grad(m_all, d_up, chip)
        near_b, d_normed, act, down_sum = after(near_b, d_normed, act, down_sum)
        grad_w_down = mm(lax.dynamic_slice(act, (0, side * f_blk), (group * tokens, f_blk)), dy_all, TN_DIMS)[:f_loc] + down_sum[:f_loc]
        grad_attn_gain = jnp.sum(d_normed * hid_wide * inv_one, axis=0)
        small_grads = jnp.concatenate([grad_attn_gain.reshape(n_dev, h_loc), grad_b_qkv.reshape(n_dev, q_loc), grad_mlp_gain.reshape(n_dev, h_loc)], axis=1)

        def halved(sums, k):
            pair = sums.reshape(-1, 2, h_loc + q_loc + h_loc)
            mine = lax.div(me, k) % 2
            return lax.dynamic_index_in_dim(pair, mine, 1, keepdims=False) + hop(lax.dynamic_index_in_dim(pair, 1 - mine, 1, keepdims=False), k)

        small_grads = halved(halved(small_grads, 1), 2)
        scaled_one = d_normed * gain_one
        grad_hidden = (d_mid + inv_one * (scaled_one - hid_wide * inv_one * inv_one * jnp.mean(scaled_one * hid_wide, axis=-1, keepdims=True))).astype(BF16)
        y0, y1, y2, mid_late, grad_hidden = after(y0, y1, y2, mid, grad_hidden)
        output = (mid_late.astype(F32) + (y0 + y1 + y2)).astype(BF16)
        far_b, output, grad_hidden, grad_w_down, small_grads = after(far_b, output, grad_hidden, grad_w_down, small_grads)
        small_grads = halved(small_grads, group).reshape(-1)
        piece0 = rows_of(core, near_b, far_b)
        piece1 = hop(rows_of(1 - core, near_b, far_b), 1)
        grad_w_up = join_up([piece0, piece1, piece2, piece3], rank, group, f_loc)
        return (output.reshape(hidden.shape), grad_hidden.reshape(hidden.shape), small_grads[:h_loc], grad_w_qkv, small_grads[h_loc:h_loc + q_loc], grad_w_out, small_grads[h_loc + q_loc:], grad_w_up, grad_w_down)

    row_spec = P(ax)
    return jax.shard_map(layer, mesh=mesh, in_specs=(row_spec,) * 10, out_specs=(row_spec,) * 9, check_vma=False)
```

```python
import functools

import jax
import jax.numpy as jnp
from jax import lax
from jax.experimental import pallas as pl
from jax.experimental.pallas import tpu as pltpu
from jax.sharding import PartitionSpec as P


HEAD_DIM = 128
ROT_DIM = 64
ROPE_BASE = 10000.0
EPS = 1e-5

NT_DIMS = (((1,), (1,)), ((), ()))
TN_DIMS = (((0,), (0,)), ((), ()))
NN_DIMS = (((1,), (0,)), ((), ()))
F32 = jnp.float32
BF16 = jnp.bfloat16
SCALE = HEAD_DIM ** -0.5
MASKED = -1e30
Q_BLOCK = 128
S_BLOCK = 64
T_BLOCK = 768
F_BLOCK = 256
LANES = 128
LOG2_E = 1.4426950408889634


def mm(a, b, dims):
    return lax.dot_general(a, b, dims, preferred_element_type=F32)


def after(*vals):
    return lax.optimization_barrier(vals)


def norm_scale(rows_in):
    return lax.rsqrt(jnp.mean(rows_in * rows_in, axis=-1, keepdims=True) + EPS)


def rope_tables(positions):
    lane = jnp.arange(HEAD_DIM, dtype=jnp.int32)
    pair = (lane - lane % 2).astype(F32)
    inv_freq = 1.0 / (ROPE_BASE ** (pair / ROT_DIM))
    angles = positions.astype(F32).reshape(-1, 1) * inv_freq
    turned = lane < ROT_DIM
    sines = jnp.sin(angles)
    return jnp.where(turned, jnp.cos(angles), 1.0), jnp.where(turned, jnp.where(lane % 2 == 0, -sines, sines), 0.0)


def swap_pairs(v):
    lane = lax.broadcasted_iota(jnp.int32, v.shape, 1)
    return jnp.where(lane % 2 == 0, pltpu.roll(v, HEAD_DIM - 1, 1), pltpu.roll(v, 1, 1))


def attend_kernel(heads, kv_heads, z_ref, cos_ref, sin_ref, qkv_ref, ctx_ref, *bufs):
    s_refs, p_refs = bufs[:2], bufs[2:]
    seq_len = z_ref.shape[0]
    group = heads // kv_heads
    cos_t, sin_t = cos_ref[...], sin_ref[...]

    def cols(i):
        return pl.ds(pl.multiple_of(i * HEAD_DIM, HEAD_DIM), HEAD_DIM)

    @pl.loop(0, heads + kv_heads, unroll=3)
    def _(i):
        zh = z_ref[:, cols(i)]
        qkv_ref[:, cols(i)] = (zh * cos_t + swap_pairs(zh) * sin_t).astype(BF16)

    qkv_ref[:, (heads + kv_heads) * HEAD_DIM:] = z_ref[:, (heads + kv_heads) * HEAD_DIM:].astype(BF16)

    @pl.loop(0, kv_heads)
    def _(g):
        kc, vc = cols(heads + g), cols(heads + kv_heads + g)
        for r in range(0, seq_len, Q_BLOCK):
            n = r + Q_BLOCK
            q = jnp.concatenate([qkv_ref[r:n, cols(g * group + h)] for h in range(group)], axis=0)
            s_ref, p_ref = s_refs[r // Q_BLOCK % 2], p_refs[r // Q_BLOCK % 2]
            s_ref[:, :n] = mm(q, qkv_ref[:n, kc], NT_DIMS)

            @pl.loop(0, group * Q_BLOCK // S_BLOCK, unroll=True)
            def _(c):
                rows = pl.ds(pl.multiple_of(c * S_BLOCK, S_BLOCK), S_BLOCK)
                s = s_ref[rows, :n]
                row = lax.broadcasted_iota(jnp.int32, (S_BLOCK, Q_BLOCK), 0) + lax.rem(c * S_BLOCK, Q_BLOCK)
                col = lax.broadcasted_iota(jnp.int32, (S_BLOCK, Q_BLOCK), 1)
                own = jnp.where(row >= col, s[:, r:], MASKED)
                s = own if r == 0 else jnp.concatenate([s[:, :r], own], axis=1)
                e = jnp.exp2((s - jnp.max(s, axis=1, keepdims=True)) * (SCALE * LOG2_E))
                p_ref[rows, :n] = (e * (1.0 / jnp.sum(e, axis=1, keepdims=True))).astype(BF16)

            ctx = mm(p_ref[:, :n], qkv_ref[:n, vc], NN_DIMS).astype(BF16)
            for h in range(group):
                ctx_ref[r:n, cols(g * group + h)] = ctx[h * Q_BLOCK:(h + 1) * Q_BLOCK]


def attend_back_kernel(heads, kv_heads, qkv_ref, dctx_ref, cos_ref, sin_ref, dz_ref, sum_ref, dk_ref, dv_ref, s_ref, dp_ref, p_ref, ds_ref):
    seq_len = qkv_ref.shape[0]
    group = heads // kv_heads

    def cols(i):
        return pl.ds(pl.multiple_of(i * HEAD_DIM, HEAD_DIM), HEAD_DIM)

    @pl.when(pl.program_id(0) == 0)
    def _():
        sum_ref[...] = jnp.zeros_like(sum_ref)

    def put(rows, c, d):
        dz_ref[rows, c] = d.astype(BF16)
        sum_ref[:, c] += jnp.sum(d, axis=0, keepdims=True)

    def turned_back(rows, d):
        return d * cos_ref[rows, :] - swap_pairs(d) * sin_ref[rows, :]

    @pl.loop(0, kv_heads)
    def _(g):
        kc, vc = cols(heads + g), cols(heads + kv_heads + g)
        dk_ref[...] = jnp.zeros_like(dk_ref)
        dv_ref[...] = jnp.zeros_like(dv_ref)
        for r in range(0, seq_len, Q_BLOCK):
            n = r + Q_BLOCK
            q = jnp.concatenate([qkv_ref[r:n, cols(g * group + h)] for h in range(group)], axis=0)
            d = jnp.concatenate([dctx_ref[r:n, cols(g * group + h)] for h in range(group)], axis=0)
            s_ref[:n] = mm(qkv_ref[:n, kc], q, NT_DIMS)
            dp_ref[:n] = mm(qkv_ref[:n, vc], d, NT_DIMS)

            @pl.loop(0, group, unroll=True)
            def _(h):
                c = cols(h)
                s, dp = s_ref[:n, c], dp_ref[:n, c]
                row = lax.broadcasted_iota(jnp.int32, (Q_BLOCK, Q_BLOCK), 0)
                col = lax.broadcasted_iota(jnp.int32, (Q_BLOCK, Q_BLOCK), 1)
                own = jnp.where(row <= col, s[r:], MASKED)
                s = own if r == 0 else jnp.concatenate([s[:r], own], axis=0)
                e = jnp.exp2((s - jnp.max(s, axis=0, keepdims=True)) * (SCALE * LOG2_E))
                p = e * (1.0 / jnp.sum(e, axis=0, keepdims=True))
                p_ref[:n, c] = p.astype(BF16)
                ds_ref[:n, c] = (p * (dp - jnp.sum(p * dp, axis=0, keepdims=True)) * SCALE).astype(BF16)

            dv_ref[:n] += mm(p_ref[:n], d, NN_DIMS)
            dk_ref[:n] += mm(ds_ref[:n], q, NN_DIMS)
            dq = mm(qkv_ref[:n, kc], ds_ref[:n], TN_DIMS)
            for h in range(group):
                rows = slice(r, n)
                put(rows, cols(g * group + h), turned_back(rows, jnp.transpose(dq[:, h * Q_BLOCK:(h + 1) * Q_BLOCK])))

        rows = slice(0, seq_len)
        put(rows, kc, turned_back(rows, dk_ref[...]))
        put(rows, vc, dv_ref[...])


def attend(z, cos_t, sin_t, batch, heads, kv_heads):
    tokens, width = z.shape
    seq_len = tokens // batch
    row = lambda b: (b, 0)
    flops = 4 * tokens * seq_len * heads * HEAD_DIM
    return pl.pallas_call(
        functools.partial(attend_kernel, heads, kv_heads),
        grid=(batch,),
        in_specs=[pl.BlockSpec((seq_len, width), row), pl.BlockSpec((seq_len, HEAD_DIM), row), pl.BlockSpec((seq_len, HEAD_DIM), row)],
        out_specs=[pl.BlockSpec((seq_len, width), row), pl.BlockSpec((seq_len, heads * HEAD_DIM), row)],
        out_shape=[jax.ShapeDtypeStruct((tokens, width), BF16), jax.ShapeDtypeStruct((tokens, heads * HEAD_DIM), BF16)],
        scratch_shapes=[pltpu.VMEM((heads // kv_heads * Q_BLOCK, seq_len), t) for t in (F32, F32, BF16, BF16)],
        compiler_params=pltpu.CompilerParams(dimension_semantics=("arbitrary",), vmem_limit_bytes=48 * 2 ** 20),
        cost_estimate=pl.CostEstimate(flops=3 * flops, bytes_accessed=tokens * width * 8, transcendentals=tokens * seq_len * heads),
        name="attend",
    )(z, cos_t, sin_t)


def attend_back(qkv, d_ctx, cos_t, sin_t, batch, heads, kv_heads):
    tokens, width = qkv.shape
    seq_len = tokens // batch
    row = lambda b: (b, 0)
    flops = 10 * tokens * seq_len * heads * HEAD_DIM
    return pl.pallas_call(
        functools.partial(attend_back_kernel, heads, kv_heads),
        grid=(batch,),
        in_specs=[pl.BlockSpec((seq_len, width), row), pl.BlockSpec((seq_len, heads * HEAD_DIM), row), pl.BlockSpec((seq_len, HEAD_DIM), row), pl.BlockSpec((seq_len, HEAD_DIM), row)],
        out_specs=[pl.BlockSpec((seq_len, width), row), pl.BlockSpec((1, width), lambda b: (0, 0))],
        out_shape=[jax.ShapeDtypeStruct((tokens, width), BF16), jax.ShapeDtypeStruct((1, width), F32)],
        scratch_shapes=[pltpu.VMEM((seq_len, HEAD_DIM), F32)] * 2 + [pltpu.VMEM((seq_len, heads // kv_heads * Q_BLOCK), F32)] * 2 + [pltpu.VMEM((seq_len, heads // kv_heads * Q_BLOCK), BF16)] * 2,
        compiler_params=pltpu.CompilerParams(dimension_semantics=("arbitrary",), vmem_limit_bytes=48 * 2 ** 20),
        cost_estimate=pl.CostEstimate(flops=3 * flops, bytes_accessed=tokens * width * 8, transcendentals=tokens * seq_len * heads),
        name="attend_back",
    )(qkv, d_ctx, cos_t, sin_t)


def up_kernel(m_ref, w_ref, g_ref, l_ref, a_ref):
    f_pad = g_ref.shape[1]
    for j in range(0, f_pad, F_BLOCK):
        c = slice(j, j + F_BLOCK)
        gate_low = mm(m_ref[...], w_ref[:, c], NN_DIMS).astype(BF16)
        lin_low = mm(m_ref[...], w_ref[:, f_pad + j:f_pad + j + F_BLOCK], NN_DIMS).astype(BF16)
        g_ref[:, c] = gate_low
        l_ref[:, c] = lin_low
        gate = gate_low.astype(F32)
        a_ref[:, c] = (gate * (1.0 / (1.0 + jnp.exp(-gate))) * lin_low.astype(F32)).astype(BF16)


def up_act(m, w):
    tokens, width = m.shape
    f_pad = w.shape[1] // 2
    row = lambda i: (i, 0)
    return pl.pallas_call(
        up_kernel,
        grid=(tokens // T_BLOCK,),
        in_specs=[pl.BlockSpec((T_BLOCK, width), row), pl.BlockSpec(w.shape, lambda i: (0, 0), pipeline_mode=pl.Buffered(1))],
        out_specs=[pl.BlockSpec((T_BLOCK, f_pad), row)] * 3,
        out_shape=[jax.ShapeDtypeStruct((tokens, f_pad), BF16)] * 3,
        compiler_params=pltpu.CompilerParams(dimension_semantics=("arbitrary",), vmem_limit_bytes=60 * 2 ** 20),
        cost_estimate=pl.CostEstimate(flops=2 * tokens * width * 2 * f_pad, bytes_accessed=2 * (m.size + w.size + 3 * tokens * f_pad), transcendentals=2 * tokens * f_pad),
        name="up_act",
    )(m, w)


def up_back_kernel(dy_ref, wd_ref, g_ref, l_ref, out_ref):
    f_pad = g_ref.shape[1]
    for j in range(0, f_pad, F_BLOCK):
        c = slice(j, j + F_BLOCK)
        d_act = mm(dy_ref[...], wd_ref[c, :], NT_DIMS)
        gate, lin = g_ref[:, c].astype(F32), l_ref[:, c].astype(F32)
        sig = 1.0 / (1.0 + jnp.exp(-gate))
        gate_sig = gate * sig
        out_ref[:, c] = (d_act * (lin * (sig + gate_sig * (1.0 - sig)))).astype(BF16)
        out_ref[:, f_pad + j:f_pad + j + F_BLOCK] = (d_act * gate_sig).astype(BF16)


def up_back(dy, wd, gate_low, lin_low):
    tokens, width = dy.shape
    f_pad = wd.shape[0]
    row = lambda i: (i, 0)
    return pl.pallas_call(
        up_back_kernel,
        grid=(tokens // T_BLOCK,),
        in_specs=[pl.BlockSpec((T_BLOCK, width), row), pl.BlockSpec(wd.shape, lambda i: (0, 0), pipeline_mode=pl.Buffered(1)), pl.BlockSpec((T_BLOCK, f_pad), row), pl.BlockSpec((T_BLOCK, f_pad), row)],
        out_specs=pl.BlockSpec((T_BLOCK, 2 * f_pad), row),
        out_shape=jax.ShapeDtypeStruct((tokens, 2 * f_pad), BF16),
        compiler_params=pltpu.CompilerParams(dimension_semantics=("arbitrary",), vmem_limit_bytes=60 * 2 ** 20),
        cost_estimate=pl.CostEstimate(flops=2 * tokens * width * f_pad, bytes_accessed=2 * (dy.size + wd.size + 4 * tokens * f_pad), transcendentals=2 * tokens * f_pad),
        name="up_back",
    )(dy, wd, gate_low, lin_low)


def shifted_tile(load, start, limit):
    tile, phase = start // LANES, start % LANES
    near = load(min(max(tile, 0), limit - 1))
    if phase == 0:
        return near
    after_it = load(min(max(tile + 1, 0), limit - 1))
    lane = lax.broadcasted_iota(jnp.int32, near.shape, 1)
    return jnp.where(lane < LANES - phase, pltpu.roll(near, LANES - phase, 1), pltpu.roll(after_it, LANES - phase, 1))


def gathered_tile(lo, segments, shape):
    lane = lax.broadcasted_iota(jnp.int32, shape, 1)
    out = jnp.zeros(shape, F32)
    for first, length, load, there, limit in segments:
        a, b = max(first, lo), min(first + length, lo + LANES)
        if a < b:
            part = shifted_tile(load, there + lo - first, limit)
            inside = (lane >= a - lo) & (lane < b - lo)
            out = part if b - a == LANES else jnp.where(inside, part, out)
    return out


def split_kernel(group, f_loc, rank_ref, w_ref, *out_refs):
    rows, cols = w_ref.shape
    f_pad = out_refs[0].shape[1] // 2

    def load(t):
        return w_ref[:, t * LANES:(t + 1) * LANES].astype(F32)

    for r in range(group):
        @pl.when(rank_ref[0] == r)
        def _():
            for q in range(group):
                for h in range(2):
                    segments = [(s * f_pad // 2, f_loc, load, ((2 * h + s) * group + q) * f_loc, cols // LANES) for s in range(2)]
                    for lo in range(0, f_pad, LANES):
                        out_refs[r ^ q][:, h * f_pad + lo:h * f_pad + lo + LANES] = gathered_tile(lo, segments, (rows, LANES)).astype(BF16)


def split_up(w_up, rank, group, f_loc, f_pad):
    rows, cols = w_up.shape
    step = 32
    return pl.pallas_call(
        functools.partial(split_kernel, group, f_loc),
        grid_spec=pltpu.PrefetchScalarGridSpec(
            num_scalar_prefetch=1,
            grid=(rows // step,),
            in_specs=[pl.BlockSpec((step, cols), lambda i, r: (i, 0))],
            out_specs=[pl.BlockSpec((step, 2 * f_pad), lambda i, r: (i, 0))] * group,
        ),
        out_shape=[jax.ShapeDtypeStruct((rows, 2 * f_pad), BF16)] * group,
        compiler_params=pltpu.CompilerParams(dimension_semantics=("arbitrary",)),
        cost_estimate=pl.CostEstimate(flops=20 * rows * cols, bytes_accessed=4 * rows * cols, transcendentals=0),
        name="split_up",
    )(rank.reshape(1), w_up)


def join_kernel(group, f_loc, rank_ref, *refs):
    parts, out_ref = refs[:group], refs[group]
    rows, cols = out_ref.shape
    f_pad = parts[0].shape[1] // 2
    half = cols // 2
    for r in range(group):
        @pl.when(rank_ref[0] == r)
        def _():
            def loader(ref):
                return lambda t: ref[:, t * LANES:(t + 1) * LANES]

            for h in range(2):
                segments = [(b * f_loc, f_loc, loader(parts[r ^ (b % group)]), h * f_pad + b // group * f_pad // 2, 2 * f_pad // LANES) for b in range(2 * group)]
                for lo in range(0, half, LANES):
                    out_ref[:, h * half + lo:h * half + lo + LANES] = gathered_tile(lo, segments, (rows, LANES))


def join_up(parts, rank, group, f_loc):
    rows, width = parts[0].shape
    cols = 4 * group * f_loc
    step = 32
    return pl.pallas_call(
        functools.partial(join_kernel, group, f_loc),
        grid_spec=pltpu.PrefetchScalarGridSpec(
            num_scalar_prefetch=1,
            grid=(rows // step,),
            in_specs=[pl.BlockSpec((step, width), lambda i, r: (i, 0))] * group,
            out_specs=pl.BlockSpec((step, cols), lambda i, r: (i, 0)),
        ),
        out_shape=jax.ShapeDtypeStruct((rows, cols), F32),
        compiler_params=pltpu.CompilerParams(dimension_semantics=("arbitrary",)),
        cost_estimate=pl.CostEstimate(flops=20 * rows * cols, bytes_accessed=8 * rows * cols, transcendentals=0),
        name="join_up",
    )(rank.reshape(1), *parts)


def solution(mesh):
    ax = mesh.axis_names[0]
    n_dev = mesh.shape[ax]
    group = n_dev // 2

    def hop(v, k):
        return lax.ppermute(v, ax, [(i, i ^ k) for i in range(n_dev)])

    def gather_rows(shard):
        return lax.all_gather(shard, ax, axis=0, tiled=True)

    def scatter_rows(full):
        return lax.psum_scatter(full, ax, scatter_dimension=0, tiled=True)

    def joined(parts):
        rows, cols = parts[0].shape
        out = jnp.zeros((group * rows, cols), parts[0].dtype)
        for k, v in enumerate(parts):
            out = lax.dynamic_update_slice(out, v, (k * rows, 0))
        return out

    def layer(hidden, positions, grad_y, attn_gain, w_qkv, b_qkv, w_out, mlp_gain, w_up, w_down):
        batch, seq_len, width = hidden.shape
        tokens = batch * seq_len
        h_loc = w_up.shape[0]
        h_chip = 2 * h_loc
        f_loc = w_down.shape[0]
        f_blk = f_loc + -f_loc % LANES
        f_pad = 2 * f_blk
        q_loc = b_qkv.shape[0]
        me = lax.axis_index(ax)
        rank = lax.rem(me, group)
        side = lax.div(me, group)
        core = lax.rem(me, 2)
        chip = lax.div(me, 2)

        wqkv = gather_rows(w_qkv)
        wout = gather_rows(w_out)
        small = jnp.concatenate([attn_gain, b_qkv, mlp_gain])[None]
        for k in (1, 2, group):
            far = hop(small, k)
            small = jnp.where((me & k) == 0, jnp.concatenate([small, far]), jnp.concatenate([far, small]))
        up_part = split_up(w_up, rank, group, f_loc, f_pad)
        small, *up_part, w_down, grad_y = after(small, *up_part, w_down, grad_y)
        gain_one = small[:, :h_loc].reshape(1, width).astype(F32)
        bias = small[:, h_loc:h_loc + q_loc].reshape(1, n_dev * q_loc).astype(F32)
        gain_two = small[:, h_loc + q_loc:].reshape(1, width).astype(F32)

        up_near = [up_part[0]] + [hop(up_part[k], k) for k in (1, 2, 3)]
        up_far = [hop(v, group) for v in up_near]
        down_far = hop(w_down, group)
        dy = grad_y.reshape(tokens, width)
        dy_parts = [dy, hop(dy, 1), hop(dy, 2)]

        hid_wide = hidden.astype(F32).reshape(tokens, width)
        inv_one = norm_scale(hid_wide)
        normed = (hid_wide * inv_one * gain_one).astype(BF16)
        q_width = wout.shape[0]
        kv_width = (wqkv.shape[1] - q_width) // 2
        kv_heads = kv_width // HEAD_DIM
        heads = q_width // HEAD_DIM
        cos_t, sin_t = rope_tables(positions)
        z = mm(normed, wqkv, NN_DIMS) + bias
        qkv, context = attend(z, cos_t, sin_t, batch, heads, kv_heads)
        mid = (hid_wide + mm(context, wout, NN_DIMS)).astype(BF16)
        mid_wide = mid.astype(F32)
        inv_two = norm_scale(mid_wide)
        mlp_in = (mid_wide * inv_two * gain_two).astype(BF16)
        w_all = jnp.zeros((width, 2 * f_pad), BF16)
        for k in range(group):
            w_all = lax.dynamic_update_slice(w_all, up_near[k], ((me ^ k) * h_loc, 0))
        for k in (0, 1, 2):
            w_all = lax.dynamic_update_slice(w_all, up_far[k], ((me ^ group ^ k) * h_loc, 0))
        m_all = joined([mlp_in, hop(mlp_in, 1)])
        dy_all = joined(dy_parts[:2])
        wd_all = lax.dynamic_update_slice(jnp.zeros((f_pad, width), BF16), w_down, (side * f_blk, 0))
        m_far = hop(mlp_in, 2)
        m_all, dy_all, w_all, wd_all, m_far = after(m_all, dy_all, w_all, wd_all, m_far)
        w_all = lax.dynamic_update_slice(w_all, up_far[3], ((me ^ group ^ 3) * h_loc, 0))
        m_all = lax.dynamic_update_slice(m_all, m_far, (2 * tokens, 0))
        m_all = lax.dynamic_update_slice(m_all, hop(m_far, 1), (3 * tokens, 0))

        gate_low, lin_low, act = up_act(m_all, w_all)
        act, dy_far, down_far, dy_all = after(act, dy_parts[2], down_far, dy_all)
        dy_parts[2:] = [dy_far, hop(dy_far, 1)]
        for k in (2, 3):
            dy_all = lax.dynamic_update_slice(dy_all, dy_parts[k], (k * tokens, 0))
        wd_all = lax.dynamic_update_slice(wd_all, down_far, ((1 - side) * f_blk, 0))

        def block(rows, k, w, dims):
            return mm(rows[k * tokens:(k + 1) * tokens], w, dims)

        def down_grad(a, blk):
            return mm(lax.dynamic_slice(a, (0, blk * f_blk), (group * tokens, f_blk)), dy_all, TN_DIMS)

        def up_grad(m, d_up, block_id, chips):
            cols = lax.dynamic_slice(m, (0, block_id * chips * h_chip), (group * tokens, chips * h_chip))
            return mm(cols, d_up, TN_DIMS)

        y3 = block(act, 3, wd_all, NN_DIMS)
        act, y3 = after(act, y3)
        y3 = hop(y3, 1)
        y2 = block(act, 2, wd_all, NN_DIMS)
        act, y2 = after(act, y2)
        act, dy_all, y2 = after(act, dy_all, y2 + y3)
        y2 = hop(y2, 2)
        down_sum = down_grad(act, 1 - side)
        down_sum, act, gate_low, lin_low = after(down_sum, act, gate_low, lin_low)
        down_sum = hop(down_sum, group)
        d_up = up_back(dy_all, wd_all, gate_low, lin_low)

        dm3 = block(d_up, 3, w_all, NT_DIMS)
        d_up, dm3 = after(d_up, dm3)
        dm3 = hop(dm3, 1)
        dm2 = block(d_up, 2, w_all, NT_DIMS)
        d_up, dm2 = after(d_up, dm2)
        d_up, dm2 = after(d_up, dm2 + dm3)
        dm2 = hop(dm2, 2)

        far_a = up_grad(m_all, d_up, chip ^ 3, 1)
        d_up, far_a = after(d_up, far_a)
        far_a = hop(far_a, group)
        far_b = up_grad(m_all, d_up, chip ^ 2, 1)
        d_up, far_b = after(d_up, far_b)
        far_b = hop(far_b, group)
        near = up_grad(m_all, d_up, side, 2)
        d_up, near = after(d_up, near)
        dm1 = block(d_up, 1, w_all, NT_DIMS)
        d_up, dm1 = after(d_up, dm1)
        dm1 = hop(dm1, 1)
        dm0 = block(d_up, 0, w_all, NT_DIMS)
        d_up, dm0, act, dm2, near = after(d_up, dm0, act, dm2, near)

        x_id = lax.rem(chip, 2)

        def rows_of(near, x, c, far):
            own = lax.dynamic_slice(near, (x * h_chip + c * h_loc, 0), (h_loc, 2 * f_pad))
            return own + lax.dynamic_slice(far, (c * h_loc, 0), (h_loc, 2 * f_pad))

        piece2 = hop(rows_of(near, 1 - x_id, core, far_a), 2)
        piece3 = hop(rows_of(near, 1 - x_id, 1 - core, far_a), 3)

        d_m = dm0 + dm1 + dm2
        grad_mlp_gain = jnp.sum(d_m * mid_wide * inv_two, axis=0)
        scaled_two = d_m * gain_two
        d_mid = dy.astype(F32) + inv_two * (scaled_two - mid_wide * inv_two * inv_two * jnp.mean(scaled_two * mid_wide, axis=-1, keepdims=True))
        d_mid_low = d_mid.astype(BF16)
        grad_w_out = scatter_rows(mm(context, d_mid_low, TN_DIMS))
        d_context = mm(d_mid_low, wout, NT_DIMS).astype(BF16)
        d_proj, grad_b_qkv = attend_back(qkv, d_context, cos_t, sin_t, batch, heads, kv_heads)
        grad_w_qkv = mm(normed, d_proj, TN_DIMS)
        grad_w_qkv, d_proj = after(grad_w_qkv, d_proj)
        grad_w_qkv = scatter_rows(grad_w_qkv)
        d_normed = mm(d_proj, wqkv, NT_DIMS)
        d_normed, act = after(d_normed, act)
        y1 = hop(block(act, 1, wd_all, NN_DIMS), 1)
        act, d_normed, y1, down_sum = after(act, d_normed, y1, down_sum)
        grad_w_down = mm(lax.dynamic_slice(act, (0, side * f_blk), (group * tokens, f_blk)), dy_all, TN_DIMS)[:f_loc] + down_sum[:f_loc]
        grad_w_down, act, near = after(grad_w_down, act, near)
        grad_attn_gain = jnp.sum(d_normed * hid_wide * inv_one, axis=0)
        small_grads = jnp.concatenate([grad_attn_gain.reshape(n_dev, h_loc), grad_b_qkv.reshape(n_dev, q_loc), grad_mlp_gain.reshape(n_dev, h_loc)], axis=1)

        def halved(sums, k):
            pair = sums.reshape(-1, 2, h_loc + q_loc + h_loc)
            mine = lax.div(me, k) % 2
            return lax.dynamic_index_in_dim(pair, mine, 1, keepdims=False) + hop(lax.dynamic_index_in_dim(pair, 1 - mine, 1, keepdims=False), k)

        small_grads = halved(halved(small_grads, 1), 2)
        scaled_one = d_normed * gain_one
        grad_hidden = (d_mid + inv_one * (scaled_one - hid_wide * inv_one * inv_one * jnp.mean(scaled_one * hid_wide, axis=-1, keepdims=True))).astype(BF16)
        act, y1, y2, mid, grad_hidden = after(act, y1, y2, mid, grad_hidden)
        output = (mid.astype(F32) + (block(act, 0, wd_all, NN_DIMS) + y1 + y2)).astype(BF16)
        far_b, output, grad_hidden, grad_w_down, small_grads = after(far_b, output, grad_hidden, grad_w_down, small_grads)
        small_grads = halved(small_grads, group).reshape(-1)
        piece0 = rows_of(near, x_id, core, far_b)
        piece1 = hop(rows_of(near, x_id, 1 - core, far_b), 1)
        grad_w_up = join_up([piece0, piece1, piece2, piece3], rank, group, f_loc)
        return (output.reshape(hidden.shape), grad_hidden.reshape(hidden.shape), small_grads[:h_loc], grad_w_qkv, small_grads[h_loc:h_loc + q_loc], grad_w_out, small_grads[h_loc + q_loc:], grad_w_up, grad_w_down)

    row_spec = P(ax)
    return jax.shard_map(layer, mesh=mesh, in_specs=(row_spec,) * 10, out_specs=(row_spec,) * 9, check_vma=False)
```

```python
import functools

import jax
import jax.numpy as jnp
from jax import lax
from jax.experimental import pallas as pl
from jax.experimental.pallas import tpu as pltpu
from jax.sharding import PartitionSpec as P


HEAD_DIM = 128
ROT_DIM = 64
ROPE_BASE = 10000.0
EPS = 1e-5

NT_DIMS = (((1,), (1,)), ((), ()))
TN_DIMS = (((0,), (0,)), ((), ()))
NN_DIMS = (((1,), (0,)), ((), ()))
F32 = jnp.float32
BF16 = jnp.bfloat16
SCALE = HEAD_DIM ** -0.5
MASKED = -1e30
Q_BLOCK = 128
S_BLOCK = 64
T_BLOCK = 768
F_BLOCK = 256
LANES = 128
LOG2_E = 1.4426950408889634


def mm(a, b, dims):
    return lax.dot_general(a, b, dims, preferred_element_type=F32)


def after(*vals):
    return lax.optimization_barrier(vals)


def norm_scale(rows_in):
    return lax.rsqrt(jnp.mean(rows_in * rows_in, axis=-1, keepdims=True) + EPS)


def rope_tables(positions):
    lane = jnp.arange(HEAD_DIM, dtype=jnp.int32)
    pair = (lane - lane % 2).astype(F32)
    inv_freq = 1.0 / (ROPE_BASE ** (pair / ROT_DIM))
    angles = positions.astype(F32).reshape(-1, 1) * inv_freq
    turned = lane < ROT_DIM
    sines = jnp.sin(angles)
    return jnp.where(turned, jnp.cos(angles), 1.0), jnp.where(turned, jnp.where(lane % 2 == 0, -sines, sines), 0.0)


def swap_pairs(v):
    lane = lax.broadcasted_iota(jnp.int32, v.shape, 1)
    return jnp.where(lane % 2 == 0, pltpu.roll(v, HEAD_DIM - 1, 1), pltpu.roll(v, 1, 1))


def attend_kernel(heads, kv_heads, z_ref, cos_ref, sin_ref, qkv_ref, ctx_ref, *bufs):
    s_refs, p_refs = bufs[:2], bufs[2:]
    seq_len = z_ref.shape[0]
    group = heads // kv_heads
    cos_t, sin_t = cos_ref[...], sin_ref[...]

    def cols(i):
        return pl.ds(pl.multiple_of(i * HEAD_DIM, HEAD_DIM), HEAD_DIM)

    @pl.loop(0, heads + kv_heads, unroll=3)
    def _(i):
        zh = z_ref[:, cols(i)]
        qkv_ref[:, cols(i)] = (zh * cos_t + swap_pairs(zh) * sin_t).astype(BF16)

    qkv_ref[:, (heads + kv_heads) * HEAD_DIM:] = z_ref[:, (heads + kv_heads) * HEAD_DIM:].astype(BF16)

    @pl.loop(0, kv_heads)
    def _(g):
        kc, vc = cols(heads + g), cols(heads + kv_heads + g)
        for r in range(0, seq_len, Q_BLOCK):
            n = r + Q_BLOCK
            q = jnp.concatenate([qkv_ref[r:n, cols(g * group + h)] for h in range(group)], axis=0)
            s_ref, p_ref = s_refs[r // Q_BLOCK % 2], p_refs[r // Q_BLOCK % 2]
            s_ref[:, :n] = mm(q, qkv_ref[:n, kc], NT_DIMS)

            @pl.loop(0, group * Q_BLOCK // S_BLOCK, unroll=True)
            def _(c):
                rows = pl.ds(pl.multiple_of(c * S_BLOCK, S_BLOCK), S_BLOCK)
                s = s_ref[rows, :n]
                row = lax.broadcasted_iota(jnp.int32, (S_BLOCK, Q_BLOCK), 0) + lax.rem(c * S_BLOCK, Q_BLOCK)
                col = lax.broadcasted_iota(jnp.int32, (S_BLOCK, Q_BLOCK), 1)
                own = jnp.where(row >= col, s[:, r:], MASKED)
                s = own if r == 0 else jnp.concatenate([s[:, :r], own], axis=1)
                e = jnp.exp2((s - jnp.max(s, axis=1, keepdims=True)) * (SCALE * LOG2_E))
                p_ref[rows, :n] = (e * (1.0 / jnp.sum(e, axis=1, keepdims=True))).astype(BF16)

            ctx = mm(p_ref[:, :n], qkv_ref[:n, vc], NN_DIMS).astype(BF16)
            for h in range(group):
                ctx_ref[r:n, cols(g * group + h)] = ctx[h * Q_BLOCK:(h + 1) * Q_BLOCK]


def attend_back_kernel(heads, kv_heads, qkv_ref, dctx_ref, cos_ref, sin_ref, dz_ref, sum_ref, dk_ref, dv_ref, s_ref, dp_ref, p_ref, ds_ref):
    seq_len = qkv_ref.shape[0]
    group = heads // kv_heads

    def cols(i):
        return pl.ds(pl.multiple_of(i * HEAD_DIM, HEAD_DIM), HEAD_DIM)

    @pl.when(pl.program_id(0) == 0)
    def _():
        sum_ref[...] = jnp.zeros_like(sum_ref)

    def put(rows, c, d):
        dz_ref[rows, c] = d.astype(BF16)
        sum_ref[:, c] += jnp.sum(d, axis=0, keepdims=True)

    def turned_back(rows, d):
        return d * cos_ref[rows, :] - swap_pairs(d) * sin_ref[rows, :]

    @pl.loop(0, kv_heads)
    def _(g):
        kc, vc = cols(heads + g), cols(heads + kv_heads + g)
        dk_ref[...] = jnp.zeros_like(dk_ref)
        dv_ref[...] = jnp.zeros_like(dv_ref)
        for r in range(0, seq_len, Q_BLOCK):
            n = r + Q_BLOCK
            q = jnp.concatenate([qkv_ref[r:n, cols(g * group + h)] for h in range(group)], axis=0)
            d = jnp.concatenate([dctx_ref[r:n, cols(g * group + h)] for h in range(group)], axis=0)
            s_ref[:n] = mm(qkv_ref[:n, kc], q, NT_DIMS)
            dp_ref[:n] = mm(qkv_ref[:n, vc], d, NT_DIMS)

            @pl.loop(0, group, unroll=True)
            def _(h):
                c = cols(h)
                s, dp = s_ref[:n, c], dp_ref[:n, c]
                row = lax.broadcasted_iota(jnp.int32, (Q_BLOCK, Q_BLOCK), 0)
                col = lax.broadcasted_iota(jnp.int32, (Q_BLOCK, Q_BLOCK), 1)
                own = jnp.where(row <= col, s[r:], MASKED)
                s = own if r == 0 else jnp.concatenate([s[:r], own], axis=0)
                e = jnp.exp2((s - jnp.max(s, axis=0, keepdims=True)) * (SCALE * LOG2_E))
                p = e * (1.0 / jnp.sum(e, axis=0, keepdims=True))
                p_ref[:n, c] = p.astype(BF16)
                ds_ref[:n, c] = (p * (dp - jnp.sum(p * dp, axis=0, keepdims=True)) * SCALE).astype(BF16)

            dv_ref[:n] += mm(p_ref[:n], d, NN_DIMS)
            dk_ref[:n] += mm(ds_ref[:n], q, NN_DIMS)
            dq = mm(qkv_ref[:n, kc], ds_ref[:n], TN_DIMS)
            for h in range(group):
                rows = slice(r, n)
                put(rows, cols(g * group + h), turned_back(rows, jnp.transpose(dq[:, h * Q_BLOCK:(h + 1) * Q_BLOCK])))

        rows = slice(0, seq_len)
        put(rows, kc, turned_back(rows, dk_ref[...]))
        put(rows, vc, dv_ref[...])


def attend(z, cos_t, sin_t, batch, heads, kv_heads):
    tokens, width = z.shape
    seq_len = tokens // batch
    row = lambda b: (b, 0)
    flops = 4 * tokens * seq_len * heads * HEAD_DIM
    return pl.pallas_call(
        functools.partial(attend_kernel, heads, kv_heads),
        grid=(batch,),
        in_specs=[pl.BlockSpec((seq_len, width), row), pl.BlockSpec((seq_len, HEAD_DIM), row), pl.BlockSpec((seq_len, HEAD_DIM), row)],
        out_specs=[pl.BlockSpec((seq_len, width), row), pl.BlockSpec((seq_len, heads * HEAD_DIM), row)],
        out_shape=[jax.ShapeDtypeStruct((tokens, width), BF16), jax.ShapeDtypeStruct((tokens, heads * HEAD_DIM), BF16)],
        scratch_shapes=[pltpu.VMEM((heads // kv_heads * Q_BLOCK, seq_len), t) for t in (F32, F32, BF16, BF16)],
        compiler_params=pltpu.CompilerParams(dimension_semantics=("arbitrary",), vmem_limit_bytes=48 * 2 ** 20),
        cost_estimate=pl.CostEstimate(flops=3 * flops, bytes_accessed=tokens * width * 8, transcendentals=tokens * seq_len * heads),
        name="attend",
    )(z, cos_t, sin_t)


def attend_back(qkv, d_ctx, cos_t, sin_t, batch, heads, kv_heads):
    tokens, width = qkv.shape
    seq_len = tokens // batch
    row = lambda b: (b, 0)
    flops = 10 * tokens * seq_len * heads * HEAD_DIM
    return pl.pallas_call(
        functools.partial(attend_back_kernel, heads, kv_heads),
        grid=(batch,),
        in_specs=[pl.BlockSpec((seq_len, width), row), pl.BlockSpec((seq_len, heads * HEAD_DIM), row), pl.BlockSpec((seq_len, HEAD_DIM), row), pl.BlockSpec((seq_len, HEAD_DIM), row)],
        out_specs=[pl.BlockSpec((seq_len, width), row), pl.BlockSpec((1, width), lambda b: (0, 0))],
        out_shape=[jax.ShapeDtypeStruct((tokens, width), BF16), jax.ShapeDtypeStruct((1, width), F32)],
        scratch_shapes=[pltpu.VMEM((seq_len, HEAD_DIM), F32)] * 2 + [pltpu.VMEM((seq_len, heads // kv_heads * Q_BLOCK), F32)] * 2 + [pltpu.VMEM((seq_len, heads // kv_heads * Q_BLOCK), BF16)] * 2,
        compiler_params=pltpu.CompilerParams(dimension_semantics=("arbitrary",), vmem_limit_bytes=48 * 2 ** 20),
        cost_estimate=pl.CostEstimate(flops=3 * flops, bytes_accessed=tokens * width * 8, transcendentals=tokens * seq_len * heads),
        name="attend_back",
    )(qkv, d_ctx, cos_t, sin_t)


def up_kernel(m_ref, w_ref, *refs):
    g_ref, l_ref, a_ref = refs[-3:]
    f_pad = g_ref.shape[1]
    for j in range(0, f_pad, F_BLOCK):
        c = slice(j, j + F_BLOCK)
        gate_low = mm(m_ref[...], w_ref[:, c], NN_DIMS).astype(BF16)
        lin_low = mm(m_ref[...], w_ref[:, f_pad + j:f_pad + j + F_BLOCK], NN_DIMS).astype(BF16)
        g_ref[:, c] = gate_low
        l_ref[:, c] = lin_low
        gate = gate_low.astype(F32)
        a_ref[:, c] = (gate * (1.0 / (1.0 + jnp.exp(-gate))) * lin_low.astype(F32)).astype(BF16)


def up_act(m, w, half, filled=()):
    tokens, width = m.shape
    f_pad = w.shape[1] // 2
    steps = tokens // 2 // T_BLOCK
    row = lambda i: (i + half * steps, 0)
    return pl.pallas_call(
        up_kernel,
        grid=(steps,),
        in_specs=[pl.BlockSpec((T_BLOCK, width), row), pl.BlockSpec(w.shape, lambda i: (0, 0), pipeline_mode=pl.Buffered(1))] + [pl.BlockSpec(memory_space=pl.ANY)] * len(filled),
        out_specs=[pl.BlockSpec((T_BLOCK, f_pad), row)] * 3,
        out_shape=[jax.ShapeDtypeStruct((tokens, f_pad), BF16)] * 3,
        input_output_aliases={2 + i: i for i in range(len(filled))},
        compiler_params=pltpu.CompilerParams(dimension_semantics=("arbitrary",), vmem_limit_bytes=60 * 2 ** 20),
        cost_estimate=pl.CostEstimate(flops=2 * tokens * width * f_pad, bytes_accessed=m.size + 2 * w.size + 3 * tokens * f_pad, transcendentals=tokens * f_pad),
        name="up_act",
    )(m, w, *filled)


def up_back_kernel(dy_ref, wd_ref, g_ref, l_ref, out_ref):
    f_pad = g_ref.shape[1]
    for j in range(0, f_pad, F_BLOCK):
        c = slice(j, j + F_BLOCK)
        d_act = mm(dy_ref[...], wd_ref[c, :], NT_DIMS)
        gate, lin = g_ref[:, c].astype(F32), l_ref[:, c].astype(F32)
        sig = 1.0 / (1.0 + jnp.exp(-gate))
        gate_sig = gate * sig
        out_ref[:, c] = (d_act * (lin * (sig + gate_sig * (1.0 - sig)))).astype(BF16)
        out_ref[:, f_pad + j:f_pad + j + F_BLOCK] = (d_act * gate_sig).astype(BF16)


def up_back(dy, wd, gate_low, lin_low):
    tokens, width = dy.shape
    f_pad = wd.shape[0]
    row = lambda i: (i, 0)
    return pl.pallas_call(
        up_back_kernel,
        grid=(tokens // T_BLOCK,),
        in_specs=[pl.BlockSpec((T_BLOCK, width), row), pl.BlockSpec(wd.shape, lambda i: (0, 0), pipeline_mode=pl.Buffered(1)), pl.BlockSpec((T_BLOCK, f_pad), row), pl.BlockSpec((T_BLOCK, f_pad), row)],
        out_specs=pl.BlockSpec((T_BLOCK, 2 * f_pad), row),
        out_shape=jax.ShapeDtypeStruct((tokens, 2 * f_pad), BF16),
        compiler_params=pltpu.CompilerParams(dimension_semantics=("arbitrary",), vmem_limit_bytes=60 * 2 ** 20),
        cost_estimate=pl.CostEstimate(flops=2 * tokens * width * f_pad, bytes_accessed=2 * (dy.size + wd.size + 4 * tokens * f_pad), transcendentals=2 * tokens * f_pad),
        name="up_back",
    )(dy, wd, gate_low, lin_low)


def shifted_tile(load, start, limit):
    tile, phase = start // LANES, start % LANES
    near = load(min(max(tile, 0), limit - 1))
    if phase == 0:
        return near
    after_it = load(min(max(tile + 1, 0), limit - 1))
    lane = lax.broadcasted_iota(jnp.int32, near.shape, 1)
    return jnp.where(lane < LANES - phase, pltpu.roll(near, LANES - phase, 1), pltpu.roll(after_it, LANES - phase, 1))


def gathered_tile(lo, segments, shape):
    lane = lax.broadcasted_iota(jnp.int32, shape, 1)
    out = jnp.zeros(shape, F32)
    for first, length, load, there, limit in segments:
        a, b = max(first, lo), min(first + length, lo + LANES)
        if a < b:
            part = shifted_tile(load, there + lo - first, limit)
            inside = (lane >= a - lo) & (lane < b - lo)
            out = part if b - a == LANES else jnp.where(inside, part, out)
    return out


def split_kernel(group, f_loc, rank_ref, w_ref, *out_refs):
    rows, cols = w_ref.shape
    f_pad = out_refs[0].shape[1] // 2

    def load(t):
        return w_ref[:, t * LANES:(t + 1) * LANES].astype(F32)

    for r in range(group):
        @pl.when(rank_ref[0] == r)
        def _():
            for q in range(group):
                for h in range(2):
                    segments = [(s * f_pad // 2, f_loc, load, ((2 * h + s) * group + q) * f_loc, cols // LANES) for s in range(2)]
                    for lo in range(0, f_pad, LANES):
                        out_refs[r ^ q][:, h * f_pad + lo:h * f_pad + lo + LANES] = gathered_tile(lo, segments, (rows, LANES)).astype(BF16)


def split_up(w_up, rank, group, f_loc, f_pad):
    rows, cols = w_up.shape
    step = 32
    return pl.pallas_call(
        functools.partial(split_kernel, group, f_loc),
        grid_spec=pltpu.PrefetchScalarGridSpec(
            num_scalar_prefetch=1,
            grid=(rows // step,),
            in_specs=[pl.BlockSpec((step, cols), lambda i, r: (i, 0))],
            out_specs=[pl.BlockSpec((step, 2 * f_pad), lambda i, r: (i, 0))] * group,
        ),
        out_shape=[jax.ShapeDtypeStruct((rows, 2 * f_pad), BF16)] * group,
        compiler_params=pltpu.CompilerParams(dimension_semantics=("arbitrary",)),
        cost_estimate=pl.CostEstimate(flops=20 * rows * cols, bytes_accessed=4 * rows * cols, transcendentals=0),
        name="split_up",
    )(rank.reshape(1), w_up)


def join_kernel(group, f_loc, rank_ref, *refs):
    parts, out_ref = refs[:group], refs[group]
    rows, cols = out_ref.shape
    f_pad = parts[0].shape[1] // 2
    half = cols // 2
    for r in range(group):
        @pl.when(rank_ref[0] == r)
        def _():
            def loader(ref):
                return lambda t: ref[:, t * LANES:(t + 1) * LANES]

            for h in range(2):
                segments = [(b * f_loc, f_loc, loader(parts[r ^ (b % group)]), h * f_pad + b // group * f_pad // 2, 2 * f_pad // LANES) for b in range(2 * group)]
                for lo in range(0, half, LANES):
                    out_ref[:, h * half + lo:h * half + lo + LANES] = gathered_tile(lo, segments, (rows, LANES))


def join_up(parts, rank, group, f_loc):
    rows, width = parts[0].shape
    cols = 4 * group * f_loc
    step = 32
    return pl.pallas_call(
        functools.partial(join_kernel, group, f_loc),
        grid_spec=pltpu.PrefetchScalarGridSpec(
            num_scalar_prefetch=1,
            grid=(rows // step,),
            in_specs=[pl.BlockSpec((step, width), lambda i, r: (i, 0))] * group,
            out_specs=pl.BlockSpec((step, cols), lambda i, r: (i, 0)),
        ),
        out_shape=jax.ShapeDtypeStruct((rows, cols), F32),
        compiler_params=pltpu.CompilerParams(dimension_semantics=("arbitrary",)),
        cost_estimate=pl.CostEstimate(flops=20 * rows * cols, bytes_accessed=8 * rows * cols, transcendentals=0),
        name="join_up",
    )(rank.reshape(1), *parts)


def solution(mesh):
    ax = mesh.axis_names[0]
    n_dev = mesh.shape[ax]
    group = n_dev // 2

    def hop(v, k):
        return lax.ppermute(v, ax, [(i, i ^ k) for i in range(n_dev)])

    def gather_rows(shard):
        return lax.all_gather(shard, ax, axis=0, tiled=True)

    def scatter_rows(full):
        return lax.psum_scatter(full, ax, scatter_dimension=0, tiled=True)

    def joined(parts):
        rows, cols = parts[0].shape
        out = jnp.zeros((group * rows, cols), parts[0].dtype)
        for k, v in enumerate(parts):
            out = lax.dynamic_update_slice(out, v, (k * rows, 0))
        return out

    def layer(hidden, positions, grad_y, attn_gain, w_qkv, b_qkv, w_out, mlp_gain, w_up, w_down):
        batch, seq_len, width = hidden.shape
        tokens = batch * seq_len
        h_loc = w_up.shape[0]
        h_chip = 2 * h_loc
        f_loc = w_down.shape[0]
        f_blk = f_loc + -f_loc % LANES
        f_pad = 2 * f_blk
        q_loc = b_qkv.shape[0]
        me = lax.axis_index(ax)
        rank = lax.rem(me, group)
        side = lax.div(me, group)
        core = lax.rem(me, 2)
        chip = lax.div(me, 2)

        wqkv = gather_rows(w_qkv)
        wout = gather_rows(w_out)
        small = jnp.concatenate([attn_gain, b_qkv, mlp_gain])[None]
        for k in (1, 2, group):
            far = hop(small, k)
            small = jnp.where((me & k) == 0, jnp.concatenate([small, far]), jnp.concatenate([far, small]))
        up_part = split_up(w_up, rank, group, f_loc, f_pad)
        small, *up_part, w_down, grad_y = after(small, *up_part, w_down, grad_y)
        gain_one = small[:, :h_loc].reshape(1, width).astype(F32)
        bias = small[:, h_loc:h_loc + q_loc].reshape(1, n_dev * q_loc).astype(F32)
        gain_two = small[:, h_loc + q_loc:].reshape(1, width).astype(F32)

        up_near = [up_part[0]] + [hop(up_part[k], k) for k in (1, 2, 3)]
        up_far = [hop(v, group) for v in up_near]
        down_far = hop(w_down, group)
        dy = grad_y.reshape(tokens, width)
        dy_parts = [dy, hop(dy, 1), hop(dy, 2)]

        hid_wide = hidden.astype(F32).reshape(tokens, width)
        inv_one = norm_scale(hid_wide)
        normed = (hid_wide * inv_one * gain_one).astype(BF16)
        q_width = wout.shape[0]
        kv_width = (wqkv.shape[1] - q_width) // 2
        kv_heads = kv_width // HEAD_DIM
        heads = q_width // HEAD_DIM
        cos_t, sin_t = rope_tables(positions)
        z = mm(normed, wqkv, NN_DIMS) + bias
        qkv, context = attend(z, cos_t, sin_t, batch, heads, kv_heads)
        mid = (hid_wide + mm(context, wout, NN_DIMS)).astype(BF16)
        mid_wide = mid.astype(F32)
        inv_two = norm_scale(mid_wide)
        mlp_in = (mid_wide * inv_two * gain_two).astype(BF16)
        w_all = jnp.zeros((width, 2 * f_pad), BF16)
        for k in range(group):
            w_all = lax.dynamic_update_slice(w_all, up_near[k], ((me ^ k) * h_loc, 0))
        for k in (0, 1, 2):
            w_all = lax.dynamic_update_slice(w_all, up_far[k], ((me ^ group ^ k) * h_loc, 0))
        m_near = hop(mlp_in, 1)
        m_all = joined([mlp_in, m_near])
        dy_all = joined(dy_parts[:2])
        wd_all = lax.dynamic_update_slice(jnp.zeros((f_pad, width), BF16), w_down, (side * f_blk, 0))
        m_far = hop(mlp_in, 2)
        w_all = lax.dynamic_update_slice(w_all, up_far[3], ((me ^ group ^ 3) * h_loc, 0))
        m_all, dy_all, w_all, wd_all = after(m_all, dy_all, w_all, wd_all)

        made = up_act(m_all, w_all, 0)
        *made, m_all, m_far = after(*made, m_all, m_far)
        m_all = lax.dynamic_update_slice(m_all, m_far, (2 * tokens, 0))
        m_all = lax.dynamic_update_slice(m_all, hop(m_far, 1), (3 * tokens, 0))
        gate_low, lin_low, act = up_act(m_all, w_all, 1, made)
        act, dy_far, down_far, dy_all = after(act, dy_parts[2], down_far, dy_all)
        dy_parts[2:] = [dy_far, hop(dy_far, 1)]
        for k in (2, 3):
            dy_all = lax.dynamic_update_slice(dy_all, dy_parts[k], (k * tokens, 0))
        wd_all = lax.dynamic_update_slice(wd_all, down_far, ((1 - side) * f_blk, 0))

        def block(rows, k, w, dims):
            return mm(rows[k * tokens:(k + 1) * tokens], w, dims)

        def down_grad(a, blk):
            return mm(lax.dynamic_slice(a, (0, blk * f_blk), (group * tokens, f_blk)), dy_all, TN_DIMS)

        def up_grad(m, d_up, block_id, chips):
            cols = lax.dynamic_slice(m, (0, block_id * chips * h_chip), (group * tokens, chips * h_chip))
            return mm(cols, d_up, TN_DIMS)

        y3 = block(act, 3, wd_all, NN_DIMS)
        act, y3 = after(act, y3)
        y3 = hop(y3, 1)
        y2 = block(act, 2, wd_all, NN_DIMS)
        act, y2 = after(act, y2)
        act, dy_all, y2 = after(act, dy_all, y2 + y3)
        y2 = hop(y2, 2)
        down_sum = down_grad(act, 1 - side)
        down_sum, act, gate_low, lin_low = after(down_sum, act, gate_low, lin_low)
        down_sum = hop(down_sum, group)
        d_up = up_back(dy_all, wd_all, gate_low, lin_low)

        dm3 = block(d_up, 3, w_all, NT_DIMS)
        d_up, dm3 = after(d_up, dm3)
        dm3 = hop(dm3, 1)
        dm2 = block(d_up, 2, w_all, NT_DIMS)
        d_up, dm2 = after(d_up, dm2)
        d_up, dm2 = after(d_up, dm2 + dm3)
        dm2 = hop(dm2, 2)

        far_a = up_grad(m_all, d_up, chip ^ 3, 1)
        d_up, far_a = after(d_up, far_a)
        far_a = hop(far_a, group)
        far_b = up_grad(m_all, d_up, chip ^ 2, 1)
        d_up, far_b = after(d_up, far_b)
        far_b = hop(far_b, group)
        near = up_grad(m_all, d_up, side, 2)
        d_up, near = after(d_up, near)
        dm1 = block(d_up, 1, w_all, NT_DIMS)
        d_up, dm1 = after(d_up, dm1)
        dm1 = hop(dm1, 1)
        dm0 = block(d_up, 0, w_all, NT_DIMS)
        d_up, dm0, act, dm2, near = after(d_up, dm0, act, dm2, near)

        x_id = lax.rem(chip, 2)

        def rows_of(near, x, c, far):
            own = lax.dynamic_slice(near, (x * h_chip + c * h_loc, 0), (h_loc, 2 * f_pad))
            return own + lax.dynamic_slice(far, (c * h_loc, 0), (h_loc, 2 * f_pad))

        piece2 = hop(rows_of(near, 1 - x_id, core, far_a), 2)
        piece3 = hop(rows_of(near, 1 - x_id, 1 - core, far_a), 3)

        d_m = dm0 + dm1 + dm2
        grad_mlp_gain = jnp.sum(d_m * mid_wide * inv_two, axis=0)
        scaled_two = d_m * gain_two
        d_mid = dy.astype(F32) + inv_two * (scaled_two - mid_wide * inv_two * inv_two * jnp.mean(scaled_two * mid_wide, axis=-1, keepdims=True))
        d_mid_low = d_mid.astype(BF16)
        grad_w_out = scatter_rows(mm(context, d_mid_low, TN_DIMS))
        d_context = mm(d_mid_low, wout, NT_DIMS).astype(BF16)
        d_proj, grad_b_qkv = attend_back(qkv, d_context, cos_t, sin_t, batch, heads, kv_heads)
        grad_w_qkv = mm(normed, d_proj, TN_DIMS)
        grad_w_qkv, d_proj = after(grad_w_qkv, d_proj)
        grad_w_qkv = scatter_rows(grad_w_qkv)
        d_normed = mm(d_proj, wqkv, NT_DIMS)
        d_normed, act = after(d_normed, act)
        y1 = hop(block(act, 1, wd_all, NN_DIMS), 1)
        act, d_normed, y1, down_sum = after(act, d_normed, y1, down_sum)
        grad_w_down = mm(lax.dynamic_slice(act, (0, side * f_blk), (group * tokens, f_blk)), dy_all, TN_DIMS)[:f_loc] + down_sum[:f_loc]
        grad_w_down, act, near = after(grad_w_down, act, near)
        grad_attn_gain = jnp.sum(d_normed * hid_wide * inv_one, axis=0)
        small_grads = jnp.concatenate([grad_attn_gain.reshape(n_dev, h_loc), grad_b_qkv.reshape(n_dev, q_loc), grad_mlp_gain.reshape(n_dev, h_loc)], axis=1)

        def halved(sums, k):
            pair = sums.reshape(-1, 2, h_loc + q_loc + h_loc)
            mine = lax.div(me, k) % 2
            return lax.dynamic_index_in_dim(pair, mine, 1, keepdims=False) + hop(lax.dynamic_index_in_dim(pair, 1 - mine, 1, keepdims=False), k)

        small_grads = halved(halved(small_grads, 1), 2)
        scaled_one = d_normed * gain_one
        grad_hidden = (d_mid + inv_one * (scaled_one - hid_wide * inv_one * inv_one * jnp.mean(scaled_one * hid_wide, axis=-1, keepdims=True))).astype(BF16)
        act, y1, y2, mid, grad_hidden = after(act, y1, y2, mid, grad_hidden)
        output = (mid.astype(F32) + (block(act, 0, wd_all, NN_DIMS) + y1 + y2)).astype(BF16)
        far_b, output, grad_hidden, grad_w_down, small_grads = after(far_b, output, grad_hidden, grad_w_down, small_grads)
        small_grads = halved(small_grads, group).reshape(-1)
        piece0 = rows_of(near, x_id, core, far_b)
        piece1 = hop(rows_of(near, x_id, 1 - core, far_b), 1)
        grad_w_up = join_up([piece0, piece1, piece2, piece3], rank, group, f_loc)
        return (output.reshape(hidden.shape), grad_hidden.reshape(hidden.shape), small_grads[:h_loc], grad_w_qkv, small_grads[h_loc:h_loc + q_loc], grad_w_out, small_grads[h_loc + q_loc:], grad_w_up, grad_w_down)

    row_spec = P(ax)
    return jax.shard_map(layer, mesh=mesh, in_specs=(row_spec,) * 10, out_specs=(row_spec,) * 9, check_vma=False)
```

```python
import functools

import jax
import jax.numpy as jnp
from jax import lax
from jax.experimental import pallas as pl
from jax.experimental.pallas import tpu as pltpu
from jax.sharding import PartitionSpec as P


HEAD_DIM = 128
ROT_DIM = 64
ROPE_BASE = 10000.0
EPS = 1e-5

NT_DIMS = (((1,), (1,)), ((), ()))
TN_DIMS = (((0,), (0,)), ((), ()))
NN_DIMS = (((1,), (0,)), ((), ()))
F32 = jnp.float32
BF16 = jnp.bfloat16
SCALE = HEAD_DIM ** -0.5
MASKED = -1e30
Q_BLOCK = 128
S_BLOCK = 64
T_BLOCK = 768
F_BLOCK = 256
LANES = 128
LOG2_E = 1.4426950408889634


def mm(a, b, dims):
    return lax.dot_general(a, b, dims, preferred_element_type=F32)


def after(*vals):
    return lax.optimization_barrier(vals)


def norm_scale(rows_in):
    return lax.rsqrt(jnp.mean(rows_in * rows_in, axis=-1, keepdims=True) + EPS)


def rope_tables(positions):
    lane = jnp.arange(HEAD_DIM, dtype=jnp.int32)
    pair = (lane - lane % 2).astype(F32)
    inv_freq = 1.0 / (ROPE_BASE ** (pair / ROT_DIM))
    angles = positions.astype(F32).reshape(-1, 1) * inv_freq
    turned = lane < ROT_DIM
    sines = jnp.sin(angles)
    return jnp.where(turned, jnp.cos(angles), 1.0), jnp.where(turned, jnp.where(lane % 2 == 0, -sines, sines), 0.0)


def swap_pairs(v):
    lane = lax.broadcasted_iota(jnp.int32, v.shape, 1)
    return jnp.where(lane % 2 == 0, pltpu.roll(v, HEAD_DIM - 1, 1), pltpu.roll(v, 1, 1))


def attend_kernel(heads, kv_heads, z_ref, cos_ref, sin_ref, qkv_ref, ctx_ref, *bufs):
    s_refs, p_refs = bufs[:2], bufs[2:]
    seq_len = z_ref.shape[0]
    group = heads // kv_heads
    cos_t, sin_t = cos_ref[...], sin_ref[...]

    def cols(i):
        return pl.ds(pl.multiple_of(i * HEAD_DIM, HEAD_DIM), HEAD_DIM)

    @pl.loop(0, heads + kv_heads, unroll=3)
    def _(i):
        zh = z_ref[:, cols(i)]
        qkv_ref[:, cols(i)] = (zh * cos_t + swap_pairs(zh) * sin_t).astype(BF16)

    qkv_ref[:, (heads + kv_heads) * HEAD_DIM:] = z_ref[:, (heads + kv_heads) * HEAD_DIM:].astype(BF16)

    @pl.loop(0, kv_heads)
    def _(g):
        kc, vc = cols(heads + g), cols(heads + kv_heads + g)
        for r in range(0, seq_len, Q_BLOCK):
            n = r + Q_BLOCK
            q = jnp.concatenate([qkv_ref[r:n, cols(g * group + h)] for h in range(group)], axis=0)
            s_ref, p_ref = s_refs[r // Q_BLOCK % 2], p_refs[r // Q_BLOCK % 2]
            s_ref[:, :n] = mm(q, qkv_ref[:n, kc], NT_DIMS)

            @pl.loop(0, group * Q_BLOCK // S_BLOCK, unroll=True)
            def _(c):
                rows = pl.ds(pl.multiple_of(c * S_BLOCK, S_BLOCK), S_BLOCK)
                s = s_ref[rows, :n]
                row = lax.broadcasted_iota(jnp.int32, (S_BLOCK, Q_BLOCK), 0) + lax.rem(c * S_BLOCK, Q_BLOCK)
                col = lax.broadcasted_iota(jnp.int32, (S_BLOCK, Q_BLOCK), 1)
                own = jnp.where(row >= col, s[:, r:], MASKED)
                s = own if r == 0 else jnp.concatenate([s[:, :r], own], axis=1)
                e = jnp.exp2((s - jnp.max(s, axis=1, keepdims=True)) * (SCALE * LOG2_E))
                p_ref[rows, :n] = (e * (1.0 / jnp.sum(e, axis=1, keepdims=True))).astype(BF16)

            ctx = mm(p_ref[:, :n], qkv_ref[:n, vc], NN_DIMS).astype(BF16)
            for h in range(group):
                ctx_ref[r:n, cols(g * group + h)] = ctx[h * Q_BLOCK:(h + 1) * Q_BLOCK]


def attend_back_kernel(heads, kv_heads, qkv_ref, dctx_ref, cos_ref, sin_ref, dz_ref, sum_ref, dk_ref, dv_ref, s_ref, dp_ref, p_ref, ds_ref):
    seq_len = qkv_ref.shape[0]
    group = heads // kv_heads

    def cols(i):
        return pl.ds(pl.multiple_of(i * HEAD_DIM, HEAD_DIM), HEAD_DIM)

    @pl.when(pl.program_id(0) == 0)
    def _():
        sum_ref[...] = jnp.zeros_like(sum_ref)

    def put(rows, c, d):
        dz_ref[rows, c] = d.astype(BF16)
        sum_ref[:, c] += jnp.sum(d, axis=0, keepdims=True)

    def turned_back(rows, d):
        return d * cos_ref[rows, :] - swap_pairs(d) * sin_ref[rows, :]

    @pl.loop(0, kv_heads)
    def _(g):
        kc, vc = cols(heads + g), cols(heads + kv_heads + g)
        dk_ref[...] = jnp.zeros_like(dk_ref)
        dv_ref[...] = jnp.zeros_like(dv_ref)
        for r in range(0, seq_len, Q_BLOCK):
            n = r + Q_BLOCK
            q = jnp.concatenate([qkv_ref[r:n, cols(g * group + h)] for h in range(group)], axis=0)
            d = jnp.concatenate([dctx_ref[r:n, cols(g * group + h)] for h in range(group)], axis=0)
            s_ref[:n] = mm(qkv_ref[:n, kc], q, NT_DIMS)
            dp_ref[:n] = mm(qkv_ref[:n, vc], d, NT_DIMS)

            @pl.loop(0, group, unroll=True)
            def _(h):
                c = cols(h)
                s, dp = s_ref[:n, c], dp_ref[:n, c]
                row = lax.broadcasted_iota(jnp.int32, (Q_BLOCK, Q_BLOCK), 0)
                col = lax.broadcasted_iota(jnp.int32, (Q_BLOCK, Q_BLOCK), 1)
                own = jnp.where(row <= col, s[r:], MASKED)
                s = own if r == 0 else jnp.concatenate([s[:r], own], axis=0)
                e = jnp.exp2((s - jnp.max(s, axis=0, keepdims=True)) * (SCALE * LOG2_E))
                p = e * (1.0 / jnp.sum(e, axis=0, keepdims=True))
                p_ref[:n, c] = p.astype(BF16)
                ds_ref[:n, c] = (p * (dp - jnp.sum(p * dp, axis=0, keepdims=True)) * SCALE).astype(BF16)

            dv_ref[:n] += mm(p_ref[:n], d, NN_DIMS)
            dk_ref[:n] += mm(ds_ref[:n], q, NN_DIMS)
            dq = mm(qkv_ref[:n, kc], ds_ref[:n], TN_DIMS)
            for h in range(group):
                rows = slice(r, n)
                put(rows, cols(g * group + h), turned_back(rows, jnp.transpose(dq[:, h * Q_BLOCK:(h + 1) * Q_BLOCK])))

        rows = slice(0, seq_len)
        put(rows, kc, turned_back(rows, dk_ref[...]))
        put(rows, vc, dv_ref[...])


def attend(z, cos_t, sin_t, batch, heads, kv_heads):
    tokens, width = z.shape
    seq_len = tokens // batch
    row = lambda b: (b, 0)
    flops = 4 * tokens * seq_len * heads * HEAD_DIM
    return pl.pallas_call(
        functools.partial(attend_kernel, heads, kv_heads),
        grid=(batch,),
        in_specs=[pl.BlockSpec((seq_len, width), row), pl.BlockSpec((seq_len, HEAD_DIM), row), pl.BlockSpec((seq_len, HEAD_DIM), row)],
        out_specs=[pl.BlockSpec((seq_len, width), row), pl.BlockSpec((seq_len, heads * HEAD_DIM), row)],
        out_shape=[jax.ShapeDtypeStruct((tokens, width), BF16), jax.ShapeDtypeStruct((tokens, heads * HEAD_DIM), BF16)],
        scratch_shapes=[pltpu.VMEM((heads // kv_heads * Q_BLOCK, seq_len), t) for t in (F32, F32, BF16, BF16)],
        compiler_params=pltpu.CompilerParams(dimension_semantics=("arbitrary",), vmem_limit_bytes=48 * 2 ** 20),
        cost_estimate=pl.CostEstimate(flops=3 * flops, bytes_accessed=tokens * width * 8, transcendentals=tokens * seq_len * heads),
        name="attend",
    )(z, cos_t, sin_t)


def attend_back(qkv, d_ctx, cos_t, sin_t, batch, heads, kv_heads):
    tokens, width = qkv.shape
    seq_len = tokens // batch
    row = lambda b: (b, 0)
    flops = 10 * tokens * seq_len * heads * HEAD_DIM
    return pl.pallas_call(
        functools.partial(attend_back_kernel, heads, kv_heads),
        grid=(batch,),
        in_specs=[pl.BlockSpec((seq_len, width), row), pl.BlockSpec((seq_len, heads * HEAD_DIM), row), pl.BlockSpec((seq_len, HEAD_DIM), row), pl.BlockSpec((seq_len, HEAD_DIM), row)],
        out_specs=[pl.BlockSpec((seq_len, width), row), pl.BlockSpec((1, width), lambda b: (0, 0))],
        out_shape=[jax.ShapeDtypeStruct((tokens, width), BF16), jax.ShapeDtypeStruct((1, width), F32)],
        scratch_shapes=[pltpu.VMEM((seq_len, HEAD_DIM), F32)] * 2 + [pltpu.VMEM((seq_len, heads // kv_heads * Q_BLOCK), F32)] * 2 + [pltpu.VMEM((seq_len, heads // kv_heads * Q_BLOCK), BF16)] * 2,
        compiler_params=pltpu.CompilerParams(dimension_semantics=("arbitrary",), vmem_limit_bytes=48 * 2 ** 20),
        cost_estimate=pl.CostEstimate(flops=3 * flops, bytes_accessed=tokens * width * 8, transcendentals=tokens * seq_len * heads),
        name="attend_back",
    )(qkv, d_ctx, cos_t, sin_t)


def up_kernel(m_ref, w_ref, *refs):
    g_ref, l_ref, a_ref = refs[-3:]
    f_pad = g_ref.shape[1]
    for j in range(0, f_pad, F_BLOCK):
        c = slice(j, j + F_BLOCK)
        gate_low = mm(m_ref[...], w_ref[:, c], NN_DIMS).astype(BF16)
        lin_low = mm(m_ref[...], w_ref[:, f_pad + j:f_pad + j + F_BLOCK], NN_DIMS).astype(BF16)
        g_ref[:, c] = gate_low
        l_ref[:, c] = lin_low
        gate = gate_low.astype(F32)
        a_ref[:, c] = (gate * (1.0 / (1.0 + jnp.exp(-gate))) * lin_low.astype(F32)).astype(BF16)


def up_act(m, w, half, filled=()):
    tokens, width = m.shape
    f_pad = w.shape[1] // 2
    steps = tokens // 2 // T_BLOCK
    row = lambda i: (i + half * steps, 0)
    return pl.pallas_call(
        up_kernel,
        grid=(steps,),
        in_specs=[pl.BlockSpec((T_BLOCK, width), row), pl.BlockSpec(w.shape, lambda i: (0, 0), pipeline_mode=pl.Buffered(1))] + [pl.BlockSpec(memory_space=pl.ANY)] * len(filled),
        out_specs=[pl.BlockSpec((T_BLOCK, f_pad), row)] * 3,
        out_shape=[jax.ShapeDtypeStruct((tokens, f_pad), BF16)] * 3,
        input_output_aliases={2 + i: i for i in range(len(filled))},
        compiler_params=pltpu.CompilerParams(dimension_semantics=("arbitrary",), vmem_limit_bytes=60 * 2 ** 20),
        cost_estimate=pl.CostEstimate(flops=2 * tokens * width * f_pad, bytes_accessed=m.size + 2 * w.size + 3 * tokens * f_pad, transcendentals=tokens * f_pad),
        name="up_act",
    )(m, w, *filled)


def up_back_kernel(dy_ref, wd_ref, g_ref, l_ref, out_ref):
    f_pad = g_ref.shape[1]
    for j in range(0, f_pad, F_BLOCK):
        c = slice(j, j + F_BLOCK)
        d_act = mm(dy_ref[...], wd_ref[c, :], NT_DIMS)
        gate, lin = g_ref[:, c].astype(F32), l_ref[:, c].astype(F32)
        sig = 1.0 / (1.0 + jnp.exp(-gate))
        gate_sig = gate * sig
        out_ref[:, c] = (d_act * (lin * (sig + gate_sig * (1.0 - sig)))).astype(BF16)
        out_ref[:, f_pad + j:f_pad + j + F_BLOCK] = (d_act * gate_sig).astype(BF16)


def up_back(dy, wd, gate_low, lin_low):
    tokens, width = dy.shape
    f_pad = wd.shape[0]
    row = lambda i: (i, 0)
    return pl.pallas_call(
        up_back_kernel,
        grid=(tokens // T_BLOCK,),
        in_specs=[pl.BlockSpec((T_BLOCK, width), row), pl.BlockSpec(wd.shape, lambda i: (0, 0), pipeline_mode=pl.Buffered(1)), pl.BlockSpec((T_BLOCK, f_pad), row), pl.BlockSpec((T_BLOCK, f_pad), row)],
        out_specs=pl.BlockSpec((T_BLOCK, 2 * f_pad), row),
        out_shape=jax.ShapeDtypeStruct((tokens, 2 * f_pad), BF16),
        compiler_params=pltpu.CompilerParams(dimension_semantics=("arbitrary",), vmem_limit_bytes=60 * 2 ** 20),
        cost_estimate=pl.CostEstimate(flops=2 * tokens * width * f_pad, bytes_accessed=2 * (dy.size + wd.size + 4 * tokens * f_pad), transcendentals=2 * tokens * f_pad),
        name="up_back",
    )(dy, wd, gate_low, lin_low)


def shifted_tile(load, start, limit):
    tile, phase = start // LANES, start % LANES
    near = load(min(max(tile, 0), limit - 1))
    if phase == 0:
        return near
    after_it = load(min(max(tile + 1, 0), limit - 1))
    lane = lax.broadcasted_iota(jnp.int32, near.shape, 1)
    return jnp.where(lane < LANES - phase, pltpu.roll(near, LANES - phase, 1), pltpu.roll(after_it, LANES - phase, 1))


def gathered_tile(lo, segments, shape):
    lane = lax.broadcasted_iota(jnp.int32, shape, 1)
    out = jnp.zeros(shape, F32)
    for first, length, load, there, limit in segments:
        a, b = max(first, lo), min(first + length, lo + LANES)
        if a < b:
            part = shifted_tile(load, there + lo - first, limit)
            inside = (lane >= a - lo) & (lane < b - lo)
            out = part if b - a == LANES else jnp.where(inside, part, out)
    return out


def split_kernel(group, f_loc, rank_ref, w_ref, *out_refs):
    rows, cols = w_ref.shape
    f_pad = out_refs[0].shape[1] // 2

    def load(t):
        return w_ref[:, t * LANES:(t + 1) * LANES].astype(F32)

    for r in range(group):
        @pl.when(rank_ref[0] == r)
        def _():
            for q in range(group):
                for h in range(2):
                    segments = [(s * f_pad // 2, f_loc, load, ((2 * h + s) * group + q) * f_loc, cols // LANES) for s in range(2)]
                    for lo in range(0, f_pad, LANES):
                        out_refs[r ^ q][:, h * f_pad + lo:h * f_pad + lo + LANES] = gathered_tile(lo, segments, (rows, LANES)).astype(BF16)


def split_up(w_up, rank, group, f_loc, f_pad):
    rows, cols = w_up.shape
    step = 32
    return pl.pallas_call(
        functools.partial(split_kernel, group, f_loc),
        grid_spec=pltpu.PrefetchScalarGridSpec(
            num_scalar_prefetch=1,
            grid=(rows // step,),
            in_specs=[pl.BlockSpec((step, cols), lambda i, r: (i, 0))],
            out_specs=[pl.BlockSpec((step, 2 * f_pad), lambda i, r: (i, 0))] * group,
        ),
        out_shape=[jax.ShapeDtypeStruct((rows, 2 * f_pad), BF16)] * group,
        compiler_params=pltpu.CompilerParams(dimension_semantics=("arbitrary",)),
        cost_estimate=pl.CostEstimate(flops=20 * rows * cols, bytes_accessed=4 * rows * cols, transcendentals=0),
        name="split_up",
    )(rank.reshape(1), w_up)


def join_kernel(group, f_loc, rank_ref, *refs):
    parts, out_ref = refs[:group], refs[group]
    rows, cols = out_ref.shape
    f_pad = parts[0].shape[1] // 2
    half = cols // 2
    for r in range(group):
        @pl.when(rank_ref[0] == r)
        def _():
            def loader(ref):
                return lambda t: ref[:, t * LANES:(t + 1) * LANES]

            for h in range(2):
                segments = [(b * f_loc, f_loc, loader(parts[r ^ (b % group)]), h * f_pad + b // group * f_pad // 2, 2 * f_pad // LANES) for b in range(2 * group)]
                for lo in range(0, half, LANES):
                    out_ref[:, h * half + lo:h * half + lo + LANES] = gathered_tile(lo, segments, (rows, LANES))


def join_up(parts, rank, group, f_loc):
    rows, width = parts[0].shape
    cols = 4 * group * f_loc
    step = 32
    return pl.pallas_call(
        functools.partial(join_kernel, group, f_loc),
        grid_spec=pltpu.PrefetchScalarGridSpec(
            num_scalar_prefetch=1,
            grid=(rows // step,),
            in_specs=[pl.BlockSpec((step, width), lambda i, r: (i, 0))] * group,
            out_specs=pl.BlockSpec((step, cols), lambda i, r: (i, 0)),
        ),
        out_shape=jax.ShapeDtypeStruct((rows, cols), F32),
        compiler_params=pltpu.CompilerParams(dimension_semantics=("arbitrary",)),
        cost_estimate=pl.CostEstimate(flops=20 * rows * cols, bytes_accessed=8 * rows * cols, transcendentals=0),
        name="join_up",
    )(rank.reshape(1), *parts)


def solution(mesh):
    ax = mesh.axis_names[0]
    n_dev = mesh.shape[ax]
    group = n_dev // 2

    def hop(v, k):
        return lax.ppermute(v, ax, [(i, i ^ k) for i in range(n_dev)])

    def gather_rows(shard):
        return lax.all_gather(shard, ax, axis=0, tiled=True)

    def scatter_rows(full):
        return lax.psum_scatter(full, ax, scatter_dimension=0, tiled=True)

    def joined(parts):
        rows, cols = parts[0].shape
        out = jnp.zeros((group * rows, cols), parts[0].dtype)
        for k, v in enumerate(parts):
            out = lax.dynamic_update_slice(out, v, (k * rows, 0))
        return out

    def layer(hidden, positions, grad_y, attn_gain, w_qkv, b_qkv, w_out, mlp_gain, w_up, w_down):
        batch, seq_len, width = hidden.shape
        tokens = batch * seq_len
        h_loc = w_up.shape[0]
        h_chip = 2 * h_loc
        f_loc = w_down.shape[0]
        f_blk = f_loc + -f_loc % LANES
        f_pad = 2 * f_blk
        q_loc = b_qkv.shape[0]
        me = lax.axis_index(ax)
        rank = lax.rem(me, group)
        side = lax.div(me, group)
        core = lax.rem(me, 2)
        chip = lax.div(me, 2)

        wqkv = gather_rows(w_qkv)
        wout = gather_rows(w_out)
        small = jnp.concatenate([attn_gain, b_qkv, mlp_gain])[None]
        for k in (1, 2, group):
            far = hop(small, k)
            small = jnp.where((me & k) == 0, jnp.concatenate([small, far]), jnp.concatenate([far, small]))
        up_part = split_up(w_up, rank, group, f_loc, f_pad)
        small, *up_part, w_down, grad_y = after(small, *up_part, w_down, grad_y)
        gain_one = small[:, :h_loc].reshape(1, width).astype(F32)
        bias = small[:, h_loc:h_loc + q_loc].reshape(1, n_dev * q_loc).astype(F32)
        gain_two = small[:, h_loc + q_loc:].reshape(1, width).astype(F32)

        up_near = [up_part[0]] + [hop(up_part[k], k) for k in (1, 2, 3)]
        up_far = [hop(v, group) for v in up_near]
        down_far = hop(w_down, group)
        dy = grad_y.reshape(tokens, width)
        dy_parts = [dy, hop(dy, 1), hop(dy, 2)]

        hid_wide = hidden.astype(F32).reshape(tokens, width)
        inv_one = norm_scale(hid_wide)
        normed = (hid_wide * inv_one * gain_one).astype(BF16)
        q_width = wout.shape[0]
        kv_width = (wqkv.shape[1] - q_width) // 2
        kv_heads = kv_width // HEAD_DIM
        heads = q_width // HEAD_DIM
        cos_t, sin_t = rope_tables(positions)
        z = mm(normed, wqkv, NN_DIMS) + bias
        qkv, context = attend(z, cos_t, sin_t, batch, heads, kv_heads)
        mid = (hid_wide + mm(context, wout, NN_DIMS)).astype(BF16)
        mid_wide = mid.astype(F32)
        inv_two = norm_scale(mid_wide)
        mlp_in = (mid_wide * inv_two * gain_two).astype(BF16)
        w_all = jnp.zeros((width, 2 * f_pad), BF16)
        for k in range(group):
            w_all = lax.dynamic_update_slice(w_all, up_near[k], ((me ^ k) * h_loc, 0))
        for k in (0, 1, 2):
            w_all = lax.dynamic_update_slice(w_all, up_far[k], ((me ^ group ^ k) * h_loc, 0))
        m_near = hop(mlp_in, 1)
        m_all = joined([mlp_in, m_near])
        dy_all = joined(dy_parts[:2])
        wd_all = lax.dynamic_update_slice(jnp.zeros((f_pad, width), BF16), w_down, (side * f_blk, 0))
        m_far = hop(mlp_in, 2)
        w_all = lax.dynamic_update_slice(w_all, up_far[3], ((me ^ group ^ 3) * h_loc, 0))
        m_all, dy_all, w_all, wd_all = after(m_all, dy_all, w_all, wd_all)

        made = up_act(m_all, w_all, 0)
        *made, m_all, m_far = after(*made, m_all, m_far)
        m_all = lax.dynamic_update_slice(m_all, m_far, (2 * tokens, 0))
        m_all = lax.dynamic_update_slice(m_all, hop(m_far, 1), (3 * tokens, 0))
        gate_low, lin_low, act = up_act(m_all, w_all, 1, made)
        act, dy_far, dy_all, down_far = after(act, dy_parts[2], dy_all, down_far)
        wd_all = lax.dynamic_update_slice(wd_all, down_far, ((1 - side) * f_blk, 0))
        dy_rest = hop(dy_far, 1)

        def block(rows, k, w, dims):
            return mm(rows[k * tokens:(k + 1) * tokens], w, dims)

        def down_grad(a, blk):
            return mm(lax.dynamic_slice(a, (0, blk * f_blk), (group * tokens, f_blk)), dy_all, TN_DIMS)

        def up_grad(m, d_up, block_id, chips):
            cols = lax.dynamic_slice(m, (0, block_id * chips * h_chip), (group * tokens, chips * h_chip))
            return mm(cols, d_up, TN_DIMS)

        y3 = block(act, 3, wd_all, NN_DIMS)
        act, y3 = after(act, y3)
        y3 = hop(y3, 1)
        y2 = block(act, 2, wd_all, NN_DIMS)
        act, y2 = after(act, y2)
        act, dy_all, dy_far, dy_rest, y2 = after(act, dy_all, dy_far, dy_rest, y2 + y3)
        y2 = hop(y2, 2)
        dy_all = lax.dynamic_update_slice(dy_all, dy_far, (2 * tokens, 0))
        dy_all = lax.dynamic_update_slice(dy_all, dy_rest, (3 * tokens, 0))
        down_sum = down_grad(act, 1 - side)
        down_sum, act, gate_low, lin_low = after(down_sum, act, gate_low, lin_low)
        down_sum = hop(down_sum, group)
        d_up = up_back(dy_all, wd_all, gate_low, lin_low)

        dm3 = block(d_up, 3, w_all, NT_DIMS)
        d_up, dm3 = after(d_up, dm3)
        dm3 = hop(dm3, 1)
        far_a = up_grad(m_all, d_up, chip ^ 3, 1)
        d_up, far_a = after(d_up, far_a)
        far_a = hop(far_a, group)
        dm2 = block(d_up, 2, w_all, NT_DIMS) + dm3
        d_up, dm2 = after(d_up, dm2)
        dm2 = hop(dm2, 2)
        far_b = up_grad(m_all, d_up, chip ^ 2, 1)
        d_up, far_b = after(d_up, far_b)
        far_b = hop(far_b, group)
        near = up_grad(m_all, d_up, side, 2)
        d_up, near = after(d_up, near)
        dm1 = block(d_up, 1, w_all, NT_DIMS)
        d_up, dm1 = after(d_up, dm1)
        dm1 = hop(dm1, 1)
        dm0 = block(d_up, 0, w_all, NT_DIMS)
        d_up, dm0, act, dm2, near = after(d_up, dm0, act, dm2, near)

        x_id = lax.rem(chip, 2)

        def rows_of(near, x, c, far):
            own = lax.dynamic_slice(near, (x * h_chip + c * h_loc, 0), (h_loc, 2 * f_pad))
            return own + lax.dynamic_slice(far, (c * h_loc, 0), (h_loc, 2 * f_pad))

        piece2 = hop(rows_of(near, 1 - x_id, core, far_a), 2)
        piece3 = hop(rows_of(near, 1 - x_id, 1 - core, far_a), 3)

        d_m = dm0 + dm1 + dm2
        grad_mlp_gain = jnp.sum(d_m * mid_wide * inv_two, axis=0)
        scaled_two = d_m * gain_two
        d_mid = dy.astype(F32) + inv_two * (scaled_two - mid_wide * inv_two * inv_two * jnp.mean(scaled_two * mid_wide, axis=-1, keepdims=True))
        d_mid_low = d_mid.astype(BF16)
        grad_w_out = scatter_rows(mm(context, d_mid_low, TN_DIMS))
        d_context = mm(d_mid_low, wout, NT_DIMS).astype(BF16)
        d_proj, grad_b_qkv = attend_back(qkv, d_context, cos_t, sin_t, batch, heads, kv_heads)
        grad_w_qkv = mm(normed, d_proj, TN_DIMS)
        grad_w_qkv, d_proj = after(grad_w_qkv, d_proj)
        grad_w_qkv = scatter_rows(grad_w_qkv)
        d_normed = mm(d_proj, wqkv, NT_DIMS)
        d_normed, act = after(d_normed, act)
        y1 = block(act, 1, wd_all, NN_DIMS)
        act, d_normed, y1, down_sum = after(act, d_normed, y1, down_sum)
        y1 = hop(y1, 1)
        grad_w_down = mm(lax.dynamic_slice(act, (0, side * f_blk), (group * tokens, f_blk)), dy_all, TN_DIMS)[:f_loc] + down_sum[:f_loc]
        grad_w_down, act, near = after(grad_w_down, act, near)
        grad_attn_gain = jnp.sum(d_normed * hid_wide * inv_one, axis=0)
        small_grads = jnp.concatenate([grad_attn_gain.reshape(n_dev, h_loc), grad_b_qkv.reshape(n_dev, q_loc), grad_mlp_gain.reshape(n_dev, h_loc)], axis=1)

        def halved(sums, k):
            pair = sums.reshape(-1, 2, h_loc + q_loc + h_loc)
            mine = lax.div(me, k) % 2
            return lax.dynamic_index_in_dim(pair, mine, 1, keepdims=False) + hop(lax.dynamic_index_in_dim(pair, 1 - mine, 1, keepdims=False), k)

        small_grads = halved(halved(small_grads, 1), 2)
        scaled_one = d_normed * gain_one
        grad_hidden = (d_mid + inv_one * (scaled_one - hid_wide * inv_one * inv_one * jnp.mean(scaled_one * hid_wide, axis=-1, keepdims=True))).astype(BF16)
        act, y1, y2, mid, grad_hidden = after(act, y1, y2, mid, grad_hidden)
        output = (mid.astype(F32) + (block(act, 0, wd_all, NN_DIMS) + y1 + y2)).astype(BF16)
        far_b, output, grad_hidden, grad_w_down, small_grads = after(far_b, output, grad_hidden, grad_w_down, small_grads)
        small_grads = halved(small_grads, group).reshape(-1)
        piece0 = rows_of(near, x_id, core, far_b)
        piece1 = hop(rows_of(near, x_id, 1 - core, far_b), 1)
        grad_w_up = join_up([piece0, piece1, piece2, piece3], rank, group, f_loc)
        return (output.reshape(hidden.shape), grad_hidden.reshape(hidden.shape), small_grads[:h_loc], grad_w_qkv, small_grads[h_loc:h_loc + q_loc], grad_w_out, small_grads[h_loc + q_loc:], grad_w_up, grad_w_down)

    row_spec = P(ax)
    return jax.shard_map(layer, mesh=mesh, in_specs=(row_spec,) * 10, out_specs=(row_spec,) * 9, check_vma=False)
```
